32 devices in a mesh: height: 8 (over y, x, core), dp: 4 (over z).
Axes of the slice: x: 2, y: 2, z: 4, core: 2. Of those that a mesh axis runs over, the one named last changes fastest.
Arguments:
- x_next: bfloat16 [4, 16, 320, 128], P('dp', 'height'), may hold values from -12 to 12
- x_cur: bfloat16 [4, 16, 320, 128], P('dp', 'height'), may hold values from -12 to 12
- grad_out: bfloat16 [4, 16, 320, 128], P('dp', 'height'), may hold values from -6 to 6
- kernel: bfloat16 [3, 3, 320, 320], replicated, may hold values from -0.109375 to 0.109375
- gamma: float32 [320], replicated, may hold values from 0.25 to 1.75
- beta: float32 [320], replicated, may hold values from -2.5 to 2.5
Outputs:
- y_next: bfloat16 [4, 16, 320, 128], P('dp', 'height')
- grad_x: bfloat16 [4, 16, 320, 128], P('dp', 'height')
- grad_kernel: float32 [921600], P(('height', 'dp'))
The draws below stay inside these ranges and needn't reach their ends.
All inputs are finite; a program needn't handle non-finite values.
Results may differ from the reference program's by a relative error of at most 0.0049.
Values may be sent and summed in bfloat16 or wider, within the bound.
No kernel may reach another device: no remote copies, remote signals or barrier semaphores. Data moves between devices by JAX's collectives and lax.ppermute only.
A program may use at most 64 MiB of HBM per device.

```python
import jax
import jax.numpy as jnp
from jax import lax

CHANNELS = 320
GROUPS = 32
COLUMNS = 128
ROWS = 16
SAMPLES = 4


def draw_inputs(key):
    key_base, key_rows, key_chan, key_offset = jax.random.split(key, 4)
    shape = (SAMPLES, ROWS, CHANNELS, COLUMNS)
    base = jax.random.normal(key_base, shape, jnp.float32)
    spread = jax.random.uniform(key_rows, (1, ROWS, 1, 1), jnp.float32, 0.7, 1.3)
    rising = (0.6 + 1.2 * jnp.arange(ROWS, dtype=jnp.float32) / ROWS).reshape(1, ROWS, 1, 1)
    channel_scale = jnp.exp(jax.random.uniform(key_chan, (SAMPLES, 1, CHANNELS, 1), jnp.float32, -0.5, 0.5))
    offset = 0.3 * jax.random.normal(key_offset, (1, ROWS, 1, 1), jnp.float32)
    values = base * spread * rising * channel_scale + offset
    return jnp.clip(values, -12.0, 12.0).astype(jnp.bfloat16)


def draw_x_next(key, part):
    return draw_inputs(jax.random.fold_in(key, 11))


def draw_x_cur(key, part):
    return draw_inputs(jax.random.fold_in(key, 12))


def levels(own_key, dims, cuts, least, top_value):
    loudness, own = 1.0, jax.random.fold_in(own_key, 6)
    for dim, parts in cuts:
        heights = jnp.exp(jax.random.uniform(jax.random.fold_in(own, dim), (parts,), jnp.float32, least / len(cuts), top_value / len(cuts)))
        loudness = loudness * jnp.repeat(heights, dims[dim] // parts).reshape([-1 if axis == dim else 1 for axis in range(len(dims))])
    return loudness


def centred(stream_key, dims, width, most, cuts=(), kind=jnp.bfloat16):
    level = levels(stream_key, dims, cuts, -0.22, 0.18) if cuts else 1.0
    array = jax.random.normal(stream_key, dims, jnp.float32) * width * level
    return jnp.minimum(jnp.maximum(array, -most), most).astype(kind)


def setup_inputs(seed: int = 0) -> dict:
    arg_keys = jax.random.split(jax.random.key(seed), 7)
    x_next = draw_x_next(jax.random.fold_in(arg_keys[6], 71), 0)
    x_cur = draw_x_cur(jax.random.fold_in(arg_keys[6], 71), 0)
    grad_out = centred(arg_keys[2], (SAMPLES, ROWS, CHANNELS, COLUMNS), 1.0, 6.0, ((0, 4), (1, 8)))
    kernel = centred(arg_keys[3], (3, 3, CHANNELS, CHANNELS), (9 * CHANNELS) ** -0.5, 0.109375)
    gamma = jnp.clip(1.0 + 0.15 * jax.random.normal(arg_keys[4], (CHANNELS,), jnp.float32), 0.25, 1.75)
    beta = centred(arg_keys[5], (CHANNELS,), 0.5, 2.5, (), jnp.float32)
    return dict(x_next=x_next, x_cur=x_cur, grad_out=grad_out, kernel=kernel, gamma=gamma, beta=beta)


eps = 1e-05

def conv_full(image, weights):
    padded = jnp.pad(image, ((1, 1), (0, 0), (1, 1)))
    total = jnp.zeros((image.shape[0], weights.shape[2], image.shape[2]), jnp.float32)
    for tap_row in range(3):
        for tap_col in range(3):
            window = padded[tap_row:tap_row + image.shape[0], :, tap_col:tap_col + image.shape[2]]
            total = total + jnp.einsum('oc,hcw->how', weights[tap_row, tap_col], window)
    return total

def group_stats(value):
    grouped = value.reshape(value.shape[0], GROUPS, CHANNELS // GROUPS, value.shape[2])
    center = lax.optimization_barrier(jnp.mean(grouped, axis=(0, 2, 3), keepdims=True))
    spread = lax.optimization_barrier(jnp.mean((grouped - center) ** 2, axis=(0, 2, 3), keepdims=True))
    return (center, lax.rsqrt(spread + eps))

def normalize(value, gamma, beta):
    center, scale_inv = group_stats(value)
    grouped = value.reshape(value.shape[0], GROUPS, CHANNELS // GROUPS, value.shape[2])
    normed = ((grouped - center) * scale_inv).reshape(value.shape)
    affine = normed * gamma[None, :, None] + beta[None, :, None]
    return (normed, affine, scale_inv)

def one_sample(weights, gamma, beta, inputs):
    x_next, x_cur, grad_out = inputs
    z_next = conv_full(x_next.astype(jnp.float32), weights)
    normed, affine, scale_inv = normalize(z_next, gamma, beta)
    y_next = (affine * jax.nn.sigmoid(affine)).astype(jnp.bfloat16)
    x_float = x_cur.astype(jnp.float32)
    z_cur = conv_full(x_float, weights)
    normed, affine, scale_inv = normalize(z_cur, gamma, beta)
    sig = jax.nn.sigmoid(affine)
    grad_a = grad_out.astype(jnp.float32) * (sig * (1.0 + affine * (1.0 - sig)))
    grad_n = grad_a * gamma[None, :, None]
    shape = (z_cur.shape[0], GROUPS, CHANNELS // GROUPS, z_cur.shape[2])
    gn_grouped = grad_n.reshape(shape)
    n_grouped = normed.reshape(shape)
    first_mean = lax.optimization_barrier(jnp.mean(gn_grouped, axis=(0, 2, 3), keepdims=True))
    second_mean = lax.optimization_barrier(jnp.mean(gn_grouped * n_grouped, axis=(0, 2, 3), keepdims=True))
    grad_z = (scale_inv * (gn_grouped - first_mean - n_grouped * second_mean)).reshape(z_cur.shape)
    grad_z = grad_z.astype(jnp.bfloat16).astype(jnp.float32)
    primal, pullback = jax.vjp(conv_full, x_float, weights)
    grad_input, grad_weights = pullback(grad_z)
    return (y_next, grad_input.astype(jnp.bfloat16), grad_weights)

def reference(x_next, x_cur, grad_out, kernel, gamma, beta):
    weights = kernel.astype(jnp.float32)
    y_next, grad_x, per_sample = lax.map(lambda item: one_sample(weights, gamma, beta, item), (x_next, x_cur, grad_out))
    return (y_next, grad_x, lax.optimization_barrier(jnp.sum(per_sample, axis=0)).reshape(-1))
```

```python
import functools
import math

import jax
import jax.numpy as jnp
from jax import lax
from jax.experimental import pallas as pl
from jax.experimental.pallas import tpu as pltpu
from jax.sharding import PartitionSpec as P

GROUPS = 32

eps = 1e-05


LANES = 128
F32 = jnp.float32
BF16 = jnp.bfloat16


def extended(cells, sides, width):
    for axis, dim in sides:
        count = lax.axis_size(axis)
        ends = count - 1
        head = lax.slice_in_dim(cells, 0, width, axis=dim)
        tail = lax.slice_in_dim(cells, cells.shape[dim] - width, cells.shape[dim], axis=dim)
        cells = jnp.concatenate(
            [
                lax.ppermute(tail, axis, [(i, (i + 1) % count) for i in range(ends)]),
                cells,
                lax.ppermute(head, axis, [((i + 1) % count, i) for i in range(ends)]),
            ],
            axis=dim,
        )
    return cells


def conv_rows(padded, kernel, count):
    width = padded.shape[-1]
    wide = jnp.pad(padded, ((0, 0), (0, 0), (0, 0), (1, 1)))
    total = None
    for tap_row in range(3):
        for tap_col in range(3):
            window = wide[:, tap_row : tap_row + count, :, tap_col : tap_col + width]
            term = jnp.einsum(
                "oc,bhcw->bhow",
                kernel[tap_row, tap_col],
                window,
                preferred_element_type=jnp.float32,
            )
            total = term if total is None else total + term
    return total


def group_sum(value):
    batch, rows, chans, width = value.shape
    return jnp.sum(value.reshape(batch, rows, GROUPS, chans // GROUPS, width), axis=(1, 3, 4))


def row_sharded(x_next, x_cur, grad_out, kernel, gamma, beta):
    batch, rows, chans, width = x_next.shape
    height_count = lax.axis_size("height")
    count = height_count * rows * (chans // GROUPS) * width
    gain = gamma[None, None, :, None]
    shift_b = beta[None, None, :, None]

    def expand(stat):
        return jnp.repeat(stat, chans // GROUPS, axis=1)[:, None, :, None]

    stacked = jnp.stack((x_next, x_cur))
    padded = extended(stacked, (("height", 2),), 1)
    xp_next = padded[0]
    xp_cur = padded[1]
    z_next = conv_rows(xp_next, kernel, rows)
    z_cur = conv_rows(xp_cur, kernel, rows)
    sum_next, sum_cur, sq_next, sq_cur = lax.psum(
        (group_sum(z_next), group_sum(z_cur), group_sum(z_next * z_next), group_sum(z_cur * z_cur)),
        "height",
    )
    mean_next = sum_next / count
    mean_cur = sum_cur / count
    var_next = sq_next / count - mean_next * mean_next
    var_cur = sq_cur / count - mean_cur * mean_cur
    rstd_next = lax.rsqrt(var_next + eps)
    rstd_cur = lax.rsqrt(var_cur + eps)
    affine_next = (z_next - expand(mean_next)) * expand(rstd_next) * gain + shift_b
    y_next = (affine_next * jax.nn.sigmoid(affine_next)).astype(jnp.bfloat16)
    normed = (z_cur - expand(mean_cur)) * expand(rstd_cur)
    affine = normed * gain + shift_b
    sig = jax.nn.sigmoid(affine)
    grad_n = grad_out.astype(jnp.float32) * (sig * (1.0 + affine * (1.0 - sig))) * gain
    first_sum, second_sum = lax.psum((group_sum(grad_n), group_sum(grad_n * normed)), "height")
    grad_z = (
        expand(rstd_cur)
        * (grad_n - expand(first_sum / count) - normed * expand(second_sum / count))
    ).astype(jnp.bfloat16)
    grad_pad = extended(grad_z, (("height", 1),), 1)
    grad_own = grad_pad[:, 1:-1]
    grad_wide = jnp.pad(grad_pad, ((0, 0), (0, 0), (0, 0), (1, 1)))
    x_wide = jnp.pad(xp_cur, ((0, 0), (0, 0), (0, 0), (1, 1)))
    grad_input = None
    taps = []
    for tap_row in range(3):
        tap_list = []
        for tap_col in range(3):
            window = grad_wide[
                :, 2 - tap_row : 2 - tap_row + rows, :, 2 - tap_col : 2 - tap_col + width
            ]
            term = jnp.einsum(
                "oc,bhow->bhcw",
                kernel[tap_row, tap_col],
                window,
                preferred_element_type=jnp.float32,
            )
            grad_input = term if grad_input is None else grad_input + term
            source = x_wide[:, tap_row : tap_row + rows, :, tap_col : tap_col + width]
            tap_list.append(
                jnp.einsum("bhow,bhcw->oc", grad_own, source, preferred_element_type=jnp.float32)
            )
        taps.append(jnp.stack(tap_list))
    grad_local = jnp.stack(taps)
    grad_x = grad_input.astype(jnp.bfloat16)
    group_count = lax.axis_size("dp")
    piece = grad_local.size // (height_count * group_count)
    blocks = grad_local.reshape(height_count, group_count, piece)
    shares = lax.psum_scatter(blocks, "dp", scatter_dimension=1, tiled=True)
    grad_kernel = lax.psum_scatter(shares, "height", scatter_dimension=0, tiled=True).reshape(piece)
    return (y_next, grad_x, grad_kernel)


def params(limit=None):
    return pltpu.CompilerParams(vmem_limit_bytes=limit or 40 * 1024 * 1024)


def moved(value, by):
    width = value.shape[-1]
    lane = lax.broadcasted_iota(jnp.int32, value.shape, value.ndim - 1)
    rolled = pltpu.roll(value, by % width, value.ndim - 1)
    keep = lane >= by if by > 0 else lane < width + by
    return jnp.where(keep, rolled, jnp.zeros_like(rolled))


def moved_bf16(value, by):
    return moved(value.astype(F32), by).astype(BF16)


def same_group(chans):
    size = chans // GROUPS
    row = lax.broadcasted_iota(jnp.int32, (chans, chans), 0).astype(F32)
    col = lax.broadcasted_iota(jnp.int32, (chans, chans), 1).astype(F32)
    left = jnp.floor((row + 0.5) * (1.0 / size))
    right = jnp.floor((col + 0.5) * (1.0 / size))
    return jnp.where(left == right, 1.0, 0.0).astype(BF16)


def split3(value):
    high = value.astype(BF16)
    rest = value - high.astype(F32)
    mid = rest.astype(BF16)
    low = (rest - mid.astype(F32)).astype(BF16)
    return high, mid, low


def dot(left, right, dims=((1,), (0,))):
    return lax.dot_general(left, right, (dims, ((), ())), preferred_element_type=F32)


def group_total(same, value):
    column = jnp.sum(value, axis=1, keepdims=True)
    wide = jnp.broadcast_to(column, value.shape)
    high, mid, low = split3(wide)
    return dot(same, high) + (dot(same, mid) + dot(same, low))


def lane_tiles(size):
    return [(at, min(LANES, size - at)) for at in range(0, size, LANES)]


def sigmoid(value):
    return 1.0 / (1.0 + jnp.exp(-value))


def next_conv_kernel(top_ref, x_ref, bottom_ref, w_ref, z_ref, stat_ref, *, rows):
    cells = [top_ref[...]] + [x_ref[r] for r in range(rows)] + [bottom_ref[...]]
    chans, width = cells[0].shape
    total = None
    for b in range(3):
        side = cells if b == 1 else [moved_bf16(cell, 1 - b) for cell in cells]
        for a in range(3):
            right = jnp.concatenate(side[a : a + rows], axis=1)
            term = dot(w_ref[a, b], right)
            total = term if total is None else total + term
    parts = [total[:, r * width : (r + 1) * width] for r in range(rows)]
    for r in range(rows):
        z_ref[r] = parts[r]
    line = functools.reduce(jnp.add, parts)
    mean = jnp.sum(line, axis=1, keepdims=True) * (1.0 / (rows * width))
    off = functools.reduce(jnp.add, [(part - mean) * (part - mean) for part in parts])
    ones = jnp.ones((8, width), BF16)
    lines = []
    for value in (line, off):
        lines.append(sum(dot(ones, part, ((1,), (1,))) for part in split3(value)))
    for j in range(stat_ref.shape[0]):
        stat_ref[j, 0] = lines[0][:1]
        stat_ref[j, 1] = lines[1][:1]


def next_out_kernel(z_ref, stat_ref, gain_ref, shift_ref, y_ref, *, rows, count):
    chans, width = gain_ref.shape
    same = same_group(chans)
    sums = jnp.concatenate([stat_ref[j, 0] for j in range(stat_ref.shape[0])], axis=0)
    offs = jnp.concatenate([stat_ref[j, 1] for j in range(stat_ref.shape[0])], axis=0)
    each = rows * width
    total = jnp.broadcast_to(jnp.sum(sums, axis=0, keepdims=True), (width, chans))
    mean_line = sum(dot(part, same) for part in split3(total[:8])) * (1.0 / count)
    apart = sums * (1.0 / each) - mean_line[:1]
    spread = jnp.sum(offs + apart * apart * float(each), axis=0, keepdims=True)
    spread = jnp.broadcast_to(spread, (width, chans))
    mean = sum(dot(same, part, ((1,), (1,))) for part in split3(total)) * (1.0 / count)
    var = sum(dot(same, part, ((1,), (1,))) for part in split3(spread)) * (1.0 / count)
    rstd = lax.rsqrt(var + eps)
    for r in range(rows):
        affine = (z_ref[r] - mean) * rstd * gain_ref[...] + shift_ref[...]
        y_ref[r] = (affine * sigmoid(affine)).astype(BF16)


def current_kernel(*refs, blocks, rows, groups_dp, span, count):
    x_refs = refs[:blocks]
    g_refs = refs[blocks : 2 * blocks]
    w_ref, gain_ref, shift_ref = refs[2 * blocks : 2 * blocks + 3]
    outs = refs[2 * blocks + 3 : 2 * blocks + 3 + groups_dp]
    gz_out = refs[2 * blocks + 3 + groups_dp]
    xs, z, gn, gzs, coef, taps, flat = refs[2 * blocks + 4 + groups_dp :]
    chans, width = gain_ref.shape
    image = blocks * rows
    home = lax.axis_index("height")
    part = lax.axis_index("dp")
    step = 16

    edge = jnp.zeros((3 * chans, width), BF16)
    xs[0] = edge
    xs[image + 1] = edge
    for k in range(blocks):
        base = (home ^ k) * rows + 1
        for r in range(rows):
            cell = x_refs[k][r]
            xs[base + r, chans : 2 * chans] = cell
            xs[base + r, :chans] = moved_bf16(cell, 1)
            xs[base + r, 2 * chans :] = moved_bf16(cell, -1)

    def conv(p, carry):
        first = p * 2
        total = None
        for a in range(3):
            right = jnp.concatenate([xs[first + a], xs[first + a + 1]], axis=1)
            term = dot(w_ref[a], right)
            total = term if total is None else total + term
        z[first] = total[:, :width]
        z[first + 1] = total[:, width:]
        return carry

    lax.fori_loop(0, image // 2, conv, 0)

    same = same_group(chans)

    def summed(i, carry):
        at = pl.ds(pl.multiple_of(i * step, step), step)
        coef[0, at] = functools.reduce(jnp.add, [z[r, at] for r in range(image)])
        return carry

    lax.fori_loop(0, chans // step, summed, 0)
    coef[1] = group_total(same, coef[0]) * (1.0 / count)

    def squared(i, carry):
        at = pl.ds(pl.multiple_of(i * step, step), step)
        mean = coef[1, at]
        total = None
        for r in range(image):
            off = z[r, at] - mean
            total = off * off if total is None else total + off * off
        coef[0, at] = total
        return carry

    lax.fori_loop(0, chans // step, squared, 0)
    coef[2] = lax.rsqrt(group_total(same, coef[0]) * (1.0 / count) + eps)

    def pulled(i, carry):
        at = pl.ds(pl.multiple_of(i * step, step), step)
        mean = coef[1, at]
        rstd = coef[2, at]
        gain = gain_ref[at]
        shift = shift_ref[at]
        first = None
        second = None
        for k in range(blocks):
            base = (home ^ k) * rows
            for r in range(rows):
                n = (z[base + r, at] - mean) * rstd
                affine = n * gain + shift
                sig = sigmoid(affine)
                slope = sig * (1.0 + affine * (1.0 - sig))
                value = g_refs[k][r, at].astype(F32) * slope * gain
                gn[base + r, at] = value
                z[base + r, at] = n
                first = value if first is None else first + value
                second = value * n if second is None else second + value * n
        coef[3, at] = first
        coef[4, at] = second
        return carry

    lax.fori_loop(0, chans // step, pulled, 0)
    coef[0] = group_total(same, coef[3]) * (1.0 / count)
    coef[1] = group_total(same, coef[4]) * (1.0 / count)

    edge = jnp.zeros((chans, width), BF16)
    for b in range(3):
        gzs[b, 0] = edge
        gzs[b, image + 1] = edge

    def rounded(i, carry):
        at = pl.ds(pl.multiple_of(i * step, step), step)
        mean1 = coef[0, at]
        mean2 = coef[1, at]
        rstd = coef[2, at]
        for r in range(image):
            value = (rstd * (gn[r, at] - mean1 - z[r, at] * mean2)).astype(BF16)
            wide = value.astype(F32)
            gzs[1, r + 1, at] = value
            gzs[0, r + 1, at] = moved(wide, -1).astype(BF16)
            gzs[2, r + 1, at] = moved(wide, 1).astype(BF16)
        return carry

    lax.fori_loop(0, chans // step, rounded, 0)

    for r in range(rows + 2):
        gz_out[r] = gzs[1, home * rows + r]

    block = 9 * chans // blocks
    tap0 = (home * block) // chans
    right = jnp.concatenate([xs[r + 1, chans : 2 * chans] for r in range(image)], axis=1)
    for j in range(span):
        tap = jnp.minimum(tap0 + j, 8)
        a = tap // 3
        b = tap - a * 3
        left = jnp.concatenate([gzs[b, r + 2 - a] for r in range(image)], axis=1)
        rows_of = dot(left, right, ((1,), (1,)))
        for i, (start, size) in enumerate(lane_tiles(chans)):
            taps[i, j * chans : (j + 1) * chans, :size] = rows_of[:, start : start + size]

    off = pl.multiple_of(home * block - tap0 * chans, 8)
    shared = math.gcd(chans, LANES)
    few, many = LANES // shared, chans // shared
    for i in range(taps.shape[0]):
        taps[i, :block] = taps[i, pl.ds(off, block)]
    lines = jnp.concatenate(
        [
            taps[i, pl.ds(line, block // few, stride=few)][:, :size]
            for line in range(few)
            for i, (_, size) in enumerate(lane_tiles(chans))
        ],
        axis=1,
    )
    for i in range(many):
        flat[pl.ds(i, block // few, stride=many)] = lines[:, i * LANES : (i + 1) * LANES]
    piece = flat.shape[0] // groups_dp
    for s in range(groups_dp):
        dest = part ^ s
        value = flat[pl.ds(dest * piece, piece)]
        outs[s][...] = value.astype(outs[s].dtype)


def grad_x_kernel(gz_ref, w_ref, out_ref, *, rows):
    cells = [gz_ref[r] for r in range(rows + 2)]
    width = cells[0].shape[1]
    total = None
    for b in range(3):
        side = cells if b == 1 else [moved_bf16(cell, b - 1) for cell in cells]
        for a in range(3):
            right = jnp.concatenate(side[2 - a : 2 - a + rows], axis=1)
            term = dot(w_ref[a, b], right, ((0,), (0,)))
            total = term if total is None else total + term
    for r in range(rows):
        out_ref[r] = total[:, r * width : (r + 1) * width].astype(BF16)


def vmem(count):
    return [pl.BlockSpec(memory_space=pltpu.VMEM)] * count


def pairs(size, offset):
    return [(i, i ^ offset) for i in range(size)]


def gathered(x_next, x_cur, grad_out, kernel, gamma, beta):
    rows, chans, width = x_next.shape[1:]
    blocks = lax.axis_size("height")
    groups_dp = lax.axis_size("dp")
    image = blocks * rows
    count = image * (chans // GROUPS) * width
    block = 9 * chans // blocks
    span = max((h * block % chans + block - 1) // chans + 1 for h in range(blocks))
    piece = block * chans // (groups_dp * LANES)
    x_next = x_next[0]

    def spread(own):
        held = [None] * blocks
        held[0] = own
        for k in sorted(range(2, blocks, 2), key=lambda k: -bin(k).count("1")):
            held[k] = lax.ppermute(own, "height", pairs(blocks, k))
        for k in range(0, blocks, 2):
            held[k + 1] = lax.ppermute(held[k], "height", pairs(blocks, 1))
        return held

    x_all = spread(x_cur[0])
    g_all = spread(grad_out[0])
    ends = blocks - 1
    top = lax.ppermute(x_next[rows - 1], "height", [(i, i + 1) for i in range(ends)])
    bottom = lax.ppermute(x_next[0], "height", [(i + 1, i) for i in range(ends)])

    gain = jnp.broadcast_to(gamma[:, None], (chans, width))
    shift = jnp.broadcast_to(beta[:, None], (chans, width))
    w_flat = kernel.transpose(0, 2, 1, 3).reshape(3, chans, 3 * chans)

    z_next, stat = pl.pallas_call(
        functools.partial(next_conv_kernel, rows=rows),
        out_shape=(
            jax.ShapeDtypeStruct((rows, chans, width), F32),
            jax.ShapeDtypeStruct((blocks, 2, 1, chans), F32),
        ),
        in_specs=vmem(4),
        out_specs=tuple(vmem(2)),
        compiler_params=params(),
        name="next_conv",
    )(top, x_next, bottom, kernel)
    stats = lax.all_to_all(stat, "height", 0, 0, tiled=True)
    y_next = pl.pallas_call(
        functools.partial(next_out_kernel, rows=rows, count=count),
        out_shape=jax.ShapeDtypeStruct((rows, chans, width), BF16),
        in_specs=vmem(4),
        out_specs=vmem(1)[0],
        compiler_params=params(),
        name="next_out",
    )(z_next, stats, gain, shift)

    results = pl.pallas_call(
        functools.partial(
            current_kernel, blocks=blocks, rows=rows, groups_dp=groups_dp, span=span, count=count
        ),
        out_shape=(jax.ShapeDtypeStruct((piece, LANES), F32),)
        + (jax.ShapeDtypeStruct((piece, LANES), BF16),) * (groups_dp - 1)
        + (jax.ShapeDtypeStruct((rows + 2, chans, width), BF16),),
        in_specs=vmem(2 * blocks + 3),
        out_specs=tuple(vmem(groups_dp + 1)),
        scratch_shapes=[
            pltpu.VMEM((image + 2, 3 * chans, width), BF16),
            pltpu.VMEM((image, chans, width), F32),
            pltpu.VMEM((image, chans, width), F32),
            pltpu.VMEM((3, image + 2, chans, width), BF16),
            pltpu.VMEM((5, chans, width), F32),
            pltpu.VMEM((len(lane_tiles(chans)), span * chans, LANES), F32),
            pltpu.VMEM((groups_dp * piece, LANES), F32),
        ],
        compiler_params=params(),
        name="current",
    )(*x_all, *g_all, w_flat, gain, shift)
    total = results[0]
    for s in range(groups_dp - 1, 0, -1):
        total = total + lax.ppermute(results[s], "dp", pairs(groups_dp, s)).astype(F32)
    grad_x = pl.pallas_call(
        functools.partial(grad_x_kernel, rows=rows),
        out_shape=jax.ShapeDtypeStruct((rows, chans, width), BF16),
        in_specs=vmem(2),
        out_specs=vmem(1)[0],
        compiler_params=params(),
        name="grad_x",
    )(results[groups_dp], kernel)
    return (y_next[None], grad_x[None], total.reshape(piece * LANES))


def fits(shape, blocks, groups_dp):
    batch, rows, chans, width = shape
    image = blocks * rows
    scratch = image * chans * width * 20 + 9 * chans * chans * 4
    few = LANES // math.gcd(chans, LANES)
    return (
        batch == 1
        and width == LANES
        and chans % 16 == 0
        and chans % GROUPS == 0
        and image % 2 == 0
        and blocks & (blocks - 1) == 0
        and groups_dp & (groups_dp - 1) == 0
        and (9 * chans) % (8 * blocks) == 0
        and (9 * chans // blocks) % few == 0
        and (9 * chans // blocks) * chans % (groups_dp * LANES) == 0
        and scratch < 32 * 1024 * 1024
    )


def solution(mesh):
    blocks, groups_dp = mesh.shape["height"], mesh.shape["dp"]

    def local(x_next, x_cur, grad_out, kernel, gamma, beta):
        path = gathered if fits(x_next.shape, blocks, groups_dp) else row_sharded
        return path(x_next, x_cur, grad_out, kernel, gamma, beta)

    placed = (
        P("dp", "height", None, None),
        P("dp", "height", None, None),
        P("dp", "height", None, None),
        P(),
        P(),
        P(),
    )
    return jax.shard_map(
        local,
        mesh=mesh,
        in_specs=placed,
        out_specs=(
            P("dp", "height", None, None),
            P("dp", "height", None, None),
            P(("height", "dp")),
        ),
        check_vma=False,
    )
```

```python
import functools
import math

import jax
import jax.numpy as jnp
from jax import lax
from jax.experimental import pallas as pl
from jax.experimental.pallas import tpu as pltpu
from jax.sharding import PartitionSpec as P

GROUPS = 32

eps = 1e-05


LANES = 128
F32 = jnp.float32
BF16 = jnp.bfloat16


def extended(cells, sides, width):
    for axis, dim in sides:
        count = lax.axis_size(axis)
        ends = count - 1
        head = lax.slice_in_dim(cells, 0, width, axis=dim)
        tail = lax.slice_in_dim(cells, cells.shape[dim] - width, cells.shape[dim], axis=dim)
        cells = jnp.concatenate(
            [
                lax.ppermute(tail, axis, [(i, (i + 1) % count) for i in range(ends)]),
                cells,
                lax.ppermute(head, axis, [((i + 1) % count, i) for i in range(ends)]),
            ],
            axis=dim,
        )
    return cells


def conv_rows(padded, kernel, count):
    width = padded.shape[-1]
    wide = jnp.pad(padded, ((0, 0), (0, 0), (0, 0), (1, 1)))
    total = None
    for tap_row in range(3):
        for tap_col in range(3):
            window = wide[:, tap_row : tap_row + count, :, tap_col : tap_col + width]
            term = jnp.einsum(
                "oc,bhcw->bhow",
                kernel[tap_row, tap_col],
                window,
                preferred_element_type=jnp.float32,
            )
            total = term if total is None else total + term
    return total


def group_sum(value):
    batch, rows, chans, width = value.shape
    return jnp.sum(value.reshape(batch, rows, GROUPS, chans // GROUPS, width), axis=(1, 3, 4))


def row_sharded(x_next, x_cur, grad_out, kernel, gamma, beta):
    batch, rows, chans, width = x_next.shape
    height_count = lax.axis_size("height")
    count = height_count * rows * (chans // GROUPS) * width
    gain = gamma[None, None, :, None]
    shift_b = beta[None, None, :, None]

    def expand(stat):
        return jnp.repeat(stat, chans // GROUPS, axis=1)[:, None, :, None]

    stacked = jnp.stack((x_next, x_cur))
    padded = extended(stacked, (("height", 2),), 1)
    xp_next = padded[0]
    xp_cur = padded[1]
    z_next = conv_rows(xp_next, kernel, rows)
    z_cur = conv_rows(xp_cur, kernel, rows)
    sum_next, sum_cur, sq_next, sq_cur = lax.psum(
        (group_sum(z_next), group_sum(z_cur), group_sum(z_next * z_next), group_sum(z_cur * z_cur)),
        "height",
    )
    mean_next = sum_next / count
    mean_cur = sum_cur / count
    var_next = sq_next / count - mean_next * mean_next
    var_cur = sq_cur / count - mean_cur * mean_cur
    rstd_next = lax.rsqrt(var_next + eps)
    rstd_cur = lax.rsqrt(var_cur + eps)
    affine_next = (z_next - expand(mean_next)) * expand(rstd_next) * gain + shift_b
    y_next = (affine_next * jax.nn.sigmoid(affine_next)).astype(jnp.bfloat16)
    normed = (z_cur - expand(mean_cur)) * expand(rstd_cur)
    affine = normed * gain + shift_b
    sig = jax.nn.sigmoid(affine)
    grad_n = grad_out.astype(jnp.float32) * (sig * (1.0 + affine * (1.0 - sig))) * gain
    first_sum, second_sum = lax.psum((group_sum(grad_n), group_sum(grad_n * normed)), "height")
    grad_z = (
        expand(rstd_cur)
        * (grad_n - expand(first_sum / count) - normed * expand(second_sum / count))
    ).astype(jnp.bfloat16)
    grad_pad = extended(grad_z, (("height", 1),), 1)
    grad_own = grad_pad[:, 1:-1]
    grad_wide = jnp.pad(grad_pad, ((0, 0), (0, 0), (0, 0), (1, 1)))
    x_wide = jnp.pad(xp_cur, ((0, 0), (0, 0), (0, 0), (1, 1)))
    grad_input = None
    taps = []
    for tap_row in range(3):
        tap_list = []
        for tap_col in range(3):
            window = grad_wide[
                :, 2 - tap_row : 2 - tap_row + rows, :, 2 - tap_col : 2 - tap_col + width
            ]
            term = jnp.einsum(
                "oc,bhow->bhcw",
                kernel[tap_row, tap_col],
                window,
                preferred_element_type=jnp.float32,
            )
            grad_input = term if grad_input is None else grad_input + term
            source = x_wide[:, tap_row : tap_row + rows, :, tap_col : tap_col + width]
            tap_list.append(
                jnp.einsum("bhow,bhcw->oc", grad_own, source, preferred_element_type=jnp.float32)
            )
        taps.append(jnp.stack(tap_list))
    grad_local = jnp.stack(taps)
    grad_x = grad_input.astype(jnp.bfloat16)
    group_count = lax.axis_size("dp")
    piece = grad_local.size // (height_count * group_count)
    blocks = grad_local.reshape(height_count, group_count, piece)
    shares = lax.psum_scatter(blocks, "dp", scatter_dimension=1, tiled=True)
    grad_kernel = lax.psum_scatter(shares, "height", scatter_dimension=0, tiled=True).reshape(piece)
    return (y_next, grad_x, grad_kernel)


def params(limit=None):
    return pltpu.CompilerParams(vmem_limit_bytes=limit or 40 * 1024 * 1024)


def moved(value, by):
    width = value.shape[-1]
    lane = lax.broadcasted_iota(jnp.int32, value.shape, value.ndim - 1)
    rolled = pltpu.roll(value, by % width, value.ndim - 1)
    keep = lane >= by if by > 0 else lane < width + by
    return jnp.where(keep, rolled, jnp.zeros_like(rolled))


def moved_bf16(value, by):
    return moved(value.astype(F32), by).astype(BF16)


def same_group(chans):
    size = chans // GROUPS
    row = lax.broadcasted_iota(jnp.int32, (chans, chans), 0).astype(F32)
    col = lax.broadcasted_iota(jnp.int32, (chans, chans), 1).astype(F32)
    left = jnp.floor((row + 0.5) * (1.0 / size))
    right = jnp.floor((col + 0.5) * (1.0 / size))
    return jnp.where(left == right, 1.0, 0.0).astype(BF16)


def split3(value):
    high = value.astype(BF16)
    rest = value - high.astype(F32)
    mid = rest.astype(BF16)
    low = (rest - mid.astype(F32)).astype(BF16)
    return high, mid, low


def dot(left, right, dims=((1,), (0,))):
    return lax.dot_general(left, right, (dims, ((), ())), preferred_element_type=F32)


def group_total(same, value):
    column = jnp.sum(value, axis=1, keepdims=True)
    wide = jnp.broadcast_to(column, value.shape)
    high, mid, low = split3(wide)
    return dot(same, high) + (dot(same, mid) + dot(same, low))


def lane_tiles(size):
    return [(at, min(LANES, size - at)) for at in range(0, size, LANES)]


def sigmoid(value):
    return 1.0 / (1.0 + jnp.exp(-value))


def next_conv_kernel(
    top_ref, x_ref, bottom_ref, w_ref, g_ref, z_ref, sent_ref, flat_ref, *, rows
):
    cells = [top_ref[...]] + [x_ref[r] for r in range(rows)] + [bottom_ref[...]]
    chans, width = cells[0].shape
    total = None
    for b in range(3):
        side = cells if b == 1 else [moved_bf16(cell, 1 - b) for cell in cells]
        for a in range(3):
            right = jnp.concatenate(side[a : a + rows], axis=1)
            term = dot(w_ref[a, b], right)
            total = term if total is None else total + term
    parts = [total[:, r * width : (r + 1) * width] for r in range(rows)]
    for r in range(rows):
        z_ref[r] = parts[r]
        sent_ref[r * chans : (r + 1) * chans] = g_ref[r]
    line = functools.reduce(jnp.add, parts)
    mean = jnp.sum(line, axis=1, keepdims=True) * (1.0 / (rows * width))
    off = functools.reduce(jnp.add, [(part - mean) * (part - mean) for part in parts])
    ones = jnp.ones((8, width), BF16)
    tail = sent_ref.shape[0] - rows * chans
    row = lax.broadcasted_iota(jnp.int32, (tail, LANES), 0)
    packed = jnp.zeros((tail, LANES), F32)
    at = 0
    for value in (line, off):
        lane_sum = sum(dot(ones, part, ((1,), (1,))) for part in split3(value))
        for term in split3(lane_sum):
            term = term.astype(F32)
            for start, size in lane_tiles(chans):
                piece = term[:1, start : start + size]
                if size < LANES:
                    piece = jnp.concatenate([piece, jnp.zeros((1, LANES - size), F32)], axis=1)
                packed = jnp.where(row == at, jnp.broadcast_to(piece, packed.shape), packed)
                at += 1
    sent_ref[rows * chans :] = packed.astype(BF16)
    for a in range(3):
        for b in range(3):
            flat_ref[a, :, b * chans : (b + 1) * chans] = w_ref[a, b]


def next_out_kernel(z_ref, stat_ref, gain_ref, shift_ref, y_ref, *, rows, count):
    chans, width = gain_ref.shape
    same = same_group(chans)
    tiles = lane_tiles(chans)

    def line(j, value):
        at = value * 3 * len(tiles)
        total = None
        for term in range(3):
            cells = [
                stat_ref[j, at + term * len(tiles) + i : at + term * len(tiles) + i + 1, :size]
                for i, (_, size) in enumerate(tiles)
            ]
            term_line = jnp.concatenate(cells, axis=1)
            total = term_line if total is None else total + term_line
        return total

    sums = jnp.concatenate([line(j, 0) for j in range(stat_ref.shape[0])], axis=0)
    offs = jnp.concatenate([line(j, 1) for j in range(stat_ref.shape[0])], axis=0)
    each = rows * width
    total = jnp.broadcast_to(jnp.sum(sums, axis=0, keepdims=True), (width, chans))
    mean_line = sum(dot(part, same) for part in split3(total[:8])) * (1.0 / count)
    apart = sums * (1.0 / each) - mean_line[:1]
    spread = jnp.sum(offs + apart * apart * float(each), axis=0, keepdims=True)
    spread = jnp.broadcast_to(spread, (width, chans))
    mean = sum(dot(same, part, ((1,), (1,))) for part in split3(total)) * (1.0 / count)
    var = sum(dot(same, part, ((1,), (1,))) for part in split3(spread)) * (1.0 / count)
    rstd = lax.rsqrt(var + eps)
    for r in range(rows):
        affine = (z_ref[r] - mean) * rstd * gain_ref[...] + shift_ref[...]
        y_ref[r] = (affine * sigmoid(affine)).astype(BF16)


def conv_pairs(xs, w_ref, z, total_ref, first, last, base):
    width = z.shape[2]

    def conv(p, carry):
        row = p * 2
        total = None
        for a in range(3):
            right = jnp.concatenate([xs[row + a], xs[row + a + 1]], axis=1)
            term = dot(w_ref[a], right)
            total = term if total is None else total + term
        z[row - base] = total[:, :width]
        z[row - base + 1] = total[:, width:]
        total_ref[...] += total[:, :width] + total[:, width:]
        return carry

    lax.fori_loop(first, last, conv, 0)


def conv_first_kernel(*refs, blocks, rows, split):
    x_refs = refs[:blocks]
    w_ref, xs, z, total_ref = refs[blocks:]
    chans, width = total_ref.shape
    image = blocks * rows
    home = lax.axis_index("height")

    edge = jnp.zeros((3 * chans, width), BF16)
    xs[0] = edge
    xs[image + 1] = edge
    for k in range(blocks):
        base = (home ^ k) * rows + 1
        for r in range(rows):
            cell = x_refs[k][r]
            xs[base + r, chans : 2 * chans] = cell
            xs[base + r, :chans] = moved_bf16(cell, 1)
            xs[base + r, 2 * chans :] = moved_bf16(cell, -1)
    total_ref[...] = jnp.zeros((chans, width), F32)
    conv_pairs(xs, w_ref, z, total_ref, 0, split, 0)


def conv_second_kernel(xs, w_ref, z_first, before, z, norm, total_ref, *, split, count):
    head, chans, width = z_first.shape
    image = head + z.shape[0]
    step = 16
    total_ref[...] = before[...]
    conv_pairs(xs, w_ref, z, total_ref, split, image // 2, head)
    same = same_group(chans)
    norm[0] = group_total(same, total_ref[...]) * (1.0 / count)

    def squared(i, carry):
        at = pl.ds(pl.multiple_of(i * step, step), step)
        mean = norm[0, at]
        total = None
        for r in range(image):
            off = (z_first[r, at] if r < head else z[r - head, at]) - mean
            total = off * off if total is None else total + off * off
        total_ref[at] = total
        return carry

    lax.fori_loop(0, chans // step, squared, 0)
    norm[1] = lax.rsqrt(group_total(same, total_ref[...]) * (1.0 / count) + eps)


def current_grad_kernel(*refs, blocks, rows, groups_dp, span, count):
    g_refs = refs[:blocks]
    xs, z_first, z_second, norm, gain_ref, shift_ref = refs[blocks : blocks + 6]
    outs = refs[blocks + 6 : blocks + 6 + groups_dp]
    gz_out, stat_out = refs[blocks + 6 + groups_dp : blocks + 8 + groups_dp]
    grads, gn, ns, gz, coef, taps, flat = refs[blocks + 8 + groups_dp :]
    head, chans, width = z_first.shape
    image = head + z_second.shape[0]
    home = lax.axis_index("height")
    part = lax.axis_index("dp")
    step = 16

    for k in range(blocks):
        base = (home ^ k) * rows
        for r in range(rows):
            grads[base + r] = g_refs[k][r * chans : (r + 1) * chans]
        stat_out[k] = g_refs[k][rows * chans :].astype(F32)

    def pulled(i, carry):
        at = pl.ds(pl.multiple_of(i * step, step), step)
        mean = norm[0, at]
        rstd = norm[1, at]
        gain = gain_ref[at]
        shift = shift_ref[at]
        first = None
        second = None
        for r in range(image):
            n = ((z_first[r, at] if r < head else z_second[r - head, at]) - mean) * rstd
            affine = n * gain + shift
            sig = sigmoid(affine)
            slope = sig * (1.0 + affine * (1.0 - sig))
            value = grads[r, at].astype(F32) * slope * gain
            gn[r, at] = value
            ns[r, at] = n
            first = value if first is None else first + value
            second = value * n if second is None else second + value * n
        coef[0, at] = first
        coef[1, at] = second
        return carry

    lax.fori_loop(0, chans // step, pulled, 0)
    same = same_group(chans)
    coef[0] = group_total(same, coef[0]) * (1.0 / count)
    coef[1] = group_total(same, coef[1]) * (1.0 / count)

    edge = jnp.zeros((chans, width), BF16)
    gz[0] = edge
    gz[image + 1] = edge

    def rounded(i, carry):
        at = pl.ds(pl.multiple_of(i * step, step), step)
        mean1 = coef[0, at]
        mean2 = coef[1, at]
        rstd = norm[1, at]
        for r in range(image):
            gz[r + 1, at] = (rstd * (gn[r, at] - mean1 - ns[r, at] * mean2)).astype(BF16)
        return carry

    lax.fori_loop(0, chans // step, rounded, 0)

    for r in range(rows + 2):
        gz_out[r] = gz[home * rows + r]

    block = 9 * chans // blocks
    tap0 = (home * block) // chans
    left = jnp.concatenate([gz[r + 1] for r in range(image)], axis=1)
    for j in range(span):
        tap = jnp.minimum(tap0 + j, 8)
        a = tap // 3
        side = pl.ds(pl.multiple_of((tap - a * 3) * chans, step), chans)
        right = jnp.concatenate([xs[r + a, side] for r in range(image)], axis=1)
        rows_of = dot(left, right, ((1,), (1,)))
        for i, (start, size) in enumerate(lane_tiles(chans)):
            taps[i, j * chans : (j + 1) * chans, :size] = rows_of[:, start : start + size]

    off = pl.multiple_of(home * block - tap0 * chans, 8)
    shared = math.gcd(chans, LANES)
    few, many = LANES // shared, chans // shared
    for i in range(taps.shape[0]):
        taps[i, :block] = taps[i, pl.ds(off, block)]
    lines = jnp.concatenate(
        [
            taps[i, pl.ds(line, block // few, stride=few)][:, :size]
            for line in range(few)
            for i, (_, size) in enumerate(lane_tiles(chans))
        ],
        axis=1,
    )
    for i in range(many):
        flat[pl.ds(i, block // few, stride=many)] = lines[:, i * LANES : (i + 1) * LANES]
    piece = flat.shape[0] // groups_dp
    for s in range(groups_dp):
        dest = part ^ s
        value = flat[pl.ds(dest * piece, piece)]
        outs[s][...] = value.astype(outs[s].dtype)


def grad_x_kernel(gz_ref, w_ref, out_ref, *, rows):
    cells = [gz_ref[r] for r in range(rows + 2)]
    width = cells[0].shape[1]
    total = None
    for b in range(3):
        side = cells if b == 1 else [moved_bf16(cell, b - 1) for cell in cells]
        for a in range(3):
            right = jnp.concatenate(side[2 - a : 2 - a + rows], axis=1)
            term = dot(w_ref[a, b], right, ((0,), (0,)))
            total = term if total is None else total + term
    for r in range(rows):
        out_ref[r] = total[:, r * width : (r + 1) * width].astype(BF16)


def vmem(count):
    return [pl.BlockSpec(memory_space=pltpu.VMEM)] * count


def pairs(size, offset):
    return [(i, i ^ offset) for i in range(size)]


def gathered(x_next, x_cur, grad_out, kernel, gamma, beta):
    rows, chans, width = x_next.shape[1:]
    blocks = lax.axis_size("height")
    groups_dp = lax.axis_size("dp")
    image = blocks * rows
    count = image * (chans // GROUPS) * width
    block = 9 * chans // blocks
    span = max((h * block % chans + block - 1) // chans + 1 for h in range(blocks))
    piece = block * chans // (groups_dp * LANES)
    x_next = x_next[0]

    def far(own):
        held = {0: own}
        for k in sorted(range(2, blocks, 2), key=lambda k: -bin(k).count("1")):
            held[k] = lax.ppermute(own, "height", pairs(blocks, k))
        return held

    def near(held):
        result = [None] * blocks
        for k in range(0, blocks, 2):
            result[k] = held[k]
            result[k + 1] = lax.ppermute(held[k], "height", pairs(blocks, 1))
        return result

    tail = -(-6 * len(lane_tiles(chans)) // 16) * 16
    x_far = far(x_cur[0])
    ends = blocks - 1
    top = lax.ppermute(x_next[rows - 1], "height", [(i, i + 1) for i in range(ends)])
    bottom = lax.ppermute(x_next[0], "height", [(i + 1, i) for i in range(ends)])

    gain = jnp.broadcast_to(gamma[:, None], (chans, width))
    shift = jnp.broadcast_to(beta[:, None], (chans, width))
    flops = 18 * chans * chans * width

    z_next, sent, w_flat = pl.pallas_call(
        functools.partial(next_conv_kernel, rows=rows),
        out_shape=(
            jax.ShapeDtypeStruct((rows, chans, width), F32),
            jax.ShapeDtypeStruct((rows * chans + tail, width), BF16),
            jax.ShapeDtypeStruct((3, chans, 3 * chans), BF16),
        ),
        in_specs=vmem(5),
        out_specs=tuple(vmem(3)),
        compiler_params=params(),
        cost_estimate=pl.CostEstimate(flops=rows * flops, bytes_accessed=0, transcendentals=0),
        name="next_conv",
    )(top, x_next, bottom, kernel, grad_out[0])
    g_far = far(sent)
    x_far, z_next = lax.optimization_barrier((x_far, z_next))
    x_all = near(x_far)
    split = -(-5 * image // 16)
    xs, z_first, partial = pl.pallas_call(
        functools.partial(conv_first_kernel, blocks=blocks, rows=rows, split=split),
        out_shape=(
            jax.ShapeDtypeStruct((image + 2, 3 * chans, width), BF16),
            jax.ShapeDtypeStruct((2 * split, chans, width), F32),
            jax.ShapeDtypeStruct((chans, width), F32),
        ),
        in_specs=vmem(blocks + 1),
        out_specs=tuple(vmem(3)),
        compiler_params=params(),
        cost_estimate=pl.CostEstimate(flops=image * flops, bytes_accessed=0, transcendentals=0),
        name="conv_first",
    )(*x_all, w_flat)
    g_far, partial = lax.optimization_barrier((g_far, partial))
    g_all = near(g_far)
    z_second, norm = pl.pallas_call(
        functools.partial(conv_second_kernel, split=split, count=count),
        out_shape=(
            jax.ShapeDtypeStruct((image - 2 * split, chans, width), F32),
            jax.ShapeDtypeStruct((2, chans, width), F32),
        ),
        in_specs=vmem(4),
        out_specs=tuple(vmem(2)),
        scratch_shapes=[pltpu.VMEM((chans, width), F32)],
        compiler_params=params(),
        cost_estimate=pl.CostEstimate(flops=image * flops, bytes_accessed=0, transcendentals=0),
        name="conv_second",
    )(xs, w_flat, z_first, partial)
    results = pl.pallas_call(
        functools.partial(
            current_grad_kernel,
            blocks=blocks,
            rows=rows,
            groups_dp=groups_dp,
            span=span,
            count=count,
        ),
        out_shape=(jax.ShapeDtypeStruct((piece, LANES), F32),)
        + (jax.ShapeDtypeStruct((piece, LANES), BF16),) * (groups_dp - 1)
        + (
            jax.ShapeDtypeStruct((rows + 2, chans, width), BF16),
            jax.ShapeDtypeStruct((blocks, tail, width), F32),
        ),
        in_specs=vmem(blocks + 6),
        out_specs=tuple(vmem(groups_dp + 2)),
        scratch_shapes=[
            pltpu.VMEM((image, chans, width), BF16),
            pltpu.VMEM((image, chans, width), F32),
            pltpu.VMEM((image, chans, width), F32),
            pltpu.VMEM((image + 2, chans, width), BF16),
            pltpu.VMEM((2, chans, width), F32),
            pltpu.VMEM((len(lane_tiles(chans)), span * chans, LANES), F32),
            pltpu.VMEM((groups_dp * piece, LANES), F32),
        ],
        compiler_params=params(),
        cost_estimate=pl.CostEstimate(flops=image * flops, bytes_accessed=0, transcendentals=0),
        name="current_grad",
    )(*g_all, xs, z_first, z_second, norm, gain, shift)
    total = results[0]
    for s in range(groups_dp - 1, 0, -1):
        total = total + lax.ppermute(results[s], "dp", pairs(groups_dp, s)).astype(F32)
    grad_x = pl.pallas_call(
        functools.partial(grad_x_kernel, rows=rows),
        out_shape=jax.ShapeDtypeStruct((rows, chans, width), BF16),
        in_specs=vmem(2),
        out_specs=vmem(1)[0],
        compiler_params=params(),
        name="grad_x",
    )(results[groups_dp], kernel)
    y_next = pl.pallas_call(
        functools.partial(next_out_kernel, rows=rows, count=count),
        out_shape=jax.ShapeDtypeStruct((rows, chans, width), BF16),
        in_specs=vmem(4),
        out_specs=vmem(1)[0],
        compiler_params=params(),
        name="next_out",
    )(z_next, results[groups_dp + 1], gain, shift)
    return (y_next[None], grad_x[None], total.reshape(piece * LANES))


def fits(shape, blocks, groups_dp):
    batch, rows, chans, width = shape
    image = blocks * rows
    scratch = image * chans * width * 20 + 9 * chans * chans * 4
    few = LANES // math.gcd(chans, LANES)
    return (
        batch == 1
        and width == LANES
        and chans % 16 == 0
        and chans % GROUPS == 0
        and image % 2 == 0
        and blocks & (blocks - 1) == 0
        and groups_dp & (groups_dp - 1) == 0
        and (9 * chans) % (8 * blocks) == 0
        and (9 * chans // blocks) % few == 0
        and (9 * chans // blocks) * chans % (groups_dp * LANES) == 0
        and scratch < 32 * 1024 * 1024
    )


def solution(mesh):
    blocks, groups_dp = mesh.shape["height"], mesh.shape["dp"]

    def local(x_next, x_cur, grad_out, kernel, gamma, beta):
        path = gathered if fits(x_next.shape, blocks, groups_dp) else row_sharded
        return path(x_next, x_cur, grad_out, kernel, gamma, beta)

    placed = (
        P("dp", "height", None, None),
        P("dp", "height", None, None),
        P("dp", "height", None, None),
        P(),
        P(),
        P(),
    )
    return jax.shard_map(
        local,
        mesh=mesh,
        in_specs=placed,
        out_specs=(
            P("dp", "height", None, None),
            P("dp", "height", None, None),
            P(("height", "dp")),
        ),
        check_vma=False,
    )
```

```python
import functools
import math

import jax
import jax.numpy as jnp
from jax import lax
from jax.experimental import pallas as pl
from jax.experimental.pallas import tpu as pltpu
from jax.sharding import PartitionSpec as P

GROUPS = 32

eps = 1e-05


LANES = 128
F32 = jnp.float32
BF16 = jnp.bfloat16


def extended(cells, sides, width):
    for axis, dim in sides:
        count = lax.axis_size(axis)
        ends = count - 1
        head = lax.slice_in_dim(cells, 0, width, axis=dim)
        tail = lax.slice_in_dim(cells, cells.shape[dim] - width, cells.shape[dim], axis=dim)
        cells = jnp.concatenate(
            [
                lax.ppermute(tail, axis, [(i, (i + 1) % count) for i in range(ends)]),
                cells,
                lax.ppermute(head, axis, [((i + 1) % count, i) for i in range(ends)]),
            ],
            axis=dim,
        )
    return cells


def conv_rows(padded, kernel, count):
    width = padded.shape[-1]
    wide = jnp.pad(padded, ((0, 0), (0, 0), (0, 0), (1, 1)))
    total = None
    for tap_row in range(3):
        for tap_col in range(3):
            window = wide[:, tap_row : tap_row + count, :, tap_col : tap_col + width]
            term = jnp.einsum(
                "oc,bhcw->bhow",
                kernel[tap_row, tap_col],
                window,
                preferred_element_type=jnp.float32,
            )
            total = term if total is None else total + term
    return total


def group_sum(value):
    batch, rows, chans, width = value.shape
    return jnp.sum(value.reshape(batch, rows, GROUPS, chans // GROUPS, width), axis=(1, 3, 4))


def row_sharded(x_next, x_cur, grad_out, kernel, gamma, beta):
    _, rows, chans, width = x_next.shape
    height_count = lax.axis_size("height")
    count = height_count * rows * (chans // GROUPS) * width
    gain = gamma[None, None, :, None]
    shift_b = beta[None, None, :, None]

    def expand(stat):
        return jnp.repeat(stat, chans // GROUPS, axis=1)[:, None, :, None]

    stacked = jnp.stack((x_next, x_cur))
    padded = extended(stacked, (("height", 2),), 1)
    xp_next = padded[0]
    xp_cur = padded[1]
    z_next = conv_rows(xp_next, kernel, rows)
    z_cur = conv_rows(xp_cur, kernel, rows)
    sum_next, sum_cur, sq_next, sq_cur = lax.psum(
        (group_sum(z_next), group_sum(z_cur), group_sum(z_next * z_next), group_sum(z_cur * z_cur)),
        "height",
    )
    mean_next = sum_next / count
    mean_cur = sum_cur / count
    var_next = sq_next / count - mean_next * mean_next
    var_cur = sq_cur / count - mean_cur * mean_cur
    rstd_next = lax.rsqrt(var_next + eps)
    rstd_cur = lax.rsqrt(var_cur + eps)
    affine_next = (z_next - expand(mean_next)) * expand(rstd_next) * gain + shift_b
    y_next = (affine_next * jax.nn.sigmoid(affine_next)).astype(jnp.bfloat16)
    normed = (z_cur - expand(mean_cur)) * expand(rstd_cur)
    affine = normed * gain + shift_b
    sig = jax.nn.sigmoid(affine)
    grad_n = grad_out.astype(jnp.float32) * (sig * (1.0 + affine * (1.0 - sig))) * gain
    first_sum, second_sum = lax.psum((group_sum(grad_n), group_sum(grad_n * normed)), "height")
    grad_z = (
        expand(rstd_cur)
        * (grad_n - expand(first_sum / count) - normed * expand(second_sum / count))
    ).astype(jnp.bfloat16)
    grad_pad = extended(grad_z, (("height", 1),), 1)
    grad_own = grad_pad[:, 1:-1]
    grad_wide = jnp.pad(grad_pad, ((0, 0), (0, 0), (0, 0), (1, 1)))
    x_wide = jnp.pad(xp_cur, ((0, 0), (0, 0), (0, 0), (1, 1)))
    grad_input = None
    taps = []
    for tap_row in range(3):
        tap_list = []
        for tap_col in range(3):
            window = grad_wide[
                :, 2 - tap_row : 2 - tap_row + rows, :, 2 - tap_col : 2 - tap_col + width
            ]
            term = jnp.einsum(
                "oc,bhow->bhcw",
                kernel[tap_row, tap_col],
                window,
                preferred_element_type=jnp.float32,
            )
            grad_input = term if grad_input is None else grad_input + term
            source = x_wide[:, tap_row : tap_row + rows, :, tap_col : tap_col + width]
            tap_list.append(
                jnp.einsum("bhow,bhcw->oc", grad_own, source, preferred_element_type=jnp.float32)
            )
        taps.append(jnp.stack(tap_list))
    grad_local = jnp.stack(taps)
    grad_x = grad_input.astype(jnp.bfloat16)
    group_count = lax.axis_size("dp")
    piece = grad_local.size // (height_count * group_count)
    blocks = grad_local.reshape(height_count, group_count, piece)
    shares = lax.psum_scatter(blocks, "dp", scatter_dimension=1, tiled=True)
    grad_kernel = lax.psum_scatter(shares, "height", scatter_dimension=0, tiled=True).reshape(piece)
    return (y_next, grad_x, grad_kernel)


def params(limit=None):
    return pltpu.CompilerParams(vmem_limit_bytes=limit or 40 * 1024 * 1024)


def moved(value, by):
    width = value.shape[-1]
    lane = lax.broadcasted_iota(jnp.int32, value.shape, value.ndim - 1)
    rolled = pltpu.roll(value, by % width, value.ndim - 1)
    keep = lane >= by if by > 0 else lane < width + by
    return jnp.where(keep, rolled, jnp.zeros_like(rolled))


def moved_bf16(value, by):
    return moved(value.astype(F32), by).astype(BF16)


def same_group(rows, chans):
    size = chans // GROUPS
    row = lax.broadcasted_iota(jnp.int32, (rows, rows), 0).astype(F32)
    col = lax.broadcasted_iota(jnp.int32, (rows, rows), 1).astype(F32)
    left = jnp.floor((row + 0.5) * (1.0 / size))
    right = jnp.floor((col + 0.5) * (1.0 / size))
    return jnp.where(left == right, 1.0, 0.0).astype(BF16)


def split3(value):
    high = value.astype(BF16)
    rest = value - high.astype(F32)
    mid = rest.astype(BF16)
    low = (rest - mid.astype(F32)).astype(BF16)
    return high, mid, low


def dot(left, right, dims=((1,), (0,))):
    return lax.dot_general(left, right, (dims, ((), ())), preferred_element_type=F32)


def group_total(same, value):
    column = jnp.sum(value, axis=1, keepdims=True)
    wide = jnp.broadcast_to(column, value.shape)
    high, mid, low = split3(wide)
    return dot(same, high) + (dot(same, mid) + dot(same, low))


def lane_tiles(size):
    return [(at, min(LANES, size - at)) for at in range(0, size, LANES)]


def sigmoid(value):
    return 1.0 / (1.0 + jnp.exp(-value))


def weights_kernel(w_ref, flat_ref):
    chans = flat_ref.shape[1]
    for a in range(3):
        for b in range(3):
            flat_ref[a, :, b * chans : (b + 1) * chans] = w_ref[a, b]


def halves_kernel(g_ref, own_ref, other_ref):
    half = own_ref.shape[1]
    core = lax.axis_index("height") & 1
    for r in range(own_ref.shape[0]):
        own_ref[r] = g_ref[r, pl.ds(pl.multiple_of(core * half, 16), half)]
        other_ref[r] = g_ref[r, pl.ds(pl.multiple_of((1 - core) * half, 16), half)]


def next_conv_kernel(top_ref, x_ref, bottom_ref, w_ref, z_ref, stat_ref, *, rows):
    cells = [top_ref[...]] + [x_ref[r] for r in range(rows)] + [bottom_ref[...]]
    chans, width = cells[0].shape
    sides = [[moved_bf16(cell, 1) for cell in cells], cells, [moved_bf16(cell, -1) for cell in cells]]
    stacks = [jnp.concatenate([side[r] for side in sides], axis=0) for r in range(rows + 2)]
    total = None
    for a in range(3):
        term = dot(w_ref[a], jnp.concatenate(stacks[a : a + rows], axis=1))
        total = term if total is None else total + term
    parts = [total[:, r * width : (r + 1) * width] for r in range(rows)]
    for r in range(rows):
        z_ref[r] = parts[r]
    line = functools.reduce(jnp.add, parts)
    mean = jnp.sum(line, axis=1, keepdims=True) * (1.0 / (rows * width))
    off = functools.reduce(jnp.add, [(part - mean) * (part - mean) for part in parts])
    ones = jnp.ones((8, width), BF16)
    row = lax.broadcasted_iota(jnp.int32, stat_ref.shape, 0)
    packed = jnp.zeros(stat_ref.shape, F32)
    at = 0
    for value in (line, off):
        lane_sum = sum(dot(ones, part, ((1,), (1,))) for part in split3(value))
        for start, size in lane_tiles(chans):
            piece = lane_sum[:1, start : start + size]
            if size < LANES:
                piece = jnp.concatenate([piece, jnp.zeros((1, LANES - size), F32)], axis=1)
            packed = jnp.where(row == at, jnp.broadcast_to(piece, packed.shape), packed)
            at += 1
    stat_ref[...] = packed


def next_out_kernel(*refs, rows, count):
    stat_refs = refs[:-4]
    z_ref, gain_ref, shift_ref, y_ref = refs[-4:]
    chans, width = gain_ref.shape
    same = same_group(chans, chans)
    tiles = lane_tiles(chans)

    def line(value):
        at = value * len(tiles)
        cells = [
            jnp.concatenate([ref[j, at + i : at + i + 1, :size] for i, (_, size) in enumerate(tiles)], axis=1)
            for ref in stat_refs
            for j in range(ref.shape[0])
        ]
        return jnp.concatenate(cells, axis=0)

    sums = line(0)
    offs = line(1)
    each = rows * width
    total = jnp.broadcast_to(jnp.sum(sums, axis=0, keepdims=True), (width, chans))
    mean_line = sum(dot(part, same) for part in split3(total[:8])) * (1.0 / count)
    apart = sums * (1.0 / each) - mean_line[:1]
    spread = jnp.sum(offs + apart * apart * float(each), axis=0, keepdims=True)
    spread = jnp.broadcast_to(spread, (width, chans))
    mean = sum(dot(same, part, ((1,), (1,))) for part in split3(total)) * (1.0 / count)
    var = sum(dot(same, part, ((1,), (1,))) for part in split3(spread)) * (1.0 / count)
    rstd = lax.rsqrt(var + eps)
    for r in range(rows):
        affine = (z_ref[r] - mean) * rstd * gain_ref[...] + shift_ref[...]
        y_ref[r] = (affine * sigmoid(affine)).astype(BF16)


def conv_kernel(*refs, blocks, rows, count, wide):
    x_refs = refs[:blocks]
    w_ref, xs, z, norm, total_ref = refs[blocks:]
    image, half, width = z.shape
    chans = x_refs[0].shape[1]
    home = lax.axis_index("height")
    mine = pl.ds(pl.multiple_of((home & 1) * half, 16), half)
    step = 16

    edge = jnp.zeros((3 * chans, width), BF16)
    xs[0] = edge
    xs[image + 1] = edge
    for k in range(blocks):
        base = (home ^ k) * rows + 1
        for r in range(rows):
            cell = x_refs[k][r]
            xs[base + r, chans : 2 * chans] = cell
            xs[base + r, :chans] = moved_bf16(cell, 1)
            xs[base + r, 2 * chans :] = moved_bf16(cell, -1)

    def conv(p, carry):
        row = p * wide
        total = None
        for a in range(3):
            right = jnp.concatenate([xs[row + a + i] for i in range(wide)], axis=1)
            term = dot(w_ref[a, mine], right)
            total = term if total is None else total + term
        parts = [total[:, i * width : (i + 1) * width] for i in range(wide)]
        for i in range(wide):
            z[row + i] = parts[i]
        return carry

    lax.fori_loop(0, image // wide, conv, 0)
    same = same_group(half, chans)

    def summed(i, carry):
        at = pl.ds(pl.multiple_of(i * step, step), step)
        total_ref[at] = functools.reduce(jnp.add, [z[r, at] for r in range(image)])
        return carry

    lax.fori_loop(0, half // step, summed, 0)
    norm[0] = group_total(same, total_ref[...]) * (1.0 / count)

    def squared(i, carry):
        at = pl.ds(pl.multiple_of(i * step, step), step)
        mean = norm[0, at]
        total = None
        for r in range(image):
            off = z[r, at] - mean
            total = off * off if total is None else total + off * off
        total_ref[at] = total
        return carry

    lax.fori_loop(0, half // step, squared, 0)
    norm[1] = lax.rsqrt(group_total(same, total_ref[...]) * (1.0 / count) + eps)


def pull_kernel(*refs, blocks, rows, count):
    g_refs = refs[: blocks // 2]
    z, norm, gain_ref, shift_ref, gz_ref, gn, ns, coef = refs[blocks // 2 :]
    image, half, _ = z.shape
    chans = gain_ref.shape[0]
    home = lax.axis_index("height")
    core = home & 1
    step = 16

    def pulled(i, carry):
        start = pl.multiple_of(i * step, step)
        at = pl.ds(start, step)
        all_at = pl.ds(pl.multiple_of(core * half + start, step), step)
        mean = norm[0, at]
        rstd = norm[1, at]
        gain = gain_ref[all_at]
        shift = shift_ref[all_at]
        first = None
        second = None
        for k in range(blocks):
            base = (home ^ k) * rows
            for r in range(rows):
                n = (z[base + r, at] - mean) * rstd
                affine = n * gain + shift
                sig = sigmoid(affine)
                slope = sig * (1.0 + affine * (1.0 - sig))
                value = g_refs[k // 2][k % 2, r, at].astype(F32) * slope * gain
                gn[base + r, at] = value
                ns[base + r, at] = n
                first = value if first is None else first + value
                second = value * n if second is None else second + value * n
        coef[0, at] = first
        coef[1, at] = second
        return carry

    lax.fori_loop(0, half // step, pulled, 0)
    same = same_group(half, chans)
    coef[0] = group_total(same, coef[0]) * (1.0 / count)
    coef[1] = group_total(same, coef[1]) * (1.0 / count)

    def rounded(i, carry):
        at = pl.ds(pl.multiple_of(i * step, step), step)
        mean1 = coef[0, at]
        mean2 = coef[1, at]
        rstd = norm[1, at]
        for r in range(image):
            gz_ref[r, at] = (rstd * (gn[r, at] - mean1 - ns[r, at] * mean2)).astype(BF16)
        return carry

    lax.fori_loop(0, half // step, rounded, 0)


def filter_kernel(own_ref, other_ref, xs, *refs, blocks, rows, groups_dp, span):
    outs = refs[:groups_dp]
    gz_out, gz, taps, flat = refs[groups_dp:]
    image, half, width = own_ref.shape
    chans = 2 * half
    home = lax.axis_index("height")
    part = lax.axis_index("dp")
    core = home & 1
    step = 16

    edge = jnp.zeros((chans, width), BF16)
    gz[0] = edge
    gz[image + 1] = edge
    for r in range(image):
        gz[r + 1, pl.ds(pl.multiple_of(core * half, step), half)] = own_ref[r]
        gz[r + 1, pl.ds(pl.multiple_of((1 - core) * half, step), half)] = other_ref[r]
    for r in range(rows + 2):
        gz_out[r] = gz[home * rows + r]

    block = 9 * chans // blocks
    tap0 = (home * block) // chans
    left = jnp.concatenate([gz[r + 1] for r in range(image)], axis=1)
    for j in range(span):
        tap = jnp.minimum(tap0 + j, 8)
        a = tap // 3
        side = pl.ds(pl.multiple_of((tap - a * 3) * chans, step), chans)
        right = jnp.concatenate([xs[r + a, side] for r in range(image)], axis=1)
        rows_of = dot(left, right, ((1,), (1,)))
        for i, (start, size) in enumerate(lane_tiles(chans)):
            taps[i, j * chans : (j + 1) * chans, :size] = rows_of[:, start : start + size]

    off = pl.multiple_of(home * block - tap0 * chans, 8)
    shared = math.gcd(chans, LANES)
    few, many = LANES // shared, chans // shared
    for i in range(taps.shape[0]):
        taps[i, :block] = taps[i, pl.ds(off, block)]
    lines = jnp.concatenate(
        [
            taps[i, pl.ds(line, block // few, stride=few)][:, :size]
            for line in range(few)
            for i, (_, size) in enumerate(lane_tiles(chans))
        ],
        axis=1,
    )
    for i in range(many):
        flat[pl.ds(i, block // few, stride=many)] = lines[:, i * LANES : (i + 1) * LANES]
    piece = flat.shape[0] // groups_dp
    for s in range(groups_dp):
        dest = part ^ s
        value = flat[pl.ds(dest * piece, piece)]
        outs[s][...] = value.astype(outs[s].dtype)


def grad_x_kernel(gz_ref, w_ref, out_ref, *, rows):
    chans, width = gz_ref.shape[1:]
    total = None
    for a in range(3):
        right = jnp.concatenate([gz_ref[2 - a + r] for r in range(rows)], axis=1)
        term = dot(w_ref[a], right, ((0,), (0,)))
        total = term if total is None else total + term
    for r in range(rows):
        part = total[:, r * width : (r + 1) * width]
        value = part[chans : 2 * chans]
        value = value + moved(part[:chans], -1) + moved(part[2 * chans :], 1)
        out_ref[r] = value.astype(BF16)


def vmem(count):
    return [pl.BlockSpec(memory_space=pltpu.VMEM)] * count


def pairs(size, offset):
    return [(i, i ^ offset) for i in range(size)]


def call(kernel, out_shape, args, scratch=(), flops=0, **static):
    single = not isinstance(out_shape, tuple)
    return pl.pallas_call(
        functools.partial(kernel, **static),
        out_shape=out_shape,
        in_specs=vmem(len(args)),
        out_specs=vmem(1)[0] if single else tuple(vmem(len(out_shape))),
        scratch_shapes=list(scratch),
        compiler_params=params(),
        cost_estimate=pl.CostEstimate(flops=flops, bytes_accessed=0, transcendentals=0),
    )(*args)


def gathered(x_next, x_cur, grad_out, kernel, gamma, beta):
    rows, chans, width = x_next.shape[1:]
    blocks = lax.axis_size("height")
    groups_dp = lax.axis_size("dp")
    image = blocks * rows
    half = chans // 2
    count = image * (chans // GROUPS) * width
    block = 9 * chans // blocks
    span = max((h * block % chans + block - 1) // chans + 1 for h in range(blocks))
    piece = block * chans // (groups_dp * LANES)
    flops = 18 * chans * chans * width
    x_next, grad_out = x_next[0], grad_out[0]
    shape = jax.ShapeDtypeStruct

    def far(own):
        held = {0: own}
        for k in sorted(range(2, blocks, 2), key=lambda k: -bin(k).count("1")):
            held[k] = lax.ppermute(own, "height", pairs(blocks, k))
        return held

    def near(own):
        return lax.ppermute(own, "height", pairs(blocks, 1))

    x_far = far(x_cur[0])
    ends = blocks - 1
    top = lax.ppermute(x_next[rows - 1], "height", [(i, i + 1) for i in range(ends)])
    bottom = lax.ppermute(x_next[0], "height", [(i + 1, i) for i in range(ends)])
    own_half, other_half = call(halves_kernel, (shape((rows, half, width), BF16),) * 2, (grad_out,))
    g_pair = jnp.stack((own_half, near(other_half)))
    g_far = far(g_pair)
    gain = jnp.broadcast_to(gamma[:, None], (chans, width))
    shift = jnp.broadcast_to(beta[:, None], (chans, width))
    w_flat = call(weights_kernel, shape((3, chans, 3 * chans), BF16), (kernel,))

    x_far, top, w_flat, _ = lax.optimization_barrier((x_far, top, w_flat, g_pair))
    x_all = []
    for k in range(0, blocks, 2):
        x_all += [x_far[k], near(x_far[k])]
    z_next, stat = call(
        next_conv_kernel,
        (shape((rows, chans, width), F32), shape((8 * -(-2 * len(lane_tiles(chans)) // 8), LANES), F32)),
        (top, x_next, bottom, w_flat),
        flops=rows * flops,
        rows=rows,
    )
    xs, z_cur, norm = call(
        conv_kernel,
        (
            shape((image + 2, 3 * chans, width), BF16),
            shape((image, half, width), F32),
            shape((2, half, width), F32),
        ),
        (*x_all, w_flat),
        scratch=(pltpu.VMEM((half, width), F32),),
        flops=image * flops // 2,
        blocks=blocks,
        rows=rows,
        count=count,
        wide=4 if image % 4 == 0 else 2,
    )
    stat, norm = lax.optimization_barrier((stat, norm))
    stat_pair = jnp.stack((stat, near(stat)))
    gz_own = call(
        pull_kernel,
        shape((image, half, width), BF16),
        (*[g_far[k] for k in range(0, blocks, 2)], z_cur, norm, gain, shift),
        scratch=(
            pltpu.VMEM((image, half, width), F32),
            pltpu.VMEM((image, half, width), F32),
            pltpu.VMEM((2, half, width), F32),
        ),
        flops=image * flops // 8,
        blocks=blocks,
        rows=rows,
        count=count,
    )
    gz_other = near(gz_own)
    stat_pair, gz_own = lax.optimization_barrier((stat_pair, gz_own))
    stat_far = far(stat_pair)
    results = call(
        filter_kernel,
        (shape((piece, LANES), F32),)
        + (shape((piece, LANES), BF16),) * (groups_dp - 1)
        + (shape((rows + 2, chans, width), BF16),),
        (gz_own, gz_other, xs),
        scratch=(
            pltpu.VMEM((image + 2, chans, width), BF16),
            pltpu.VMEM((len(lane_tiles(chans)), span * chans, LANES), F32),
            pltpu.VMEM((groups_dp * piece, LANES), F32),
        ),
        flops=image * flops // 4,
        blocks=blocks,
        rows=rows,
        groups_dp=groups_dp,
        span=span,
    )
    total = results[0]
    for s in range(groups_dp - 1, 0, -1):
        total = total + lax.ppermute(results[s], "dp", pairs(groups_dp, s)).astype(F32)
    grad_x = call(
        grad_x_kernel,
        shape((rows, chans, width), BF16),
        (results[groups_dp], w_flat),
        flops=rows * flops,
        rows=rows,
    )
    y_next = call(
        next_out_kernel,
        shape((rows, chans, width), BF16),
        (*stat_far.values(), z_next, gain, shift),
        flops=rows * flops // 4,
        rows=rows,
        count=count,
    )
    return (y_next[None], grad_x[None], total.reshape(piece * LANES))


def fits(shape, blocks, groups_dp):
    batch, rows, chans, width = shape
    image = blocks * rows
    scratch = image * chans * width * 20 + 9 * chans * chans * 4
    few = LANES // math.gcd(chans, LANES)
    return (
        batch == 1
        and width == LANES
        and chans % 32 == 0
        and chans % GROUPS == 0
        and GROUPS % 2 == 0
        and blocks > 1
        and image % 2 == 0
        and blocks & (blocks - 1) == 0
        and groups_dp & (groups_dp - 1) == 0
        and (9 * chans) % (8 * blocks) == 0
        and (9 * chans // blocks) % few == 0
        and (9 * chans // blocks) * chans % (groups_dp * LANES) == 0
        and scratch < 32 * 1024 * 1024
    )


def solution(mesh):
    blocks, groups_dp = mesh.shape["height"], mesh.shape["dp"]

    def local(x_next, x_cur, grad_out, kernel, gamma, beta):
        if not fits(x_next.shape, blocks, groups_dp):
            return row_sharded(x_next, x_cur, grad_out, kernel, gamma, beta)
        return gathered(x_next, x_cur, grad_out, kernel, gamma, beta)

    placed = (
        P("dp", "height", None, None),
        P("dp", "height", None, None),
        P("dp", "height", None, None),
        P(),
        P(),
        P(),
    )
    return jax.shard_map(
        local,
        mesh=mesh,
        in_specs=placed,
        out_specs=(
            P("dp", "height", None, None),
            P("dp", "height", None, None),
            P(("height", "dp")),
        ),
        check_vma=False,
    )
```

```python
import functools
import math

import jax
import jax.numpy as jnp
from jax import lax
from jax.experimental import pallas as pl
from jax.experimental.pallas import tpu as pltpu
from jax.sharding import PartitionSpec as P

GROUPS = 32

eps = 1e-05


LANES = 128
F32 = jnp.float32
BF16 = jnp.bfloat16


def extended(cells, sides, width):
    for axis, dim in sides:
        count = lax.axis_size(axis)
        ends = count - 1
        head = lax.slice_in_dim(cells, 0, width, axis=dim)
        tail = lax.slice_in_dim(cells, cells.shape[dim] - width, cells.shape[dim], axis=dim)
        cells = jnp.concatenate(
            [
                lax.ppermute(tail, axis, [(i, (i + 1) % count) for i in range(ends)]),
                cells,
                lax.ppermute(head, axis, [((i + 1) % count, i) for i in range(ends)]),
            ],
            axis=dim,
        )
    return cells


def conv_rows(padded, kernel, count):
    width = padded.shape[-1]
    wide = jnp.pad(padded, ((0, 0), (0, 0), (0, 0), (1, 1)))
    total = None
    for tap_row in range(3):
        for tap_col in range(3):
            window = wide[:, tap_row : tap_row + count, :, tap_col : tap_col + width]
            term = jnp.einsum(
                "oc,bhcw->bhow",
                kernel[tap_row, tap_col],
                window,
                preferred_element_type=jnp.float32,
            )
            total = term if total is None else total + term
    return total


def group_sum(value):
    batch, rows, chans, width = value.shape
    return jnp.sum(value.reshape(batch, rows, GROUPS, chans // GROUPS, width), axis=(1, 3, 4))


def row_sharded(x_next, x_cur, grad_out, kernel, gamma, beta):
    _, rows, chans, width = x_next.shape
    height_count = lax.axis_size("height")
    count = height_count * rows * (chans // GROUPS) * width
    gain = gamma[None, None, :, None]
    shift_b = beta[None, None, :, None]

    def expand(stat):
        return jnp.repeat(stat, chans // GROUPS, axis=1)[:, None, :, None]

    stacked = jnp.stack((x_next, x_cur))
    padded = extended(stacked, (("height", 2),), 1)
    xp_next = padded[0]
    xp_cur = padded[1]
    z_next = conv_rows(xp_next, kernel, rows)
    z_cur = conv_rows(xp_cur, kernel, rows)
    sum_next, sum_cur, sq_next, sq_cur = lax.psum(
        (group_sum(z_next), group_sum(z_cur), group_sum(z_next * z_next), group_sum(z_cur * z_cur)),
        "height",
    )
    mean_next = sum_next / count
    mean_cur = sum_cur / count
    var_next = sq_next / count - mean_next * mean_next
    var_cur = sq_cur / count - mean_cur * mean_cur
    rstd_next = lax.rsqrt(var_next + eps)
    rstd_cur = lax.rsqrt(var_cur + eps)
    affine_next = (z_next - expand(mean_next)) * expand(rstd_next) * gain + shift_b
    y_next = (affine_next * jax.nn.sigmoid(affine_next)).astype(jnp.bfloat16)
    normed = (z_cur - expand(mean_cur)) * expand(rstd_cur)
    affine = normed * gain + shift_b
    sig = jax.nn.sigmoid(affine)
    grad_n = grad_out.astype(jnp.float32) * (sig * (1.0 + affine * (1.0 - sig))) * gain
    first_sum, second_sum = lax.psum((group_sum(grad_n), group_sum(grad_n * normed)), "height")
    grad_z = (
        expand(rstd_cur)
        * (grad_n - expand(first_sum / count) - normed * expand(second_sum / count))
    ).astype(jnp.bfloat16)
    grad_pad = extended(grad_z, (("height", 1),), 1)
    grad_own = grad_pad[:, 1:-1]
    grad_wide = jnp.pad(grad_pad, ((0, 0), (0, 0), (0, 0), (1, 1)))
    x_wide = jnp.pad(xp_cur, ((0, 0), (0, 0), (0, 0), (1, 1)))
    grad_input = None
    taps = []
    for tap_row in range(3):
        tap_list = []
        for tap_col in range(3):
            window = grad_wide[
                :, 2 - tap_row : 2 - tap_row + rows, :, 2 - tap_col : 2 - tap_col + width
            ]
            term = jnp.einsum(
                "oc,bhow->bhcw",
                kernel[tap_row, tap_col],
                window,
                preferred_element_type=jnp.float32,
            )
            grad_input = term if grad_input is None else grad_input + term
            source = x_wide[:, tap_row : tap_row + rows, :, tap_col : tap_col + width]
            tap_list.append(
                jnp.einsum("bhow,bhcw->oc", grad_own, source, preferred_element_type=jnp.float32)
            )
        taps.append(jnp.stack(tap_list))
    grad_local = jnp.stack(taps)
    grad_x = grad_input.astype(jnp.bfloat16)
    group_count = lax.axis_size("dp")
    piece = grad_local.size // (height_count * group_count)
    blocks = grad_local.reshape(height_count, group_count, piece)
    shares = lax.psum_scatter(blocks, "dp", scatter_dimension=1, tiled=True)
    grad_kernel = lax.psum_scatter(shares, "height", scatter_dimension=0, tiled=True).reshape(piece)
    return (y_next, grad_x, grad_kernel)


def params(limit=None):
    return pltpu.CompilerParams(vmem_limit_bytes=limit or 40 * 1024 * 1024)


def moved(value, by):
    width = value.shape[-1]
    lane = lax.broadcasted_iota(jnp.int32, value.shape, value.ndim - 1)
    rolled = pltpu.roll(value, by % width, value.ndim - 1)
    keep = lane >= by if by > 0 else lane < width + by
    return jnp.where(keep, rolled, jnp.zeros_like(rolled))


def moved_bf16(value, by):
    return moved(value.astype(F32), by).astype(BF16)


def same_group(rows, chans):
    size = chans // GROUPS
    row = lax.broadcasted_iota(jnp.int32, (rows, rows), 0).astype(F32)
    col = lax.broadcasted_iota(jnp.int32, (rows, rows), 1).astype(F32)
    left = jnp.floor((row + 0.5) * (1.0 / size))
    right = jnp.floor((col + 0.5) * (1.0 / size))
    return jnp.where(left == right, 1.0, 0.0).astype(BF16)


def split3(value):
    high = value.astype(BF16)
    rest = value - high.astype(F32)
    mid = rest.astype(BF16)
    low = (rest - mid.astype(F32)).astype(BF16)
    return high, mid, low


def dot(left, right, dims=((1,), (0,))):
    return lax.dot_general(left, right, (dims, ((), ())), preferred_element_type=F32)


def group_total(same, value):
    column = jnp.sum(value, axis=1, keepdims=True)
    wide = jnp.broadcast_to(column, value.shape)
    high, mid, low = split3(wide)
    return dot(same, high) + (dot(same, mid) + dot(same, low))


def lane_tiles(size):
    return [(at, min(LANES, size - at)) for at in range(0, size, LANES)]


def sigmoid(value):
    return 1.0 / (1.0 + jnp.exp(-value))


def weights_kernel(w_ref, flat_ref, held, sems):
    chans = flat_ref.shape[1]
    copies = [pltpu.make_async_copy(w_ref.at[a], held.at[a], sems.at[a]) for a in range(3)]
    for copy in copies:
        copy.start()
    for a in range(3):
        copies[a].wait()
        for b in range(3):
            flat_ref[a, :, b * chans : (b + 1) * chans] = held[a, b]


def halves_kernel(own_ref, near_ref, out_ref):
    half = out_ref.shape[2]
    core = lax.axis_index("height") & 1
    mine = pl.ds(pl.multiple_of(core * half, 16), half)
    for r in range(out_ref.shape[1]):
        out_ref[0, r] = own_ref[r, mine]
        out_ref[1, r] = near_ref[r, mine]


def next_conv_kernel(top_ref, x_ref, bottom_ref, w_ref, z_ref, stat_ref, *, rows):
    cells = [top_ref[rows - 1]] + [x_ref[r] for r in range(rows)] + [bottom_ref[0]]
    chans, width = cells[0].shape
    sides = [[moved_bf16(cell, 1) for cell in cells], cells, [moved_bf16(cell, -1) for cell in cells]]
    stacks = [jnp.concatenate([side[r] for side in sides], axis=0) for r in range(rows + 2)]
    total = None
    for a in range(3):
        term = dot(w_ref[a], jnp.concatenate(stacks[a : a + rows], axis=1))
        total = term if total is None else total + term
    parts = [total[:, r * width : (r + 1) * width] for r in range(rows)]
    for r in range(rows):
        z_ref[r] = parts[r]
    line = functools.reduce(jnp.add, parts)
    mean = jnp.sum(line, axis=1, keepdims=True) * (1.0 / (rows * width))
    off = functools.reduce(jnp.add, [(part - mean) * (part - mean) for part in parts])
    ones = jnp.ones((8, width), BF16)
    row = lax.broadcasted_iota(jnp.int32, stat_ref.shape, 0)
    packed = jnp.zeros(stat_ref.shape, F32)
    at = 0
    for value in (line, off):
        lane_sum = sum(dot(ones, part, ((1,), (1,))) for part in split3(value))
        for start, size in lane_tiles(chans):
            piece = lane_sum[:1, start : start + size]
            if size < LANES:
                piece = jnp.concatenate([piece, jnp.zeros((1, LANES - size), F32)], axis=1)
            packed = jnp.where(row == at, jnp.broadcast_to(piece, packed.shape), packed)
            at += 1
    stat_ref[...] = packed


def next_out_kernel(*refs, rows, count):
    stat_refs = refs[:-4]
    z_ref, gain_ref, shift_ref, y_ref = refs[-4:]
    chans, width = gain_ref.shape
    same = same_group(chans, chans)
    tiles = lane_tiles(chans)

    def line(value):
        at = value * len(tiles)
        cells = [
            jnp.concatenate([ref[j, at + i : at + i + 1, :size] for i, (_, size) in enumerate(tiles)], axis=1)
            for ref in stat_refs
            for j in range(ref.shape[0])
        ]
        return jnp.concatenate(cells, axis=0)

    sums = line(0)
    offs = line(1)
    each = rows * width
    total = jnp.broadcast_to(jnp.sum(sums, axis=0, keepdims=True), (width, chans))
    mean_line = sum(dot(part, same) for part in split3(total[:8])) * (1.0 / count)
    apart = sums * (1.0 / each) - mean_line[:1]
    spread = jnp.sum(offs + apart * apart * float(each), axis=0, keepdims=True)
    spread = jnp.broadcast_to(spread, (width, chans))
    mean = sum(dot(same, part, ((1,), (1,))) for part in split3(total)) * (1.0 / count)
    var = sum(dot(same, part, ((1,), (1,))) for part in split3(spread)) * (1.0 / count)
    rstd = lax.rsqrt(var + eps)
    for r in range(rows):
        affine = (z_ref[r] - mean) * rstd * gain_ref[...] + shift_ref[...]
        y_ref[r] = (affine * sigmoid(affine)).astype(BF16)


def conv_kernel(*refs, blocks, rows, count, wide):
    x_refs = refs[:blocks]
    w_ref, xs, z, norm, lane = refs[blocks:]
    image, half, width = z.shape
    chans = x_refs[0].shape[1]
    home = lax.axis_index("height")
    mine = pl.ds(pl.multiple_of((home & 1) * half, 16), half)

    edge = jnp.zeros((3 * chans, width), BF16)
    xs[0] = edge
    xs[image + 1] = edge
    for k in range(blocks):
        base = (home ^ k) * rows + 1
        for r in range(rows):
            cell = x_refs[k][r]
            xs[base + r, chans : 2 * chans] = cell
            xs[base + r, :chans] = moved_bf16(cell, 1)
            xs[base + r, 2 * chans :] = moved_bf16(cell, -1)

    def conv(p, start=False):
        row = p * wide
        total = None
        for a in range(3):
            right = jnp.concatenate([xs[row + a + i] for i in range(wide)], axis=1)
            term = dot(w_ref[a, mine], right)
            total = term if total is None else total + term
        parts = [total[:, i * width : (i + 1) * width] for i in range(wide)]
        for i in range(wide):
            z[row + i] = parts[i]
        offs = [part - (parts[0] if start else z[0]) for part in parts]
        sums = functools.reduce(jnp.add, offs)
        squares = functools.reduce(jnp.add, [off * off for off in offs])
        lane[0] = sums if start else lane[0] + sums
        lane[1] = squares if start else lane[1] + squares

    conv(0, True)
    lax.fori_loop(1, image // wide, lambda p, carry: conv(p) or carry, 0)

    same = same_group(half, chans)
    middle = lane[0] * (1.0 / image)
    spread = lane[1] - middle * lane[0]
    middle = z[0] + middle
    mean = group_total(same, middle) * (float(image) / count)
    norm[0] = mean
    apart = middle - mean
    var = group_total(same, spread + apart * apart * float(image)) * (1.0 / count)
    norm[1] = lax.rsqrt(var + eps)


def pull_kernel(*refs, blocks, rows, count):
    g_refs = refs[: blocks // 2]
    z, norm, gain_ref, shift_ref, gz_ref, gn, ns, coef = refs[blocks // 2 :]
    image, half, _ = z.shape
    chans = gain_ref.shape[0]
    home = lax.axis_index("height")
    core = home & 1
    step = 16

    def pulled(i, carry):
        start = pl.multiple_of(i * step, step)
        at = pl.ds(start, step)
        all_at = pl.ds(pl.multiple_of(core * half + start, step), step)
        mean = norm[0, at]
        rstd = norm[1, at]
        gain = gain_ref[all_at]
        shift = shift_ref[all_at]
        first = None
        second = None
        for k in range(blocks):
            base = (home ^ k) * rows
            for r in range(rows):
                n = (z[base + r, at] - mean) * rstd
                affine = n * gain + shift
                sig = sigmoid(affine)
                slope = sig * (1.0 + affine * (1.0 - sig))
                value = g_refs[k // 2][k % 2, r, at].astype(F32) * slope * gain
                gn[base + r, at] = value
                ns[base + r, at] = n
                first = value if first is None else first + value
                second = value * n if second is None else second + value * n
        coef[0, at] = first
        coef[1, at] = second
        return carry

    lax.fori_loop(0, half // step, pulled, 0)
    same = same_group(half, chans)
    coef[0] = group_total(same, coef[0]) * (1.0 / count)
    coef[1] = group_total(same, coef[1]) * (1.0 / count)

    def rounded(i, carry):
        at = pl.ds(pl.multiple_of(i * step, step), step)
        mean1 = coef[0, at]
        mean2 = coef[1, at]
        rstd = norm[1, at]
        for r in range(image):
            gz_ref[r, at] = (rstd * (gn[r, at] - mean1 - ns[r, at] * mean2)).astype(BF16)
        return carry

    lax.fori_loop(0, half // step, rounded, 0)


def filter_kernel(own_ref, other_ref, xs, *refs, blocks, rows, groups_dp, span):
    outs = refs[:groups_dp]
    gz_out, gz, taps, flat = refs[groups_dp:]
    image, half, width = own_ref.shape
    chans = 2 * half
    home = lax.axis_index("height")
    part = lax.axis_index("dp")
    core = home & 1
    step = 16

    edge = jnp.zeros((chans, width), BF16)
    gz[0] = edge
    gz[image + 1] = edge
    for r in range(image):
        gz[r + 1, pl.ds(pl.multiple_of(core * half, step), half)] = own_ref[r]
        gz[r + 1, pl.ds(pl.multiple_of((1 - core) * half, step), half)] = other_ref[r]
    for r in range(rows + 2):
        gz_out[r] = gz[home * rows + r]

    block = 9 * chans // blocks
    tap0 = (home * block) // chans
    left = jnp.concatenate([gz[r + 1] for r in range(image)], axis=1)
    for j in range(span):
        tap = jnp.minimum(tap0 + j, 8)
        a = tap // 3
        side = pl.ds(pl.multiple_of((tap - a * 3) * chans, step), chans)
        right = jnp.concatenate([xs[r + a, side] for r in range(image)], axis=1)
        rows_of = dot(left, right, ((1,), (1,)))
        for i, (start, size) in enumerate(lane_tiles(chans)):
            taps[i, j * chans : (j + 1) * chans, :size] = rows_of[:, start : start + size]

    off = pl.multiple_of(home * block - tap0 * chans, 8)
    shared = math.gcd(chans, LANES)
    few, many = LANES // shared, chans // shared
    for i in range(taps.shape[0]):
        taps[i, :block] = taps[i, pl.ds(off, block)]
    lines = jnp.concatenate(
        [
            taps[i, pl.ds(line, block // few, stride=few)][:, :size]
            for line in range(few)
            for i, (_, size) in enumerate(lane_tiles(chans))
        ],
        axis=1,
    )
    for i in range(many):
        flat[pl.ds(i, block // few, stride=many)] = lines[:, i * LANES : (i + 1) * LANES]
    piece = flat.shape[0] // groups_dp
    for s in range(groups_dp):
        dest = part ^ s
        value = flat[pl.ds(dest * piece, piece)]
        outs[s][...] = value.astype(outs[s].dtype)


def grad_x_kernel(gz_ref, w_ref, out_ref, *, rows):
    chans, width = gz_ref.shape[1:]
    total = None
    for a in range(3):
        right = jnp.concatenate([gz_ref[2 - a + r] for r in range(rows)], axis=1)
        term = dot(w_ref[a], right, ((0,), (0,)))
        total = term if total is None else total + term
    for r in range(rows):
        part = total[:, r * width : (r + 1) * width]
        value = part[chans : 2 * chans]
        value = value + moved(part[:chans], -1) + moved(part[2 * chans :], 1)
        out_ref[r] = value.astype(BF16)


def vmem(count):
    return [pl.BlockSpec(memory_space=pltpu.VMEM)] * count


def pairs(size, offset):
    return [(i, i ^ offset) for i in range(size)]


def call(kernel, out_shape, args, scratch=(), flops=0, **static):
    single = not isinstance(out_shape, tuple)
    return pl.pallas_call(
        functools.partial(kernel, **static),
        out_shape=out_shape,
        in_specs=vmem(len(args)),
        out_specs=vmem(1)[0] if single else tuple(vmem(len(out_shape))),
        scratch_shapes=list(scratch),
        compiler_params=params(),
        cost_estimate=pl.CostEstimate(flops=flops, bytes_accessed=0, transcendentals=0),
    )(*args)


def gathered(x_next, x_cur, grad_out, kernel, gamma, beta):
    rows, chans, width = x_next.shape[1:]
    blocks = lax.axis_size("height")
    groups_dp = lax.axis_size("dp")
    image = blocks * rows
    half = chans // 2
    count = image * (chans // GROUPS) * width
    block = 9 * chans // blocks
    span = max((h * block % chans + block - 1) // chans + 1 for h in range(blocks))
    piece = block * chans // (groups_dp * LANES)
    flops = 18 * chans * chans * width
    x_next, grad_out = x_next[0], grad_out[0]
    shape = jax.ShapeDtypeStruct

    def far(own):
        held = {0: own}
        for k in sorted(range(2, blocks, 2), key=lambda k: -bin(k).count("1")):
            held[k] = lax.ppermute(own, "height", pairs(blocks, k))
        return held

    def near(own):
        return lax.ppermute(own, "height", pairs(blocks, 1))

    x_far = far(x_cur[0])
    ends = blocks - 1
    top = lax.ppermute(x_next, "height", [(i, i + 1) for i in range(ends)])
    bottom = lax.ppermute(x_next, "height", [(i + 1, i) for i in range(ends)])
    g_near = near(grad_out)
    g_pair = call(halves_kernel, shape((2, rows, half, width), BF16), (grad_out, g_near))
    g_far = far(g_pair)
    gain = jnp.broadcast_to(gamma[:, None], (chans, width))
    shift = jnp.broadcast_to(beta[:, None], (chans, width))
    w_flat = pl.pallas_call(
        weights_kernel,
        out_shape=shape((3, chans, 3 * chans), BF16),
        in_specs=[pl.BlockSpec(memory_space=pltpu.HBM)],
        out_specs=vmem(1)[0],
        scratch_shapes=[pltpu.VMEM((3, 3, chans, chans), BF16), pltpu.SemaphoreType.DMA((3,))],
        compiler_params=params(),
        name="weights",
    )(pltpu.with_memory_space_constraint(kernel, pltpu.HBM))

    x_far, top, w_flat, gain, shift, _ = lax.optimization_barrier(
        (x_far, top, w_flat, gain, shift, g_pair)
    )
    x_all = []
    for k in range(0, blocks, 2):
        x_all += [x_far[k], near(x_far[k])]
    z_next, stat = call(
        next_conv_kernel,
        (shape((rows, chans, width), F32), shape((8 * -(-2 * len(lane_tiles(chans)) // 8), LANES), F32)),
        (top, x_next, bottom, w_flat),
        flops=rows * flops,
        rows=rows,
    )
    stat_near = near(stat)
    x_all, z_next = lax.optimization_barrier((x_all, z_next))
    xs, z_cur, norm = call(
        conv_kernel,
        (
            shape((image + 2, 3 * chans, width), BF16),
            shape((image, half, width), F32),
            shape((2, half, width), F32),
        ),
        (*x_all, w_flat),
        scratch=(pltpu.VMEM((2, half, width), F32),),
        flops=image * flops // 2,
        blocks=blocks,
        rows=rows,
        count=count,
        wide=4 if image % 4 == 0 else 2,
    )
    stat_pair = jnp.stack((stat, stat_near))
    gz_own = call(
        pull_kernel,
        shape((image, half, width), BF16),
        (*[g_far[k] for k in range(0, blocks, 2)], z_cur, norm, gain, shift),
        scratch=(
            pltpu.VMEM((image, half, width), F32),
            pltpu.VMEM((image, half, width), F32),
            pltpu.VMEM((2, half, width), F32),
        ),
        flops=image * flops // 8,
        blocks=blocks,
        rows=rows,
        count=count,
    )
    gz_other = near(gz_own)
    stat_pair, gz_own = lax.optimization_barrier((stat_pair, gz_own))
    stat_far = far(stat_pair)
    results = call(
        filter_kernel,
        (shape((piece, LANES), F32),)
        + (shape((piece, LANES), BF16),) * (groups_dp - 1)
        + (shape((rows + 2, chans, width), BF16),),
        (gz_own, gz_other, xs),
        scratch=(
            pltpu.VMEM((image + 2, chans, width), BF16),
            pltpu.VMEM((len(lane_tiles(chans)), span * chans, LANES), F32),
            pltpu.VMEM((groups_dp * piece, LANES), F32),
        ),
        flops=image * flops // 4,
        blocks=blocks,
        rows=rows,
        groups_dp=groups_dp,
        span=span,
    )
    total = results[0]
    for s in range(groups_dp - 1, 0, -1):
        total = total + lax.ppermute(results[s], "dp", pairs(groups_dp, s)).astype(F32)
    grad_x = call(
        grad_x_kernel,
        shape((rows, chans, width), BF16),
        (results[groups_dp], w_flat),
        flops=rows * flops,
        rows=rows,
    )
    y_next = call(
        next_out_kernel,
        shape((rows, chans, width), BF16),
        (*stat_far.values(), z_next, gain, shift),
        flops=rows * flops // 4,
        rows=rows,
        count=count,
    )
    return (y_next[None], grad_x[None], total.reshape(piece * LANES))


def fits(shape, blocks, groups_dp):
    batch, rows, chans, width = shape
    image = blocks * rows
    scratch = image * chans * width * 20 + 9 * chans * chans * 4
    few = LANES // math.gcd(chans, LANES)
    return (
        batch == 1
        and width == LANES
        and chans % 32 == 0
        and chans % GROUPS == 0
        and GROUPS % 2 == 0
        and blocks > 1
        and image % 2 == 0
        and blocks & (blocks - 1) == 0
        and groups_dp & (groups_dp - 1) == 0
        and (9 * chans) % (8 * blocks) == 0
        and (9 * chans // blocks) % few == 0
        and (9 * chans // blocks) * chans % (groups_dp * LANES) == 0
        and scratch < 32 * 1024 * 1024
    )


def solution(mesh):
    blocks, groups_dp = mesh.shape["height"], mesh.shape["dp"]

    def local(x_next, x_cur, grad_out, kernel, gamma, beta):
        if not fits(x_next.shape, blocks, groups_dp):
            return row_sharded(x_next, x_cur, grad_out, kernel, gamma, beta)
        return gathered(x_next, x_cur, grad_out, kernel, gamma, beta)

    placed = (
        P("dp", "height", None, None),
        P("dp", "height", None, None),
        P("dp", "height", None, None),
        P(),
        P(),
        P(),
    )
    return jax.shard_map(
        local,
        mesh=mesh,
        in_specs=placed,
        out_specs=(
            P("dp", "height", None, None),
            P("dp", "height", None, None),
            P(("height", "dp")),
        ),
        check_vma=False,
    )
```

```python
import functools
import math

import jax
import jax.numpy as jnp
from jax import lax
from jax.experimental import pallas as pl
from jax.experimental.pallas import tpu as pltpu
from jax.sharding import PartitionSpec as P

GROUPS = 32

eps = 1e-05


LANES = 128
F32 = jnp.float32
BF16 = jnp.bfloat16


def extended(cells, sides, width):
    for axis, dim in sides:
        count = lax.axis_size(axis)
        ends = count - 1
        head = lax.slice_in_dim(cells, 0, width, axis=dim)
        tail = lax.slice_in_dim(cells, cells.shape[dim] - width, cells.shape[dim], axis=dim)
        cells = jnp.concatenate(
            [
                lax.ppermute(tail, axis, [(i, (i + 1) % count) for i in range(ends)]),
                cells,
                lax.ppermute(head, axis, [((i + 1) % count, i) for i in range(ends)]),
            ],
            axis=dim,
        )
    return cells


def conv_rows(padded, kernel, count):
    width = padded.shape[-1]
    wide = jnp.pad(padded, ((0, 0), (0, 0), (0, 0), (1, 1)))
    total = None
    for tap_row in range(3):
        for tap_col in range(3):
            window = wide[:, tap_row : tap_row + count, :, tap_col : tap_col + width]
            term = jnp.einsum(
                "oc,bhcw->bhow",
                kernel[tap_row, tap_col],
                window,
                preferred_element_type=jnp.float32,
            )
            total = term if total is None else total + term
    return total


def group_sum(value):
    batch, rows, chans, width = value.shape
    return jnp.sum(value.reshape(batch, rows, GROUPS, chans // GROUPS, width), axis=(1, 3, 4))


def row_sharded(x_next, x_cur, grad_out, kernel, gamma, beta):
    _, rows, chans, width = x_next.shape
    height_count = lax.axis_size("height")
    count = height_count * rows * (chans // GROUPS) * width
    gain = gamma[None, None, :, None]
    shift_b = beta[None, None, :, None]

    def expand(stat):
        return jnp.repeat(stat, chans // GROUPS, axis=1)[:, None, :, None]

    stacked = jnp.stack((x_next, x_cur))
    padded = extended(stacked, (("height", 2),), 1)
    xp_next = padded[0]
    xp_cur = padded[1]
    z_next = conv_rows(xp_next, kernel, rows)
    z_cur = conv_rows(xp_cur, kernel, rows)
    sum_next, sum_cur, sq_next, sq_cur = lax.psum(
        (group_sum(z_next), group_sum(z_cur), group_sum(z_next * z_next), group_sum(z_cur * z_cur)),
        "height",
    )
    mean_next = sum_next / count
    mean_cur = sum_cur / count
    var_next = sq_next / count - mean_next * mean_next
    var_cur = sq_cur / count - mean_cur * mean_cur
    rstd_next = lax.rsqrt(var_next + eps)
    rstd_cur = lax.rsqrt(var_cur + eps)
    affine_next = (z_next - expand(mean_next)) * expand(rstd_next) * gain + shift_b
    y_next = (affine_next * jax.nn.sigmoid(affine_next)).astype(jnp.bfloat16)
    normed = (z_cur - expand(mean_cur)) * expand(rstd_cur)
    affine = normed * gain + shift_b
    sig = jax.nn.sigmoid(affine)
    grad_n = grad_out.astype(jnp.float32) * (sig * (1.0 + affine * (1.0 - sig))) * gain
    first_sum, second_sum = lax.psum((group_sum(grad_n), group_sum(grad_n * normed)), "height")
    grad_z = (
        expand(rstd_cur)
        * (grad_n - expand(first_sum / count) - normed * expand(second_sum / count))
    ).astype(jnp.bfloat16)
    grad_pad = extended(grad_z, (("height", 1),), 1)
    grad_own = grad_pad[:, 1:-1]
    grad_wide = jnp.pad(grad_pad, ((0, 0), (0, 0), (0, 0), (1, 1)))
    x_wide = jnp.pad(xp_cur, ((0, 0), (0, 0), (0, 0), (1, 1)))
    grad_input = None
    taps = []
    for tap_row in range(3):
        tap_list = []
        for tap_col in range(3):
            window = grad_wide[
                :, 2 - tap_row : 2 - tap_row + rows, :, 2 - tap_col : 2 - tap_col + width
            ]
            term = jnp.einsum(
                "oc,bhow->bhcw",
                kernel[tap_row, tap_col],
                window,
                preferred_element_type=jnp.float32,
            )
            grad_input = term if grad_input is None else grad_input + term
            source = x_wide[:, tap_row : tap_row + rows, :, tap_col : tap_col + width]
            tap_list.append(
                jnp.einsum("bhow,bhcw->oc", grad_own, source, preferred_element_type=jnp.float32)
            )
        taps.append(jnp.stack(tap_list))
    grad_local = jnp.stack(taps)
    grad_x = grad_input.astype(jnp.bfloat16)
    group_count = lax.axis_size("dp")
    piece = grad_local.size // (height_count * group_count)
    blocks = grad_local.reshape(height_count, group_count, piece)
    shares = lax.psum_scatter(blocks, "dp", scatter_dimension=1, tiled=True)
    grad_kernel = lax.psum_scatter(shares, "height", scatter_dimension=0, tiled=True).reshape(piece)
    return (y_next, grad_x, grad_kernel)


def params(limit=None):
    return pltpu.CompilerParams(vmem_limit_bytes=limit or 40 * 1024 * 1024)


def moved(value, by):
    width = value.shape[-1]
    lane = lax.broadcasted_iota(jnp.int32, value.shape, value.ndim - 1)
    rolled = pltpu.roll(value, by % width, value.ndim - 1)
    keep = lane >= by if by > 0 else lane < width + by
    return jnp.where(keep, rolled, jnp.zeros_like(rolled))


def moved_bf16(value, by):
    return moved(value.astype(F32), by).astype(BF16)


def same_group(rows, chans):
    size = chans // GROUPS
    row = lax.broadcasted_iota(jnp.int32, (rows, rows), 0).astype(F32)
    col = lax.broadcasted_iota(jnp.int32, (rows, rows), 1).astype(F32)
    left = jnp.floor((row + 0.5) * (1.0 / size))
    right = jnp.floor((col + 0.5) * (1.0 / size))
    return jnp.where(left == right, 1.0, 0.0).astype(BF16)


def split3(value):
    high = value.astype(BF16)
    rest = value - high.astype(F32)
    mid = rest.astype(BF16)
    low = (rest - mid.astype(F32)).astype(BF16)
    return high, mid, low


def dot(left, right, dims=((1,), (0,))):
    return lax.dot_general(left, right, (dims, ((), ())), preferred_element_type=F32)


def group_total(same, value):
    column = jnp.sum(value, axis=1, keepdims=True)
    wide = jnp.broadcast_to(column, value.shape)
    high, mid, low = split3(wide)
    return dot(same, high) + (dot(same, mid) + dot(same, low))


def lane_tiles(size):
    return [(at, min(LANES, size - at)) for at in range(0, size, LANES)]


def sigmoid(value):
    return 1.0 / (1.0 + jnp.exp(-value))


def weights_kernel(w_ref, flat_ref):
    chans = flat_ref.shape[1]
    for a in range(3):
        for b in range(3):
            flat_ref[a, :, b * chans : (b + 1) * chans] = w_ref[a, b]


def halves_kernel(own_ref, near_ref, out_ref):
    half = out_ref.shape[2]
    core = lax.axis_index("height") & 1
    mine = pl.ds(pl.multiple_of(core * half, 16), half)
    for r in range(out_ref.shape[1]):
        out_ref[0, r] = own_ref[r, mine]
        out_ref[1, r] = near_ref[r, mine]


def next_conv_kernel(edge_ref, near_ref, x_ref, w_ref, z_ref, stat_ref, *, rows):
    even = (lax.axis_index("height") & 1) == 0
    side = edge_ref[...].astype(F32)
    top = jnp.where(even, side, near_ref[rows - 1].astype(F32)).astype(BF16)
    bottom = jnp.where(even, near_ref[0].astype(F32), side).astype(BF16)
    cells = [top] + [x_ref[r] for r in range(rows)] + [bottom]
    chans, width = cells[0].shape
    sides = [[moved_bf16(cell, 1) for cell in cells], cells, [moved_bf16(cell, -1) for cell in cells]]
    stacks = [jnp.concatenate([side[r] for side in sides], axis=0) for r in range(rows + 2)]
    total = None
    for a in range(3):
        term = dot(w_ref[a], jnp.concatenate(stacks[a : a + rows], axis=1))
        total = term if total is None else total + term
    parts = [total[:, r * width : (r + 1) * width] for r in range(rows)]
    for r in range(rows):
        z_ref[r] = parts[r]
    line = functools.reduce(jnp.add, parts)
    mean = jnp.sum(line, axis=1, keepdims=True) * (1.0 / (rows * width))
    off = functools.reduce(jnp.add, [(part - mean) * (part - mean) for part in parts])
    ones = jnp.ones((8, width), BF16)
    row = lax.broadcasted_iota(jnp.int32, stat_ref.shape, 0)
    packed = jnp.zeros(stat_ref.shape, F32)
    at = 0
    for value in (line, off):
        lane_sum = sum(dot(ones, part, ((1,), (1,))) for part in split3(value))
        for start, size in lane_tiles(chans):
            piece = lane_sum[:1, start : start + size]
            if size < LANES:
                piece = jnp.concatenate([piece, jnp.zeros((1, LANES - size), F32)], axis=1)
            packed = jnp.where(row == at, jnp.broadcast_to(piece, packed.shape), packed)
            at += 1
    stat_ref[...] = packed


def next_out_kernel(*refs, rows, count):
    stat_refs = refs[:-4]
    z_ref, gain_ref, shift_ref, y_ref = refs[-4:]
    chans, width = gain_ref.shape
    same = same_group(chans, chans)
    tiles = lane_tiles(chans)

    def line(value):
        at = value * len(tiles)
        cells = [
            jnp.concatenate([ref[j, at + i : at + i + 1, :size] for i, (_, size) in enumerate(tiles)], axis=1)
            for ref in stat_refs
            for j in range(ref.shape[0])
        ]
        return jnp.concatenate(cells, axis=0)

    sums = line(0)
    offs = line(1)
    each = rows * width
    total = jnp.broadcast_to(jnp.sum(sums, axis=0, keepdims=True), (width, chans))
    mean_line = sum(dot(part, same) for part in split3(total[:8])) * (1.0 / count)
    apart = sums * (1.0 / each) - mean_line[:1]
    spread = jnp.sum(offs + apart * apart * float(each), axis=0, keepdims=True)
    spread = jnp.broadcast_to(spread, (width, chans))
    mean = sum(dot(same, part, ((1,), (1,))) for part in split3(total)) * (1.0 / count)
    var = sum(dot(same, part, ((1,), (1,))) for part in split3(spread)) * (1.0 / count)
    rstd = lax.rsqrt(var + eps)
    for r in range(rows):
        affine = (z_ref[r] - mean) * rstd * gain_ref[...] + shift_ref[...]
        y_ref[r] = (affine * sigmoid(affine)).astype(BF16)


def conv_kernel(*refs, blocks, rows, count, wide):
    x_refs = refs[:blocks]
    w_ref, xs, z, norm, lane = refs[blocks:]
    image, half, width = z.shape
    chans = x_refs[0].shape[1]
    home = lax.axis_index("height")
    mine = pl.ds(pl.multiple_of((home & 1) * half, 16), half)

    edge = jnp.zeros((3 * chans, width), BF16)
    xs[0] = edge
    xs[image + 1] = edge
    for k in range(blocks):
        base = (home ^ k) * rows + 1
        for r in range(rows):
            cell = x_refs[k][r]
            xs[base + r, chans : 2 * chans] = cell
            xs[base + r, :chans] = moved_bf16(cell, 1)
            xs[base + r, 2 * chans :] = moved_bf16(cell, -1)

    def conv(p, start=False):
        row = p * wide
        total = None
        for a in range(3):
            right = jnp.concatenate([xs[row + a + i] for i in range(wide)], axis=1)
            term = dot(w_ref[a, mine], right)
            total = term if total is None else total + term
        parts = [total[:, i * width : (i + 1) * width] for i in range(wide)]
        for i in range(wide):
            z[row + i] = parts[i]
        offs = [part - (parts[0] if start else z[0]) for part in parts]
        sums = functools.reduce(jnp.add, offs)
        squares = functools.reduce(jnp.add, [off * off for off in offs])
        lane[0] = sums if start else lane[0] + sums
        lane[1] = squares if start else lane[1] + squares

    conv(0, True)
    lax.fori_loop(1, image // wide, lambda p, carry: conv(p) or carry, 0)

    same = same_group(half, chans)
    middle = lane[0] * (1.0 / image)
    spread = lane[1] - middle * lane[0]
    middle = z[0] + middle
    mean = group_total(same, middle) * (float(image) / count)
    norm[0] = mean
    apart = middle - mean
    var = group_total(same, spread + apart * apart * float(image)) * (1.0 / count)
    norm[1] = lax.rsqrt(var + eps)


def pull_kernel(*refs, blocks, rows, count):
    g_refs = refs[: blocks // 2]
    z, norm, gain_ref, shift_ref, gz_ref, gn, ns, coef = refs[blocks // 2 :]
    image, half, _ = z.shape
    chans = gain_ref.shape[0]
    home = lax.axis_index("height")
    core = home & 1
    step = 16

    def pulled(i, carry):
        start = pl.multiple_of(i * step, step)
        at = pl.ds(start, step)
        all_at = pl.ds(pl.multiple_of(core * half + start, step), step)
        mean = norm[0, at]
        rstd = norm[1, at]
        gain = gain_ref[all_at]
        shift = shift_ref[all_at]
        first = None
        second = None
        for k in range(blocks):
            base = (home ^ k) * rows
            for r in range(rows):
                n = (z[base + r, at] - mean) * rstd
                affine = n * gain + shift
                sig = sigmoid(affine)
                slope = sig * (1.0 + affine * (1.0 - sig))
                value = g_refs[k // 2][k % 2, r, at].astype(F32) * slope * gain
                gn[base + r, at] = value
                ns[base + r, at] = n
                first = value if first is None else first + value
                second = value * n if second is None else second + value * n
        coef[0, at] = first
        coef[1, at] = second
        return carry

    lax.fori_loop(0, half // step, pulled, 0)
    same = same_group(half, chans)
    coef[0] = group_total(same, coef[0]) * (1.0 / count)
    coef[1] = group_total(same, coef[1]) * (1.0 / count)

    def rounded(i, carry):
        at = pl.ds(pl.multiple_of(i * step, step), step)
        mean1 = coef[0, at]
        mean2 = coef[1, at]
        rstd = norm[1, at]
        for r in range(image):
            gz_ref[r, at] = (rstd * (gn[r, at] - mean1 - ns[r, at] * mean2)).astype(BF16)
        return carry

    lax.fori_loop(0, half // step, rounded, 0)


def filter_kernel(own_ref, other_ref, xs, *refs, blocks, rows, groups_dp, span):
    outs = refs[:groups_dp]
    gz_out, gz, taps, flat = refs[groups_dp:]
    image, half, width = own_ref.shape
    chans = 2 * half
    home = lax.axis_index("height")
    part = lax.axis_index("dp")
    core = home & 1
    step = 16

    edge = jnp.zeros((chans, width), BF16)
    gz[0] = edge
    gz[image + 1] = edge
    for r in range(image):
        gz[r + 1, pl.ds(pl.multiple_of(core * half, step), half)] = own_ref[r]
        gz[r + 1, pl.ds(pl.multiple_of((1 - core) * half, step), half)] = other_ref[r]
    for r in range(rows + 2):
        gz_out[r] = gz[home * rows + r]

    block = 9 * chans // blocks
    tap0 = (home * block) // chans
    left = jnp.concatenate([gz[r + 1] for r in range(image)], axis=1)
    for j in range(span):
        tap = jnp.minimum(tap0 + j, 8)
        a = tap // 3
        side = pl.ds(pl.multiple_of((tap - a * 3) * chans, step), chans)
        right = jnp.concatenate([xs[r + a, side] for r in range(image)], axis=1)
        rows_of = dot(left, right, ((1,), (1,)))
        for i, (start, size) in enumerate(lane_tiles(chans)):
            taps[i, j * chans : (j + 1) * chans, :size] = rows_of[:, start : start + size]

    off = pl.multiple_of(home * block - tap0 * chans, 8)
    shared = math.gcd(chans, LANES)
    few, many = LANES // shared, chans // shared
    for i in range(taps.shape[0]):
        taps[i, :block] = taps[i, pl.ds(off, block)]
    lines = jnp.concatenate(
        [
            taps[i, pl.ds(line, block // few, stride=few)][:, :size]
            for line in range(few)
            for i, (_, size) in enumerate(lane_tiles(chans))
        ],
        axis=1,
    )
    for i in range(many):
        flat[pl.ds(i, block // few, stride=many)] = lines[:, i * LANES : (i + 1) * LANES]
    piece = flat.shape[0] // groups_dp
    for s in range(groups_dp):
        dest = part ^ s
        value = flat[pl.ds(dest * piece, piece)]
        outs[s][...] = value.astype(outs[s].dtype)


def grad_x_kernel(gz_ref, w_ref, out_ref, *, rows):
    chans, width = gz_ref.shape[1:]
    total = None
    for a in range(3):
        right = jnp.concatenate([gz_ref[2 - a + r] for r in range(rows)], axis=1)
        term = dot(w_ref[a], right, ((0,), (0,)))
        total = term if total is None else total + term
    for r in range(rows):
        part = total[:, r * width : (r + 1) * width]
        value = part[chans : 2 * chans]
        value = value + moved(part[:chans], -1) + moved(part[2 * chans :], 1)
        out_ref[r] = value.astype(BF16)


def vmem(count):
    return [pl.BlockSpec(memory_space=pltpu.VMEM)] * count


def pairs(size, offset):
    return [(i, i ^ offset) for i in range(size)]


def call(kernel, out_shape, args, scratch=(), flops=0, **static):
    single = not isinstance(out_shape, tuple)
    return pl.pallas_call(
        functools.partial(kernel, **static),
        out_shape=out_shape,
        in_specs=vmem(len(args)),
        out_specs=vmem(1)[0] if single else tuple(vmem(len(out_shape))),
        scratch_shapes=list(scratch),
        compiler_params=params(),
        cost_estimate=pl.CostEstimate(flops=flops, bytes_accessed=0, transcendentals=0),
    )(*args)


def gathered(x_next, x_cur, grad_out, kernel, gamma, beta):
    rows, chans, width = x_next.shape[1:]
    blocks = lax.axis_size("height")
    groups_dp = lax.axis_size("dp")
    image = blocks * rows
    half = chans // 2
    count = image * (chans // GROUPS) * width
    block = 9 * chans // blocks
    span = max((h * block % chans + block - 1) // chans + 1 for h in range(blocks))
    piece = block * chans // (groups_dp * LANES)
    flops = 18 * chans * chans * width
    x_next, grad_out = x_next[0], grad_out[0]
    shape = jax.ShapeDtypeStruct

    def far(own):
        held = {0: own}
        for k in sorted(range(2, blocks, 2), key=lambda k: -bin(k).count("1")):
            held[k] = lax.ppermute(own, "height", pairs(blocks, k))
        return held

    def near(own):
        return lax.ppermute(own, "height", pairs(blocks, 1))

    x_far = far(x_cur[0])
    even = (lax.axis_index("height") & 1) == 0
    edge = lax.dynamic_index_in_dim(x_next, jnp.where(even, 0, rows - 1), 0, keepdims=False)
    next_near = near(x_next)
    swaps = [(i, i + 1) for i in range(1, blocks - 1, 2)]
    edge = lax.ppermute(edge, "height", swaps + [(j, i) for i, j in swaps])
    g_near = near(grad_out)
    g_pair = call(
        halves_kernel, shape((2, rows, half, width), BF16), (grad_out, g_near), flops=image * flops
    )
    g_far = far(g_pair)
    gain = jnp.broadcast_to(gamma[:, None], (chans, width))
    shift = jnp.broadcast_to(beta[:, None], (chans, width))
    w_flat = call(weights_kernel, shape((3, chans, 3 * chans), BF16), (kernel,))

    x_far, w_flat, gain, shift, _ = lax.optimization_barrier((x_far, w_flat, gain, shift, g_pair))
    x_all = []
    for k in range(0, blocks, 2):
        x_all += [x_far[k], near(x_far[k])]
    z_next, stat = call(
        next_conv_kernel,
        (shape((rows, chans, width), F32), shape((8 * -(-2 * len(lane_tiles(chans)) // 8), LANES), F32)),
        (edge, next_near, x_next, w_flat),
        flops=rows * flops,
        rows=rows,
    )
    stat_near = near(stat)
    x_all, z_next = lax.optimization_barrier((x_all, z_next))
    xs, z_cur, norm = call(
        conv_kernel,
        (
            shape((image + 2, 3 * chans, width), BF16),
            shape((image, half, width), F32),
            shape((2, half, width), F32),
        ),
        (*x_all, w_flat),
        scratch=(pltpu.VMEM((2, half, width), F32),),
        flops=image * flops // 2,
        blocks=blocks,
        rows=rows,
        count=count,
        wide=4 if image % 4 == 0 else 2,
    )
    stat_pair = jnp.stack((stat, stat_near))
    gz_own = call(
        pull_kernel,
        shape((image, half, width), BF16),
        (*[g_far[k] for k in range(0, blocks, 2)], z_cur, norm, gain, shift),
        scratch=(
            pltpu.VMEM((image, half, width), F32),
            pltpu.VMEM((image, half, width), F32),
            pltpu.VMEM((2, half, width), F32),
        ),
        flops=image * flops // 8,
        blocks=blocks,
        rows=rows,
        count=count,
    )
    gz_other = near(gz_own)
    stat_pair, gz_own = lax.optimization_barrier((stat_pair, gz_own))
    stat_far = far(stat_pair)
    results = call(
        filter_kernel,
        (shape((piece, LANES), F32),)
        + (shape((piece, LANES), BF16),) * (groups_dp - 1)
        + (shape((rows + 2, chans, width), BF16),),
        (gz_own, gz_other, xs),
        scratch=(
            pltpu.VMEM((image + 2, chans, width), BF16),
            pltpu.VMEM((len(lane_tiles(chans)), span * chans, LANES), F32),
            pltpu.VMEM((groups_dp * piece, LANES), F32),
        ),
        flops=image * flops // 4,
        blocks=blocks,
        rows=rows,
        groups_dp=groups_dp,
        span=span,
    )
    total = results[0]
    for s in range(groups_dp - 1, 0, -1):
        total = total + lax.ppermute(results[s], "dp", pairs(groups_dp, s)).astype(F32)
    grad_x = call(
        grad_x_kernel,
        shape((rows, chans, width), BF16),
        (results[groups_dp], w_flat),
        flops=rows * flops,
        rows=rows,
    )
    y_next = call(
        next_out_kernel,
        shape((rows, chans, width), BF16),
        (*stat_far.values(), z_next, gain, shift),
        flops=rows * flops // 4,
        rows=rows,
        count=count,
    )
    return (y_next[None], grad_x[None], total.reshape(piece * LANES))


def fits(shape, blocks, groups_dp):
    batch, rows, chans, width = shape
    image = blocks * rows
    scratch = image * chans * width * 20 + 9 * chans * chans * 4
    few = LANES // math.gcd(chans, LANES)
    return (
        batch == 1
        and width == LANES
        and chans % 32 == 0
        and chans % GROUPS == 0
        and GROUPS % 2 == 0
        and blocks > 1
        and image % 2 == 0
        and blocks & (blocks - 1) == 0
        and groups_dp & (groups_dp - 1) == 0
        and (9 * chans) % (8 * blocks) == 0
        and (9 * chans // blocks) % few == 0
        and (9 * chans // blocks) * chans % (groups_dp * LANES) == 0
        and scratch < 32 * 1024 * 1024
    )


def solution(mesh):
    blocks, groups_dp = mesh.shape["height"], mesh.shape["dp"]

    def local(x_next, x_cur, grad_out, kernel, gamma, beta):
        if not fits(x_next.shape, blocks, groups_dp):
            return row_sharded(x_next, x_cur, grad_out, kernel, gamma, beta)
        return gathered(x_next, x_cur, grad_out, kernel, gamma, beta)

    placed = (
        P("dp", "height", None, None),
        P("dp", "height", None, None),
        P("dp", "height", None, None),
        P(),
        P(),
        P(),
    )
    return jax.shard_map(
        local,
        mesh=mesh,
        in_specs=placed,
        out_specs=(
            P("dp", "height", None, None),
            P("dp", "height", None, None),
            P(("height", "dp")),
        ),
        check_vma=False,
    )
```

```python
import functools
import math

import jax
import jax.numpy as jnp
from jax import lax
from jax.experimental import pallas as pl
from jax.experimental.pallas import tpu as pltpu
from jax.sharding import PartitionSpec as P

GROUPS = 32

eps = 1e-05


LANES = 128
F32 = jnp.float32
BF16 = jnp.bfloat16


def extended(cells, sides, width):
    for axis, dim in sides:
        count = lax.axis_size(axis)
        ends = count - 1
        head = lax.slice_in_dim(cells, 0, width, axis=dim)
        tail = lax.slice_in_dim(cells, cells.shape[dim] - width, cells.shape[dim], axis=dim)
        cells = jnp.concatenate(
            [
                lax.ppermute(tail, axis, [(i, (i + 1) % count) for i in range(ends)]),
                cells,
                lax.ppermute(head, axis, [((i + 1) % count, i) for i in range(ends)]),
            ],
            axis=dim,
        )
    return cells


def conv_rows(padded, kernel, count):
    width = padded.shape[-1]
    wide = jnp.pad(padded, ((0, 0), (0, 0), (0, 0), (1, 1)))
    total = None
    for tap_row in range(3):
        for tap_col in range(3):
            window = wide[:, tap_row : tap_row + count, :, tap_col : tap_col + width]
            term = jnp.einsum(
                "oc,bhcw->bhow",
                kernel[tap_row, tap_col],
                window,
                preferred_element_type=jnp.float32,
            )
            total = term if total is None else total + term
    return total


def group_sum(value):
    batch, rows, chans, width = value.shape
    return jnp.sum(value.reshape(batch, rows, GROUPS, chans // GROUPS, width), axis=(1, 3, 4))


def row_sharded(x_next, x_cur, grad_out, kernel, gamma, beta):
    _, rows, chans, width = x_next.shape
    height_count = lax.axis_size("height")
    count = height_count * rows * (chans // GROUPS) * width
    gain = gamma[None, None, :, None]
    shift_b = beta[None, None, :, None]

    def expand(stat):
        return jnp.repeat(stat, chans // GROUPS, axis=1)[:, None, :, None]

    stacked = jnp.stack((x_next, x_cur))
    padded = extended(stacked, (("height", 2),), 1)
    xp_next = padded[0]
    xp_cur = padded[1]
    z_next = conv_rows(xp_next, kernel, rows)
    z_cur = conv_rows(xp_cur, kernel, rows)
    sum_next, sum_cur, sq_next, sq_cur = lax.psum(
        (group_sum(z_next), group_sum(z_cur), group_sum(z_next * z_next), group_sum(z_cur * z_cur)),
        "height",
    )
    mean_next = sum_next / count
    mean_cur = sum_cur / count
    var_next = sq_next / count - mean_next * mean_next
    var_cur = sq_cur / count - mean_cur * mean_cur
    rstd_next = lax.rsqrt(var_next + eps)
    rstd_cur = lax.rsqrt(var_cur + eps)
    affine_next = (z_next - expand(mean_next)) * expand(rstd_next) * gain + shift_b
    y_next = (affine_next * jax.nn.sigmoid(affine_next)).astype(jnp.bfloat16)
    normed = (z_cur - expand(mean_cur)) * expand(rstd_cur)
    affine = normed * gain + shift_b
    sig = jax.nn.sigmoid(affine)
    grad_n = grad_out.astype(jnp.float32) * (sig * (1.0 + affine * (1.0 - sig))) * gain
    first_sum, second_sum = lax.psum((group_sum(grad_n), group_sum(grad_n * normed)), "height")
    grad_z = (
        expand(rstd_cur)
        * (grad_n - expand(first_sum / count) - normed * expand(second_sum / count))
    ).astype(jnp.bfloat16)
    grad_pad = extended(grad_z, (("height", 1),), 1)
    grad_own = grad_pad[:, 1:-1]
    grad_wide = jnp.pad(grad_pad, ((0, 0), (0, 0), (0, 0), (1, 1)))
    x_wide = jnp.pad(xp_cur, ((0, 0), (0, 0), (0, 0), (1, 1)))
    grad_input = None
    taps = []
    for tap_row in range(3):
        tap_list = []
        for tap_col in range(3):
            window = grad_wide[
                :, 2 - tap_row : 2 - tap_row + rows, :, 2 - tap_col : 2 - tap_col + width
            ]
            term = jnp.einsum(
                "oc,bhow->bhcw",
                kernel[tap_row, tap_col],
                window,
                preferred_element_type=jnp.float32,
            )
            grad_input = term if grad_input is None else grad_input + term
            source = x_wide[:, tap_row : tap_row + rows, :, tap_col : tap_col + width]
            tap_list.append(
                jnp.einsum("bhow,bhcw->oc", grad_own, source, preferred_element_type=jnp.float32)
            )
        taps.append(jnp.stack(tap_list))
    grad_local = jnp.stack(taps)
    grad_x = grad_input.astype(jnp.bfloat16)
    group_count = lax.axis_size("dp")
    piece = grad_local.size // (height_count * group_count)
    blocks = grad_local.reshape(height_count, group_count, piece)
    shares = lax.psum_scatter(blocks, "dp", scatter_dimension=1, tiled=True)
    grad_kernel = lax.psum_scatter(shares, "height", scatter_dimension=0, tiled=True).reshape(piece)
    return (y_next, grad_x, grad_kernel)


def params(limit=None):
    return pltpu.CompilerParams(vmem_limit_bytes=limit or 40 * 1024 * 1024)


def moved(value, by):
    width = value.shape[-1]
    lane = lax.broadcasted_iota(jnp.int32, value.shape, value.ndim - 1)
    rolled = pltpu.roll(value, by % width, value.ndim - 1)
    keep = lane >= by if by > 0 else lane < width + by
    return jnp.where(keep, rolled, jnp.zeros_like(rolled))


def moved_bf16(value, by):
    return moved(value.astype(F32), by).astype(BF16)


def same_group(rows, chans):
    size = chans // GROUPS
    row = lax.broadcasted_iota(jnp.int32, (rows, rows), 0).astype(F32)
    col = lax.broadcasted_iota(jnp.int32, (rows, rows), 1).astype(F32)
    left = jnp.floor((row + 0.5) * (1.0 / size))
    right = jnp.floor((col + 0.5) * (1.0 / size))
    return jnp.where(left == right, 1.0, 0.0).astype(BF16)


def split3(value):
    high = value.astype(BF16)
    rest = value - high.astype(F32)
    mid = rest.astype(BF16)
    low = (rest - mid.astype(F32)).astype(BF16)
    return high, mid, low


def dot(left, right, dims=((1,), (0,))):
    return lax.dot_general(left, right, (dims, ((), ())), preferred_element_type=F32)


def group_total(same, value):
    column = jnp.sum(value, axis=1, keepdims=True)
    wide = jnp.broadcast_to(column, value.shape)
    high, mid, low = split3(wide)
    return dot(same, high) + (dot(same, mid) + dot(same, low))


def lane_tiles(size):
    return [(at, min(LANES, size - at)) for at in range(0, size, LANES)]


def sigmoid(value):
    return 1.0 / (1.0 + jnp.exp(-value))


def weights_kernel(w_ref, flat_ref):
    chans = flat_ref.shape[1]
    for a in range(3):
        for b in range(3):
            flat_ref[a, :, b * chans : (b + 1) * chans] = w_ref[a, b]


def halves_kernel(own_ref, near_ref, out_ref):
    half = out_ref.shape[2]
    core = lax.axis_index("height") & 1
    mine = pl.ds(pl.multiple_of(core * half, 16), half)
    for r in range(out_ref.shape[1]):
        out_ref[0, r] = own_ref[r, mine]
        out_ref[1, r] = near_ref[r, mine]


def next_conv_kernel(edge_ref, near_ref, x_ref, w_ref, z_ref, stat_ref, *, rows):
    even = (lax.axis_index("height") & 1) == 0
    side = edge_ref[...].astype(F32)
    top = jnp.where(even, side, near_ref[rows - 1].astype(F32)).astype(BF16)
    bottom = jnp.where(even, near_ref[0].astype(F32), side).astype(BF16)
    cells = [top] + [x_ref[r] for r in range(rows)] + [bottom]
    chans, width = cells[0].shape
    sides = [[moved_bf16(cell, 1) for cell in cells], cells, [moved_bf16(cell, -1) for cell in cells]]
    stacks = [jnp.concatenate([side[r] for side in sides], axis=0) for r in range(rows + 2)]
    total = None
    for a in range(3):
        term = dot(w_ref[a], jnp.concatenate(stacks[a : a + rows], axis=1))
        total = term if total is None else total + term
    parts = [total[:, r * width : (r + 1) * width] for r in range(rows)]
    for r in range(rows):
        z_ref[r] = parts[r]
    line = functools.reduce(jnp.add, parts)
    mean = jnp.sum(line, axis=1, keepdims=True) * (1.0 / (rows * width))
    off = functools.reduce(jnp.add, [(part - mean) * (part - mean) for part in parts])
    ones = jnp.ones((8, width), BF16)
    row = lax.broadcasted_iota(jnp.int32, stat_ref.shape, 0)
    packed = jnp.zeros(stat_ref.shape, F32)
    at = 0
    for value in (line, off):
        lane_sum = sum(dot(ones, part, ((1,), (1,))) for part in split3(value))
        for start, size in lane_tiles(chans):
            piece = lane_sum[:1, start : start + size]
            if size < LANES:
                piece = jnp.concatenate([piece, jnp.zeros((1, LANES - size), F32)], axis=1)
            packed = jnp.where(row == at, jnp.broadcast_to(piece, packed.shape), packed)
            at += 1
    stat_ref[...] = packed


def next_out_kernel(*refs, rows, count):
    stat_refs = refs[:-4]
    z_ref, gain_ref, shift_ref, y_ref = refs[-4:]
    chans, width = gain_ref.shape
    same = same_group(chans, chans)
    tiles = lane_tiles(chans)

    def line(value):
        at = value * len(tiles)
        cells = [
            jnp.concatenate([ref[j, at + i : at + i + 1, :size] for i, (_, size) in enumerate(tiles)], axis=1)
            for ref in stat_refs
            for j in range(ref.shape[0])
        ]
        return jnp.concatenate(cells, axis=0)

    sums = line(0)
    offs = line(1)
    each = rows * width
    total = jnp.broadcast_to(jnp.sum(sums, axis=0, keepdims=True), (width, chans))
    mean_line = sum(dot(part, same) for part in split3(total[:8])) * (1.0 / count)
    apart = sums * (1.0 / each) - mean_line[:1]
    spread = jnp.sum(offs + apart * apart * float(each), axis=0, keepdims=True)
    spread = jnp.broadcast_to(spread, (width, chans))
    mean = sum(dot(same, part, ((1,), (1,))) for part in split3(total)) * (1.0 / count)
    var = sum(dot(same, part, ((1,), (1,))) for part in split3(spread)) * (1.0 / count)
    rstd = lax.rsqrt(var + eps)
    for r in range(rows):
        affine = (z_ref[r] - mean) * rstd * gain_ref[...] + shift_ref[...]
        y_ref[r] = (affine * sigmoid(affine)).astype(BF16)


def conv_kernel(*refs, blocks, rows, count, wide):
    x_refs = refs[:blocks]
    w_ref, xs, z, norm, lane = refs[blocks:]
    image, half, width = z.shape
    chans = x_refs[0].shape[1]
    home = lax.axis_index("height")
    mine = pl.ds(pl.multiple_of((home & 1) * half, 16), half)

    edge = jnp.zeros((3 * chans, width), BF16)
    xs[0] = edge
    xs[image + 1] = edge
    for k in range(blocks):
        base = (home ^ k) * rows + 1
        for r in range(rows):
            cell = x_refs[k][r]
            xs[base + r, chans : 2 * chans] = cell
            xs[base + r, :chans] = moved_bf16(cell, 1)
            xs[base + r, 2 * chans :] = moved_bf16(cell, -1)

    def conv(p, start=False):
        row = p * wide
        total = None
        for a in range(3):
            right = jnp.concatenate([xs[row + a + i] for i in range(wide)], axis=1)
            term = dot(w_ref[a, mine], right)
            total = term if total is None else total + term
        parts = [total[:, i * width : (i + 1) * width] for i in range(wide)]
        for i in range(wide):
            z[row + i] = parts[i]
        offs = [part - (parts[0] if start else z[0]) for part in parts]
        sums = functools.reduce(jnp.add, offs)
        squares = functools.reduce(jnp.add, [off * off for off in offs])
        lane[0] = sums if start else lane[0] + sums
        lane[1] = squares if start else lane[1] + squares

    conv(0, True)
    lax.fori_loop(1, image // wide, lambda p, carry: conv(p) or carry, 0)

    same = same_group(half, chans)
    middle = lane[0] * (1.0 / image)
    spread = lane[1] - middle * lane[0]
    middle = z[0] + middle
    mean = group_total(same, middle) * (float(image) / count)
    norm[0] = mean
    apart = middle - mean
    var = group_total(same, spread + apart * apart * float(image)) * (1.0 / count)
    norm[1] = lax.rsqrt(var + eps)


def pull_kernel(*refs, blocks, rows, count):
    g_refs = refs[: blocks // 2]
    z, norm, gain_ref, shift_ref, gz_ref, gn, ns, coef = refs[blocks // 2 :]
    image, half, _ = z.shape
    chans = gain_ref.shape[0]
    home = lax.axis_index("height")
    core = home & 1
    step = 16

    def pulled(i, carry):
        start = pl.multiple_of(i * step, step)
        at = pl.ds(start, step)
        all_at = pl.ds(pl.multiple_of(core * half + start, step), step)
        mean = norm[0, at]
        rstd = norm[1, at]
        gain = gain_ref[all_at]
        shift = shift_ref[all_at]
        first = None
        second = None
        for k in range(blocks):
            base = (home ^ k) * rows
            for r in range(rows):
                n = (z[base + r, at] - mean) * rstd
                affine = n * gain + shift
                sig = sigmoid(affine)
                slope = sig * (1.0 + affine * (1.0 - sig))
                value = g_refs[k // 2][k % 2, r, at].astype(F32) * slope * gain
                gn[base + r, at] = value
                ns[base + r, at] = n
                first = value if first is None else first + value
                second = value * n if second is None else second + value * n
        coef[0, at] = first
        coef[1, at] = second
        return carry

    lax.fori_loop(0, half // step, pulled, 0)
    same = same_group(half, chans)
    coef[0] = group_total(same, coef[0]) * (1.0 / count)
    coef[1] = group_total(same, coef[1]) * (1.0 / count)

    def rounded(i, carry):
        at = pl.ds(pl.multiple_of(i * step, step), step)
        mean1 = coef[0, at]
        mean2 = coef[1, at]
        rstd = norm[1, at]
        for r in range(image):
            gz_ref[r, at] = (rstd * (gn[r, at] - mean1 - ns[r, at] * mean2)).astype(BF16)
        return carry

    lax.fori_loop(0, half // step, rounded, 0)


def filter_kernel(own_ref, other_ref, xs, *refs, blocks, rows, groups_dp, span):
    outs = refs[:groups_dp]
    gz_out, gz, taps, flat = refs[groups_dp:]
    image, half, width = own_ref.shape
    chans = 2 * half
    home = lax.axis_index("height")
    part = lax.axis_index("dp")
    core = home & 1
    step = 16

    edge = jnp.zeros((chans, width), BF16)
    gz[0] = edge
    gz[image + 1] = edge
    for r in range(image):
        gz[r + 1, pl.ds(pl.multiple_of(core * half, step), half)] = own_ref[r]
        gz[r + 1, pl.ds(pl.multiple_of((1 - core) * half, step), half)] = other_ref[r]
    for r in range(rows + 2):
        gz_out[r] = gz[home * rows + r]

    block = 9 * chans // blocks
    tap0 = (home * block) // chans
    left = jnp.concatenate([gz[r + 1] for r in range(image)], axis=1)
    for j in range(span):
        tap = jnp.minimum(tap0 + j, 8)
        a = tap // 3
        side = pl.ds(pl.multiple_of((tap - a * 3) * chans, step), chans)
        right = jnp.concatenate([xs[r + a, side] for r in range(image)], axis=1)
        rows_of = dot(left, right, ((1,), (1,)))
        for i, (start, size) in enumerate(lane_tiles(chans)):
            taps[i, j * chans : (j + 1) * chans, :size] = rows_of[:, start : start + size]

    off = pl.multiple_of(home * block - tap0 * chans, 8)
    shared = math.gcd(chans, LANES)
    few, many = LANES // shared, chans // shared
    for i in range(taps.shape[0]):
        taps[i, :block] = taps[i, pl.ds(off, block)]
    lines = jnp.concatenate(
        [
            taps[i, pl.ds(line, block // few, stride=few)][:, :size]
            for line in range(few)
            for i, (_, size) in enumerate(lane_tiles(chans))
        ],
        axis=1,
    )
    for i in range(many):
        flat[pl.ds(i, block // few, stride=many)] = lines[:, i * LANES : (i + 1) * LANES]
    piece = flat.shape[0] // groups_dp
    for s in range(groups_dp):
        dest = part ^ s
        value = flat[pl.ds(dest * piece, piece)]
        outs[s][...] = value.astype(outs[s].dtype)


def grad_x_kernel(gz_ref, w_ref, out_ref, *, rows):
    chans, width = gz_ref.shape[1:]
    total = None
    for a in range(3):
        right = jnp.concatenate([gz_ref[2 - a + r] for r in range(rows)], axis=1)
        term = dot(w_ref[a], right, ((0,), (0,)))
        total = term if total is None else total + term
    for r in range(rows):
        part = total[:, r * width : (r + 1) * width]
        value = part[chans : 2 * chans]
        value = value + moved(part[:chans], -1) + moved(part[2 * chans :], 1)
        out_ref[r] = value.astype(BF16)


def vmem(count):
    return [pl.BlockSpec(memory_space=pltpu.VMEM)] * count


def pairs(size, offset):
    return [(i, i ^ offset) for i in range(size)]


def call(kernel, out_shape, args, scratch=(), flops=0, **static):
    single = not isinstance(out_shape, tuple)
    return pl.pallas_call(
        functools.partial(kernel, **static),
        out_shape=out_shape,
        in_specs=vmem(len(args)),
        out_specs=vmem(1)[0] if single else tuple(vmem(len(out_shape))),
        scratch_shapes=list(scratch),
        compiler_params=params(),
        cost_estimate=pl.CostEstimate(flops=flops, bytes_accessed=0, transcendentals=0),
    )(*args)


def gathered(x_next, x_cur, grad_out, kernel, gamma, beta):
    rows, chans, width = x_next.shape[1:]
    blocks = lax.axis_size("height")
    groups_dp = lax.axis_size("dp")
    image = blocks * rows
    half = chans // 2
    count = image * (chans // GROUPS) * width
    block = 9 * chans // blocks
    span = max((h * block % chans + block - 1) // chans + 1 for h in range(blocks))
    piece = block * chans // (groups_dp * LANES)
    flops = 18 * chans * chans * width
    x_next, grad_out = x_next[0], grad_out[0]
    shape = jax.ShapeDtypeStruct

    def far(own):
        held = {0: own}
        for k in sorted(range(2, blocks, 2), key=lambda k: -bin(k).count("1")):
            held[k] = lax.ppermute(own, "height", pairs(blocks, k))
        return held

    def near(own):
        return lax.ppermute(own, "height", pairs(blocks, 1))

    x_far = far(x_cur[0])
    even = (lax.axis_index("height") & 1) == 0
    edge = lax.dynamic_index_in_dim(x_next, jnp.where(even, 0, rows - 1), 0, keepdims=False)
    next_near = near(x_next)
    swaps = [(i, i + 1) for i in range(1, blocks - 1, 2)]
    edge = lax.ppermute(edge, "height", swaps + [(j, i) for i, j in swaps])
    g_near = near(grad_out)
    g_pair = call(
        halves_kernel, shape((2, rows, half, width), BF16), (grad_out, g_near), flops=image * flops
    )
    g_far = far(g_pair)
    gain = jnp.broadcast_to(gamma[:, None], (chans, width))
    shift = jnp.broadcast_to(beta[:, None], (chans, width))
    w_flat = call(weights_kernel, shape((3, chans, 3 * chans), BF16), (kernel,))

    x_far, w_flat, gain, shift, _ = lax.optimization_barrier((x_far, w_flat, gain, shift, g_pair))
    x_all = []
    for k in range(0, blocks, 2):
        x_all += [x_far[k], near(x_far[k])]
    xs, z_cur, norm = call(
        conv_kernel,
        (
            shape((image + 2, 3 * chans, width), BF16),
            shape((image, half, width), F32),
            shape((2, half, width), F32),
        ),
        (*x_all, w_flat),
        scratch=(pltpu.VMEM((2, half, width), F32),),
        flops=image * flops // 2,
        blocks=blocks,
        rows=rows,
        count=count,
        wide=4 if image % 4 == 0 else 2,
    )
    gz_own = call(
        pull_kernel,
        shape((image, half, width), BF16),
        (*[g_far[k] for k in range(0, blocks, 2)], z_cur, norm, gain, shift),
        scratch=(
            pltpu.VMEM((image, half, width), F32),
            pltpu.VMEM((image, half, width), F32),
            pltpu.VMEM((2, half, width), F32),
        ),
        flops=image * flops // 8,
        blocks=blocks,
        rows=rows,
        count=count,
    )
    gz_other = near(gz_own)
    edge, gz_own = lax.optimization_barrier((edge, gz_own))
    z_next, stat = call(
        next_conv_kernel,
        (shape((rows, chans, width), F32), shape((8 * -(-2 * len(lane_tiles(chans)) // 8), LANES), F32)),
        (edge, next_near, x_next, w_flat),
        flops=rows * flops,
        rows=rows,
    )
    stat_near = near(stat)
    gz_other, z_next = lax.optimization_barrier((gz_other, z_next))
    results = call(
        filter_kernel,
        (shape((piece, LANES), F32),)
        + (shape((piece, LANES), BF16),) * (groups_dp - 1)
        + (shape((rows + 2, chans, width), BF16),),
        (gz_own, gz_other, xs),
        scratch=(
            pltpu.VMEM((image + 2, chans, width), BF16),
            pltpu.VMEM((len(lane_tiles(chans)), span * chans, LANES), F32),
            pltpu.VMEM((groups_dp * piece, LANES), F32),
        ),
        flops=image * flops // 4,
        blocks=blocks,
        rows=rows,
        groups_dp=groups_dp,
        span=span,
    )
    total = results[0]
    for s in range(groups_dp - 1, 0, -1):
        total = total + lax.ppermute(results[s], "dp", pairs(groups_dp, s)).astype(F32)
    stat_near, gz_rows = lax.optimization_barrier((stat_near, results[groups_dp]))
    stat_pair = jnp.stack((stat, stat_near))
    stat_far = far(stat_pair)
    grad_x = call(
        grad_x_kernel,
        shape((rows, chans, width), BF16),
        (gz_rows, w_flat),
        flops=rows * flops,
        rows=rows,
    )
    y_next = call(
        next_out_kernel,
        shape((rows, chans, width), BF16),
        (*stat_far.values(), z_next, gain, shift),
        flops=rows * flops // 4,
        rows=rows,
        count=count,
    )
    return (y_next[None], grad_x[None], total.reshape(piece * LANES))


def fits(shape, blocks, groups_dp):
    batch, rows, chans, width = shape
    image = blocks * rows
    scratch = image * chans * width * 20 + 9 * chans * chans * 4
    few = LANES // math.gcd(chans, LANES)
    return (
        batch == 1
        and width == LANES
        and chans % 32 == 0
        and chans % GROUPS == 0
        and GROUPS % 2 == 0
        and blocks > 1
        and image % 2 == 0
        and blocks & (blocks - 1) == 0
        and groups_dp & (groups_dp - 1) == 0
        and (9 * chans) % (8 * blocks) == 0
        and (9 * chans // blocks) % few == 0
        and (9 * chans // blocks) * chans % (groups_dp * LANES) == 0
        and scratch < 32 * 1024 * 1024
    )


def solution(mesh):
    blocks, groups_dp = mesh.shape["height"], mesh.shape["dp"]

    def local(x_next, x_cur, grad_out, kernel, gamma, beta):
        if not fits(x_next.shape, blocks, groups_dp):
            return row_sharded(x_next, x_cur, grad_out, kernel, gamma, beta)
        return gathered(x_next, x_cur, grad_out, kernel, gamma, beta)

    placed = (
        P("dp", "height", None, None),
        P("dp", "height", None, None),
        P("dp", "height", None, None),
        P(),
        P(),
        P(),
    )
    return jax.shard_map(
        local,
        mesh=mesh,
        in_specs=placed,
        out_specs=(
            P("dp", "height", None, None),
            P("dp", "height", None, None),
            P(("height", "dp")),
        ),
        check_vma=False,
    )
```

```python
import functools
import math

import jax
import jax.numpy as jnp
from jax import lax
from jax.experimental import pallas as pl
from jax.experimental.pallas import tpu as pltpu
from jax.sharding import PartitionSpec as P

GROUPS = 32

eps = 1e-05


LANES = 128
F32 = jnp.float32
BF16 = jnp.bfloat16


def extended(cells, sides, width):
    for axis, dim in sides:
        count = lax.axis_size(axis)
        ends = count - 1
        head = lax.slice_in_dim(cells, 0, width, axis=dim)
        tail = lax.slice_in_dim(cells, cells.shape[dim] - width, cells.shape[dim], axis=dim)
        cells = jnp.concatenate(
            [
                lax.ppermute(tail, axis, [(i, (i + 1) % count) for i in range(ends)]),
                cells,
                lax.ppermute(head, axis, [((i + 1) % count, i) for i in range(ends)]),
            ],
            axis=dim,
        )
    return cells


def conv_rows(padded, kernel, count):
    width = padded.shape[-1]
    wide = jnp.pad(padded, ((0, 0), (0, 0), (0, 0), (1, 1)))
    total = None
    for tap_row in range(3):
        for tap_col in range(3):
            window = wide[:, tap_row : tap_row + count, :, tap_col : tap_col + width]
            term = jnp.einsum(
                "oc,bhcw->bhow",
                kernel[tap_row, tap_col],
                window,
                preferred_element_type=jnp.float32,
            )
            total = term if total is None else total + term
    return total


def group_sum(value):
    batch, rows, chans, width = value.shape
    return jnp.sum(value.reshape(batch, rows, GROUPS, chans // GROUPS, width), axis=(1, 3, 4))


def row_sharded(x_next, x_cur, grad_out, kernel, gamma, beta):
    _, rows, chans, width = x_next.shape
    height_count = lax.axis_size("height")
    count = height_count * rows * (chans // GROUPS) * width
    gain = gamma[None, None, :, None]
    shift_b = beta[None, None, :, None]

    def expand(stat):
        return jnp.repeat(stat, chans // GROUPS, axis=1)[:, None, :, None]

    stacked = jnp.stack((x_next, x_cur))
    padded = extended(stacked, (("height", 2),), 1)
    xp_next = padded[0]
    xp_cur = padded[1]
    z_next = conv_rows(xp_next, kernel, rows)
    z_cur = conv_rows(xp_cur, kernel, rows)
    sum_next, sum_cur, sq_next, sq_cur = lax.psum(
        (group_sum(z_next), group_sum(z_cur), group_sum(z_next * z_next), group_sum(z_cur * z_cur)),
        "height",
    )
    mean_next = sum_next / count
    mean_cur = sum_cur / count
    var_next = sq_next / count - mean_next * mean_next
    var_cur = sq_cur / count - mean_cur * mean_cur
    rstd_next = lax.rsqrt(var_next + eps)
    rstd_cur = lax.rsqrt(var_cur + eps)
    affine_next = (z_next - expand(mean_next)) * expand(rstd_next) * gain + shift_b
    y_next = (affine_next * jax.nn.sigmoid(affine_next)).astype(jnp.bfloat16)
    normed = (z_cur - expand(mean_cur)) * expand(rstd_cur)
    affine = normed * gain + shift_b
    sig = jax.nn.sigmoid(affine)
    grad_n = grad_out.astype(jnp.float32) * (sig * (1.0 + affine * (1.0 - sig))) * gain
    first_sum, second_sum = lax.psum((group_sum(grad_n), group_sum(grad_n * normed)), "height")
    grad_z = (
        expand(rstd_cur)
        * (grad_n - expand(first_sum / count) - normed * expand(second_sum / count))
    ).astype(jnp.bfloat16)
    grad_pad = extended(grad_z, (("height", 1),), 1)
    grad_own = grad_pad[:, 1:-1]
    grad_wide = jnp.pad(grad_pad, ((0, 0), (0, 0), (0, 0), (1, 1)))
    x_wide = jnp.pad(xp_cur, ((0, 0), (0, 0), (0, 0), (1, 1)))
    grad_input = None
    taps = []
    for tap_row in range(3):
        tap_list = []
        for tap_col in range(3):
            window = grad_wide[
                :, 2 - tap_row : 2 - tap_row + rows, :, 2 - tap_col : 2 - tap_col + width
            ]
            term = jnp.einsum(
                "oc,bhow->bhcw",
                kernel[tap_row, tap_col],
                window,
                preferred_element_type=jnp.float32,
            )
            grad_input = term if grad_input is None else grad_input + term
            source = x_wide[:, tap_row : tap_row + rows, :, tap_col : tap_col + width]
            tap_list.append(
                jnp.einsum("bhow,bhcw->oc", grad_own, source, preferred_element_type=jnp.float32)
            )
        taps.append(jnp.stack(tap_list))
    grad_local = jnp.stack(taps)
    grad_x = grad_input.astype(jnp.bfloat16)
    group_count = lax.axis_size("dp")
    piece = grad_local.size // (height_count * group_count)
    blocks = grad_local.reshape(height_count, group_count, piece)
    shares = lax.psum_scatter(blocks, "dp", scatter_dimension=1, tiled=True)
    grad_kernel = lax.psum_scatter(shares, "height", scatter_dimension=0, tiled=True).reshape(piece)
    return (y_next, grad_x, grad_kernel)


def params(limit=None):
    return pltpu.CompilerParams(vmem_limit_bytes=limit or 40 * 1024 * 1024)


def moved(value, by):
    width = value.shape[-1]
    lane = lax.broadcasted_iota(jnp.int32, value.shape, value.ndim - 1)
    rolled = pltpu.roll(value, by % width, value.ndim - 1)
    keep = lane >= by if by > 0 else lane < width + by
    return jnp.where(keep, rolled, jnp.zeros_like(rolled))


def moved_bf16(value, by):
    return moved(value.astype(F32), by).astype(BF16)


def same_group(rows, chans):
    size = chans // GROUPS
    row = lax.broadcasted_iota(jnp.int32, (rows, rows), 0).astype(F32)
    col = lax.broadcasted_iota(jnp.int32, (rows, rows), 1).astype(F32)
    left = jnp.floor((row + 0.5) * (1.0 / size))
    right = jnp.floor((col + 0.5) * (1.0 / size))
    return jnp.where(left == right, 1.0, 0.0).astype(BF16)


def split3(value):
    high = value.astype(BF16)
    rest = value - high.astype(F32)
    mid = rest.astype(BF16)
    low = (rest - mid.astype(F32)).astype(BF16)
    return high, mid, low


def dot(left, right, dims=((1,), (0,))):
    return lax.dot_general(left, right, (dims, ((), ())), preferred_element_type=F32)


def group_total(same, value):
    column = jnp.sum(value, axis=1, keepdims=True)
    wide = jnp.broadcast_to(column, value.shape)
    high, mid, low = split3(wide)
    return dot(same, high) + (dot(same, mid) + dot(same, low))


def lane_tiles(size):
    return [(at, min(LANES, size - at)) for at in range(0, size, LANES)]


def sigmoid(value):
    return 1.0 / (1.0 + jnp.exp(-value))


def weights_kernel(w_ref, flat_ref):
    chans = flat_ref.shape[1]
    for a in range(3):
        for b in range(3):
            flat_ref[a, :, b * chans : (b + 1) * chans] = w_ref[a, b]


def edge_kernel(x_ref, edge_ref, sem):
    row = (lax.axis_index("height") & 1) * (x_ref.shape[0] - 1)
    copy = pltpu.make_async_copy(x_ref.at[row], edge_ref, sem)
    copy.start()
    copy.wait()


def halves_kernel(own_ref, near_ref, out_ref):
    half = out_ref.shape[2]
    core = lax.axis_index("height") & 1
    mine = pl.ds(pl.multiple_of(core * half, 16), half)
    for r in range(out_ref.shape[1]):
        out_ref[0, r] = own_ref[r, mine]
        out_ref[1, r] = near_ref[r, mine]


def next_conv_kernel(edge_ref, near_ref, x_ref, w_ref, z_ref, stat_ref, *, rows):
    even = (lax.axis_index("height") & 1) == 0
    side = edge_ref[...].astype(F32)
    top = jnp.where(even, side, near_ref[rows - 1].astype(F32)).astype(BF16)
    bottom = jnp.where(even, near_ref[0].astype(F32), side).astype(BF16)
    cells = [top] + [x_ref[r] for r in range(rows)] + [bottom]
    chans, width = cells[0].shape
    sides = [[moved_bf16(cell, 1) for cell in cells], cells, [moved_bf16(cell, -1) for cell in cells]]
    stacks = [jnp.concatenate([side[r] for side in sides], axis=0) for r in range(rows + 2)]
    total = None
    for a in range(3):
        term = dot(w_ref[a], jnp.concatenate(stacks[a : a + rows], axis=1))
        total = term if total is None else total + term
    parts = [total[:, r * width : (r + 1) * width] for r in range(rows)]
    for r in range(rows):
        z_ref[r] = parts[r]
    line = functools.reduce(jnp.add, parts)
    mean = jnp.sum(line, axis=1, keepdims=True) * (1.0 / (rows * width))
    off = functools.reduce(jnp.add, [(part - mean) * (part - mean) for part in parts])
    ones = jnp.ones((8, width), BF16)
    row = lax.broadcasted_iota(jnp.int32, stat_ref.shape, 0)
    packed = jnp.zeros(stat_ref.shape, F32)
    at = 0
    for value in (line, off):
        lane_sum = sum(dot(ones, part, ((1,), (1,))) for part in split3(value))
        for start, size in lane_tiles(chans):
            piece = lane_sum[:1, start : start + size]
            if size < LANES:
                piece = jnp.concatenate([piece, jnp.zeros((1, LANES - size), F32)], axis=1)
            packed = jnp.where(row == at, jnp.broadcast_to(piece, packed.shape), packed)
            at += 1
    stat_ref[...] = packed


def next_out_kernel(*refs, rows, count):
    stat_refs = refs[:-4]
    z_ref, gain_ref, shift_ref, y_ref = refs[-4:]
    chans, width = gain_ref.shape
    same = same_group(chans, chans)
    tiles = lane_tiles(chans)

    def line(value):
        at = value * len(tiles)
        cells = [
            jnp.concatenate([ref[j, at + i : at + i + 1, :size] for i, (_, size) in enumerate(tiles)], axis=1)
            for ref in stat_refs
            for j in range(ref.shape[0])
        ]
        return jnp.concatenate(cells, axis=0)

    sums = line(0)
    offs = line(1)
    each = rows * width
    total = jnp.broadcast_to(jnp.sum(sums, axis=0, keepdims=True), (width, chans))
    mean_line = sum(dot(part, same) for part in split3(total[:8])) * (1.0 / count)
    apart = sums * (1.0 / each) - mean_line[:1]
    spread = jnp.sum(offs + apart * apart * float(each), axis=0, keepdims=True)
    spread = jnp.broadcast_to(spread, (width, chans))
    mean = sum(dot(same, part, ((1,), (1,))) for part in split3(total)) * (1.0 / count)
    var = sum(dot(same, part, ((1,), (1,))) for part in split3(spread)) * (1.0 / count)
    rstd = lax.rsqrt(var + eps)
    for r in range(rows):
        affine = (z_ref[r] - mean) * rstd * gain_ref[...] + shift_ref[...]
        y_ref[r] = (affine * sigmoid(affine)).astype(BF16)


def conv_kernel(*refs, blocks, rows, count, wide):
    x_refs = refs[:blocks]
    w_ref, xs, z, norm, lane = refs[blocks:]
    image, half, width = z.shape
    chans = x_refs[0].shape[1]
    home = lax.axis_index("height")
    mine = pl.ds(pl.multiple_of((home & 1) * half, 16), half)

    edge = jnp.zeros((3 * chans, width), BF16)
    xs[0] = edge
    xs[image + 1] = edge
    for k in range(blocks):
        base = (home ^ k) * rows + 1
        for r in range(rows):
            cell = x_refs[k][r]
            xs[base + r, chans : 2 * chans] = cell
            xs[base + r, :chans] = moved_bf16(cell, 1)
            xs[base + r, 2 * chans :] = moved_bf16(cell, -1)

    def conv(p, start=False):
        row = p * wide
        total = None
        for a in range(3):
            right = jnp.concatenate([xs[row + a + i] for i in range(wide)], axis=1)
            term = dot(w_ref[a, mine], right)
            total = term if total is None else total + term
        parts = [total[:, i * width : (i + 1) * width] for i in range(wide)]
        for i in range(wide):
            z[row + i] = parts[i]
        offs = [part - (parts[0] if start else z[0]) for part in parts]
        sums = functools.reduce(jnp.add, offs)
        squares = functools.reduce(jnp.add, [off * off for off in offs])
        lane[0] = sums if start else lane[0] + sums
        lane[1] = squares if start else lane[1] + squares

    conv(0, True)
    lax.fori_loop(1, image // wide, lambda p, carry: conv(p) or carry, 0)

    same = same_group(half, chans)
    middle = lane[0] * (1.0 / image)
    spread = lane[1] - middle * lane[0]
    middle = z[0] + middle
    mean = group_total(same, middle) * (float(image) / count)
    norm[0] = mean
    apart = middle - mean
    var = group_total(same, spread + apart * apart * float(image)) * (1.0 / count)
    norm[1] = lax.rsqrt(var + eps)


def pull_kernel(*refs, blocks, rows, count):
    g_refs = refs[: blocks // 2]
    z, norm, gain_ref, shift_ref, gz_ref, gn, ns, coef = refs[blocks // 2 :]
    image, half, _ = z.shape
    chans = gain_ref.shape[0]
    home = lax.axis_index("height")
    core = home & 1
    step = 16

    def pulled(i, carry):
        start = pl.multiple_of(i * step, step)
        at = pl.ds(start, step)
        all_at = pl.ds(pl.multiple_of(core * half + start, step), step)
        mean = norm[0, at]
        rstd = norm[1, at]
        gain = gain_ref[all_at]
        shift = shift_ref[all_at]
        first = None
        second = None
        for k in range(blocks):
            base = (home ^ k) * rows
            for r in range(rows):
                n = (z[base + r, at] - mean) * rstd
                affine = n * gain + shift
                sig = sigmoid(affine)
                slope = sig * (1.0 + affine * (1.0 - sig))
                value = g_refs[k // 2][k % 2, r, at].astype(F32) * slope * gain
                gn[base + r, at] = value
                ns[base + r, at] = n
                first = value if first is None else first + value
                second = value * n if second is None else second + value * n
        coef[0, at] = first
        coef[1, at] = second
        return carry

    lax.fori_loop(0, half // step, pulled, 0)
    same = same_group(half, chans)
    coef[0] = group_total(same, coef[0]) * (1.0 / count)
    coef[1] = group_total(same, coef[1]) * (1.0 / count)

    def rounded(i, carry):
        at = pl.ds(pl.multiple_of(i * step, step), step)
        mean1 = coef[0, at]
        mean2 = coef[1, at]
        rstd = norm[1, at]
        for r in range(image):
            gz_ref[r, at] = (rstd * (gn[r, at] - mean1 - ns[r, at] * mean2)).astype(BF16)
        return carry

    lax.fori_loop(0, half // step, rounded, 0)


def filter_kernel(own_ref, other_ref, xs, *refs, blocks, rows, groups_dp, span):
    outs = refs[:groups_dp]
    gz_out, gz, taps, flat = refs[groups_dp:]
    image, half, width = own_ref.shape
    chans = 2 * half
    home = lax.axis_index("height")
    part = lax.axis_index("dp")
    core = home & 1
    step = 16

    edge = jnp.zeros((chans, width), BF16)
    gz[0] = edge
    gz[image + 1] = edge
    for r in range(image):
        gz[r + 1, pl.ds(pl.multiple_of(core * half, step), half)] = own_ref[r]
        gz[r + 1, pl.ds(pl.multiple_of((1 - core) * half, step), half)] = other_ref[r]
    for r in range(rows + 2):
        gz_out[r] = gz[home * rows + r]

    block = 9 * chans // blocks
    tap0 = (home * block) // chans
    left = jnp.concatenate([gz[r + 1] for r in range(image)], axis=1)
    for j in range(span):
        tap = jnp.minimum(tap0 + j, 8)
        a = tap // 3
        side = pl.ds(pl.multiple_of((tap - a * 3) * chans, step), chans)
        right = jnp.concatenate([xs[r + a, side] for r in range(image)], axis=1)
        rows_of = dot(left, right, ((1,), (1,)))
        for i, (start, size) in enumerate(lane_tiles(chans)):
            taps[i, j * chans : (j + 1) * chans, :size] = rows_of[:, start : start + size]

    off = pl.multiple_of(home * block - tap0 * chans, 8)
    shared = math.gcd(chans, LANES)
    few, many = LANES // shared, chans // shared
    for i in range(taps.shape[0]):
        taps[i, :block] = taps[i, pl.ds(off, block)]
    lines = jnp.concatenate(
        [
            taps[i, pl.ds(line, block // few, stride=few)][:, :size]
            for line in range(few)
            for i, (_, size) in enumerate(lane_tiles(chans))
        ],
        axis=1,
    )
    for i in range(many):
        flat[pl.ds(i, block // few, stride=many)] = lines[:, i * LANES : (i + 1) * LANES]
    piece = flat.shape[0] // groups_dp
    for s in range(groups_dp):
        dest = part ^ s
        value = flat[pl.ds(dest * piece, piece)]
        outs[s][...] = value.astype(outs[s].dtype)


def grad_x_kernel(gz_ref, w_ref, out_ref, *, rows):
    chans, width = gz_ref.shape[1:]
    total = None
    for a in range(3):
        right = jnp.concatenate([gz_ref[2 - a + r] for r in range(rows)], axis=1)
        term = dot(w_ref[a], right, ((0,), (0,)))
        total = term if total is None else total + term
    for r in range(rows):
        part = total[:, r * width : (r + 1) * width]
        value = part[chans : 2 * chans]
        value = value + moved(part[:chans], -1) + moved(part[2 * chans :], 1)
        out_ref[r] = value.astype(BF16)


def vmem(count):
    return [pl.BlockSpec(memory_space=pltpu.VMEM)] * count


def pairs(size, offset):
    return [(i, i ^ offset) for i in range(size)]


def call(kernel, out_shape, args, scratch=(), flops=0, **static):
    single = not isinstance(out_shape, tuple)
    return pl.pallas_call(
        functools.partial(kernel, **static),
        out_shape=out_shape,
        in_specs=vmem(len(args)),
        out_specs=vmem(1)[0] if single else tuple(vmem(len(out_shape))),
        scratch_shapes=list(scratch),
        compiler_params=params(),
        cost_estimate=pl.CostEstimate(flops=flops, bytes_accessed=0, transcendentals=0),
    )(*args)


def gathered(x_next, x_cur, grad_out, kernel, gamma, beta):
    rows, chans, width = x_next.shape[1:]
    blocks = lax.axis_size("height")
    groups_dp = lax.axis_size("dp")
    image = blocks * rows
    half = chans // 2
    count = image * (chans // GROUPS) * width
    block = 9 * chans // blocks
    span = max((h * block % chans + block - 1) // chans + 1 for h in range(blocks))
    piece = block * chans // (groups_dp * LANES)
    flops = 18 * chans * chans * width
    x_next, grad_out = x_next[0], grad_out[0]
    shape = jax.ShapeDtypeStruct

    chips = sorted(range(2, blocks, 2), key=lambda k: -bin(k).count("1"))
    last = chips[:1]

    def far(own, offsets):
        return {k: lax.ppermute(own, "height", pairs(blocks, k)) for k in offsets}

    def near(own):
        return lax.ppermute(own, "height", pairs(blocks, 1))

    x_far = {0: x_cur[0]} | far(x_cur[0], chips)
    edge = pl.pallas_call(
        edge_kernel,
        out_shape=shape((chans, width), BF16),
        in_specs=[pl.BlockSpec(memory_space=pltpu.HBM)],
        out_specs=vmem(1)[0],
        scratch_shapes=[pltpu.SemaphoreType.DMA],
        compiler_params=params(),
        cost_estimate=pl.CostEstimate(flops=image * flops, bytes_accessed=0, transcendentals=0),
        name="edge",
    )(pltpu.with_memory_space_constraint(x_next, pltpu.HBM))
    next_near = near(x_next)
    swaps = [(i, i + 1) for i in range(1, blocks - 1, 2)]
    edge = lax.ppermute(edge, "height", swaps + [(j, i) for i, j in swaps])
    g_near = near(grad_out)
    g_pair = call(
        halves_kernel, shape((2, rows, half, width), BF16), (grad_out, g_near), flops=image * flops
    )
    g_far = {0: g_pair} | far(g_pair, chips)
    gain = jnp.broadcast_to(gamma[:, None], (chans, width))
    shift = jnp.broadcast_to(beta[:, None], (chans, width))
    w_flat = call(weights_kernel, shape((3, chans, 3 * chans), BF16), (kernel,))

    x_far, w_flat, gain, shift, _ = lax.optimization_barrier((x_far, w_flat, gain, shift, g_pair))
    x_all = []
    for k in range(0, blocks, 2):
        x_all += [x_far[k], near(x_far[k])]
    z_next, stat = call(
        next_conv_kernel,
        (shape((rows, chans, width), F32), shape((8 * -(-2 * len(lane_tiles(chans)) // 8), LANES), F32)),
        (edge, next_near, x_next, w_flat),
        flops=rows * flops,
        rows=rows,
    )
    stat_near = near(stat)
    x_all, z_next = lax.optimization_barrier((x_all, z_next))
    xs, z_cur, norm = call(
        conv_kernel,
        (
            shape((image + 2, 3 * chans, width), BF16),
            shape((image, half, width), F32),
            shape((2, half, width), F32),
        ),
        (*x_all, w_flat),
        scratch=(pltpu.VMEM((2, half, width), F32),),
        flops=image * flops // 2,
        blocks=blocks,
        rows=rows,
        count=count,
        wide=4 if image % 4 == 0 else 2,
    )
    stat_pair = jnp.stack((stat, stat_near))
    gz_own = call(
        pull_kernel,
        shape((image, half, width), BF16),
        (*[g_far[k] for k in range(0, blocks, 2)], z_cur, norm, gain, shift),
        scratch=(
            pltpu.VMEM((image, half, width), F32),
            pltpu.VMEM((image, half, width), F32),
            pltpu.VMEM((2, half, width), F32),
        ),
        flops=image * flops // 8,
        blocks=blocks,
        rows=rows,
        count=count,
    )
    gz_other = near(gz_own)
    stat_pair, gz_own = lax.optimization_barrier((stat_pair, gz_own))
    stat_far = far(stat_pair, last)
    results = call(
        filter_kernel,
        (shape((piece, LANES), F32),)
        + (shape((piece, LANES), BF16),) * (groups_dp - 1)
        + (shape((rows + 2, chans, width), BF16),),
        (gz_own, gz_other, xs),
        scratch=(
            pltpu.VMEM((image + 2, chans, width), BF16),
            pltpu.VMEM((len(lane_tiles(chans)), span * chans, LANES), F32),
            pltpu.VMEM((groups_dp * piece, LANES), F32),
        ),
        flops=image * flops // 4,
        blocks=blocks,
        rows=rows,
        groups_dp=groups_dp,
        span=span,
    )
    total = results[0]
    for s in range(groups_dp - 1, 0, -1):
        total = total + lax.ppermute(results[s], "dp", pairs(groups_dp, s)).astype(F32)
    stat_far |= far(stat_pair, [k for k in chips if k not in last])
    grad_x = call(
        grad_x_kernel,
        shape((rows, chans, width), BF16),
        (results[groups_dp], w_flat),
        flops=rows * flops,
        rows=rows,
    )
    y_next = call(
        next_out_kernel,
        shape((rows, chans, width), BF16),
        (stat_pair, *stat_far.values(), z_next, gain, shift),
        flops=rows * flops // 4,
        rows=rows,
        count=count,
    )
    return (y_next[None], grad_x[None], total.reshape(piece * LANES))


def fits(shape, blocks, groups_dp):
    batch, rows, chans, width = shape
    image = blocks * rows
    scratch = image * chans * width * 20 + 9 * chans * chans * 4
    few = LANES // math.gcd(chans, LANES)
    return (
        batch == 1
        and width == LANES
        and chans % 32 == 0
        and chans % GROUPS == 0
        and GROUPS % 2 == 0
        and blocks > 1
        and image % 2 == 0
        and blocks & (blocks - 1) == 0
        and groups_dp & (groups_dp - 1) == 0
        and (9 * chans) % (8 * blocks) == 0
        and (9 * chans // blocks) % few == 0
        and (9 * chans // blocks) * chans % (groups_dp * LANES) == 0
        and scratch < 32 * 1024 * 1024
    )


def solution(mesh):
    blocks, groups_dp = mesh.shape["height"], mesh.shape["dp"]

    def local(x_next, x_cur, grad_out, kernel, gamma, beta):
        if not fits(x_next.shape, blocks, groups_dp):
            return row_sharded(x_next, x_cur, grad_out, kernel, gamma, beta)
        return gathered(x_next, x_cur, grad_out, kernel, gamma, beta)

    placed = (
        P("dp", "height", None, None),
        P("dp", "height", None, None),
        P("dp", "height", None, None),
        P(),
        P(),
        P(),
    )
    return jax.shard_map(
        local,
        mesh=mesh,
        in_specs=placed,
        out_specs=(
            P("dp", "height", None, None),
            P("dp", "height", None, None),
            P(("height", "dp")),
        ),
        check_vma=False,
    )
```

```python
import functools
import math

import jax
import jax.numpy as jnp
from jax import lax
from jax.experimental import pallas as pl
from jax.experimental.pallas import tpu as pltpu
from jax.sharding import PartitionSpec as P

GROUPS = 32

eps = 1e-05


LANES = 128
F32 = jnp.float32
BF16 = jnp.bfloat16


def extended(cells, sides, width):
    for axis, dim in sides:
        count = lax.axis_size(axis)
        ends = count - 1
        head = lax.slice_in_dim(cells, 0, width, axis=dim)
        tail = lax.slice_in_dim(cells, cells.shape[dim] - width, cells.shape[dim], axis=dim)
        cells = jnp.concatenate(
            [
                lax.ppermute(tail, axis, [(i, (i + 1) % count) for i in range(ends)]),
                cells,
                lax.ppermute(head, axis, [((i + 1) % count, i) for i in range(ends)]),
            ],
            axis=dim,
        )
    return cells


def conv_rows(padded, kernel, count):
    width = padded.shape[-1]
    wide = jnp.pad(padded, ((0, 0), (0, 0), (0, 0), (1, 1)))
    total = None
    for tap_row in range(3):
        for tap_col in range(3):
            window = wide[:, tap_row : tap_row + count, :, tap_col : tap_col + width]
            term = jnp.einsum(
                "oc,bhcw->bhow",
                kernel[tap_row, tap_col],
                window,
                preferred_element_type=jnp.float32,
            )
            total = term if total is None else total + term
    return total


def group_sum(value):
    batch, rows, chans, width = value.shape
    return jnp.sum(value.reshape(batch, rows, GROUPS, chans // GROUPS, width), axis=(1, 3, 4))


def row_sharded(x_next, x_cur, grad_out, kernel, gamma, beta):
    _, rows, chans, width = x_next.shape
    height_count = lax.axis_size("height")
    count = height_count * rows * (chans // GROUPS) * width
    gain = gamma[None, None, :, None]
    shift_b = beta[None, None, :, None]

    def expand(stat):
        return jnp.repeat(stat, chans // GROUPS, axis=1)[:, None, :, None]

    stacked = jnp.stack((x_next, x_cur))
    padded = extended(stacked, (("height", 2),), 1)
    xp_next = padded[0]
    xp_cur = padded[1]
    z_next = conv_rows(xp_next, kernel, rows)
    z_cur = conv_rows(xp_cur, kernel, rows)
    sum_next, sum_cur, sq_next, sq_cur = lax.psum(
        (group_sum(z_next), group_sum(z_cur), group_sum(z_next * z_next), group_sum(z_cur * z_cur)),
        "height",
    )
    mean_next = sum_next / count
    mean_cur = sum_cur / count
    var_next = sq_next / count - mean_next * mean_next
    var_cur = sq_cur / count - mean_cur * mean_cur
    rstd_next = lax.rsqrt(var_next + eps)
    rstd_cur = lax.rsqrt(var_cur + eps)
    affine_next = (z_next - expand(mean_next)) * expand(rstd_next) * gain + shift_b
    y_next = (affine_next * jax.nn.sigmoid(affine_next)).astype(jnp.bfloat16)
    normed = (z_cur - expand(mean_cur)) * expand(rstd_cur)
    affine = normed * gain + shift_b
    sig = jax.nn.sigmoid(affine)
    grad_n = grad_out.astype(jnp.float32) * (sig * (1.0 + affine * (1.0 - sig))) * gain
    first_sum, second_sum = lax.psum((group_sum(grad_n), group_sum(grad_n * normed)), "height")
    grad_z = (
        expand(rstd_cur)
        * (grad_n - expand(first_sum / count) - normed * expand(second_sum / count))
    ).astype(jnp.bfloat16)
    grad_pad = extended(grad_z, (("height", 1),), 1)
    grad_own = grad_pad[:, 1:-1]
    grad_wide = jnp.pad(grad_pad, ((0, 0), (0, 0), (0, 0), (1, 1)))
    x_wide = jnp.pad(xp_cur, ((0, 0), (0, 0), (0, 0), (1, 1)))
    grad_input = None
    taps = []
    for tap_row in range(3):
        tap_list = []
        for tap_col in range(3):
            window = grad_wide[
                :, 2 - tap_row : 2 - tap_row + rows, :, 2 - tap_col : 2 - tap_col + width
            ]
            term = jnp.einsum(
                "oc,bhow->bhcw",
                kernel[tap_row, tap_col],
                window,
                preferred_element_type=jnp.float32,
            )
            grad_input = term if grad_input is None else grad_input + term
            source = x_wide[:, tap_row : tap_row + rows, :, tap_col : tap_col + width]
            tap_list.append(
                jnp.einsum("bhow,bhcw->oc", grad_own, source, preferred_element_type=jnp.float32)
            )
        taps.append(jnp.stack(tap_list))
    grad_local = jnp.stack(taps)
    grad_x = grad_input.astype(jnp.bfloat16)
    group_count = lax.axis_size("dp")
    piece = grad_local.size // (height_count * group_count)
    blocks = grad_local.reshape(height_count, group_count, piece)
    shares = lax.psum_scatter(blocks, "dp", scatter_dimension=1, tiled=True)
    grad_kernel = lax.psum_scatter(shares, "height", scatter_dimension=0, tiled=True).reshape(piece)
    return (y_next, grad_x, grad_kernel)


def params(limit=None):
    return pltpu.CompilerParams(vmem_limit_bytes=limit or 40 * 1024 * 1024)


def moved(value, by):
    width = value.shape[-1]
    lane = lax.broadcasted_iota(jnp.int32, value.shape, value.ndim - 1)
    rolled = pltpu.roll(value, by % width, value.ndim - 1)
    keep = lane >= by if by > 0 else lane < width + by
    return jnp.where(keep, rolled, jnp.zeros_like(rolled))


def moved_bf16(value, by):
    return moved(value.astype(F32), by).astype(BF16)


def same_group(rows, chans):
    size = chans // GROUPS
    row = lax.broadcasted_iota(jnp.int32, (rows, rows), 0).astype(F32)
    col = lax.broadcasted_iota(jnp.int32, (rows, rows), 1).astype(F32)
    left = jnp.floor((row + 0.5) * (1.0 / size))
    right = jnp.floor((col + 0.5) * (1.0 / size))
    return jnp.where(left == right, 1.0, 0.0).astype(BF16)


def split3(value):
    high = value.astype(BF16)
    rest = value - high.astype(F32)
    mid = rest.astype(BF16)
    low = (rest - mid.astype(F32)).astype(BF16)
    return high, mid, low


def dot(left, right, dims=((1,), (0,))):
    return lax.dot_general(left, right, (dims, ((), ())), preferred_element_type=F32)


def group_totals(same, values, scale):
    width = values[0].shape[1]
    columns = [jnp.sum(value, axis=1, keepdims=True) * scale for value in values]
    wide = jnp.concatenate([jnp.broadcast_to(c, values[0].shape) for c in columns], axis=1)
    high, mid, low = split3(wide)
    total = dot(same, high) + (dot(same, mid) + dot(same, low))
    return [total[:, i * width : (i + 1) * width] for i in range(len(values))]


def lane_tiles(size):
    return [(at, min(LANES, size - at)) for at in range(0, size, LANES)]


def sigmoid(value):
    return 1.0 / (1.0 + jnp.exp(-value))


def weights_kernel(w_ref, flat_ref):
    chans = flat_ref.shape[1]
    for a in range(3):
        for b in range(3):
            flat_ref[a, :, b * chans : (b + 1) * chans] = w_ref[a, b]


def edge_kernel(x_ref, edge_ref, sem):
    row = (lax.axis_index("height") & 1) * (x_ref.shape[0] - 1)
    copy = pltpu.make_async_copy(x_ref.at[row], edge_ref, sem)
    copy.start()
    copy.wait()


def halves_kernel(own_ref, near_ref, out_ref):
    half = out_ref.shape[2]
    core = lax.axis_index("height") & 1
    mine = pl.ds(pl.multiple_of(core * half, 16), half)
    for r in range(out_ref.shape[1]):
        out_ref[0, r] = own_ref[r, mine]
        out_ref[1, r] = near_ref[r, mine]


def next_conv_kernel(edge_ref, near_ref, x_ref, w_ref, z_ref, stat_ref, *, rows):
    even = (lax.axis_index("height") & 1) == 0
    side = edge_ref[...].astype(F32)
    top = jnp.where(even, side, near_ref[rows - 1].astype(F32)).astype(BF16)
    bottom = jnp.where(even, near_ref[0].astype(F32), side).astype(BF16)
    cells = [top] + [x_ref[r] for r in range(rows)] + [bottom]
    chans, width = cells[0].shape
    sides = [[moved_bf16(cell, 1) for cell in cells], cells, [moved_bf16(cell, -1) for cell in cells]]
    stacks = [jnp.concatenate([side[r] for side in sides], axis=0) for r in range(rows + 2)]
    total = None
    for a in range(3):
        term = dot(w_ref[a], jnp.concatenate(stacks[a : a + rows], axis=1))
        total = term if total is None else total + term
    parts = [total[:, r * width : (r + 1) * width] for r in range(rows)]
    for r in range(rows):
        z_ref[r] = parts[r]
    line = functools.reduce(jnp.add, parts)
    mean = jnp.sum(line, axis=1, keepdims=True) * (1.0 / (rows * width))
    off = functools.reduce(jnp.add, [(part - mean) * (part - mean) for part in parts])
    ones = jnp.ones((8, width), BF16)
    row = lax.broadcasted_iota(jnp.int32, stat_ref.shape, 0)
    packed = jnp.zeros(stat_ref.shape, F32)
    at = 0
    for value in (line, off):
        lane_sum = sum(dot(ones, part, ((1,), (1,))) for part in split3(value))
        for start, size in lane_tiles(chans):
            piece = lane_sum[:1, start : start + size]
            if size < LANES:
                piece = jnp.concatenate([piece, jnp.zeros((1, LANES - size), F32)], axis=1)
            packed = jnp.where(row == at, jnp.broadcast_to(piece, packed.shape), packed)
            at += 1
    stat_ref[...] = packed


def next_out_kernel(*refs, rows, count):
    stat_refs = refs[:-4]
    z_ref, gain_ref, shift_ref, y_ref = refs[-4:]
    chans, width = gain_ref.shape
    same = same_group(chans, chans)
    tiles = lane_tiles(chans)

    def line(value):
        at = value * len(tiles)
        cells = [
            jnp.concatenate([ref[j, at + i : at + i + 1, :size] for i, (_, size) in enumerate(tiles)], axis=1)
            for ref in stat_refs
            for j in range(ref.shape[0])
        ]
        return jnp.concatenate(cells, axis=0)

    sums = line(0)
    offs = line(1)
    each = rows * width
    total = jnp.broadcast_to(jnp.sum(sums, axis=0, keepdims=True), (width, chans))
    mean_line = sum(dot(part, same) for part in split3(total[:8])) * (1.0 / count)
    apart = sums * (1.0 / each) - mean_line[:1]
    spread = jnp.sum(offs + apart * apart * float(each), axis=0, keepdims=True)
    spread = jnp.broadcast_to(spread, (width, chans))
    mean = sum(dot(same, part, ((1,), (1,))) for part in split3(total)) * (1.0 / count)
    var = sum(dot(same, part, ((1,), (1,))) for part in split3(spread)) * (1.0 / count)
    rstd = lax.rsqrt(var + eps)
    for r in range(rows):
        affine = (z_ref[r] - mean) * rstd * gain_ref[...] + shift_ref[...]
        y_ref[r] = (affine * sigmoid(affine)).astype(BF16)


def conv_kernel(*refs, blocks, rows, count, wide):
    x_refs = refs[:blocks]
    w_ref, xs, z, norm, lane = refs[blocks:]
    image, half, width = z.shape
    chans = x_refs[0].shape[1]
    home = lax.axis_index("height")
    mine = pl.ds(pl.multiple_of((home & 1) * half, 16), half)

    edge = jnp.zeros((3 * chans, width), BF16)
    xs[0] = edge
    xs[image + 1] = edge
    for k in range(blocks):
        base = (home ^ k) * rows + 1
        for r in range(rows):
            cell = x_refs[k][r]
            xs[base + r, chans : 2 * chans] = cell
            xs[base + r, :chans] = moved_bf16(cell, 1)
            xs[base + r, 2 * chans :] = moved_bf16(cell, -1)

    def conv(p, start=False):
        row = p * wide
        total = None
        for a in range(3):
            right = jnp.concatenate([xs[row + a + i] for i in range(wide)], axis=1)
            term = dot(w_ref[a, mine], right)
            total = term if total is None else total + term
        parts = [total[:, i * width : (i + 1) * width] for i in range(wide)]
        for i in range(wide):
            z[row + i] = parts[i]
        sums = functools.reduce(jnp.add, parts)
        squares = functools.reduce(jnp.add, [part * part for part in parts])
        lane[0] = sums if start else lane[0] + sums
        lane[1] = squares if start else lane[1] + squares

    conv(0, True)
    lax.fori_loop(1, image // wide, lambda p, carry: conv(p) or carry, 0)
    mean, square = group_totals(same_group(half, chans), (lane[0], lane[1]), 1.0 / count)
    norm[0] = mean
    norm[1] = lax.rsqrt(square - mean * mean + eps)


def pull_kernel(*refs, blocks, rows, count):
    g_refs = refs[: blocks // 2]
    z, norm, gain_ref, shift_ref, gz_ref, gn, ns, coef = refs[blocks // 2 :]
    image, half, _ = z.shape
    chans = gain_ref.shape[0]
    home = lax.axis_index("height")
    core = home & 1
    step = 16

    def pulled(i, carry):
        start = pl.multiple_of(i * step, step)
        at = pl.ds(start, step)
        all_at = pl.ds(pl.multiple_of(core * half + start, step), step)
        mean = norm[0, at]
        rstd = norm[1, at]
        gain = gain_ref[all_at]
        shift = shift_ref[all_at]
        first = None
        second = None
        for k in range(blocks):
            base = (home ^ k) * rows
            for r in range(rows):
                n = (z[base + r, at] - mean) * rstd
                affine = n * gain + shift
                sig = sigmoid(affine)
                slope = sig * (1.0 + affine * (1.0 - sig))
                value = g_refs[k // 2][k % 2, r, at].astype(F32) * slope * gain
                gn[base + r, at] = value
                ns[base + r, at] = n
                first = value if first is None else first + value
                second = value * n if second is None else second + value * n
        coef[0, at] = first
        coef[1, at] = second
        return carry

    lax.fori_loop(0, half // step, pulled, 0)
    coef[0], coef[1] = group_totals(same_group(half, chans), (coef[0], coef[1]), 1.0 / count)

    def rounded(i, carry):
        at = pl.ds(pl.multiple_of(i * step, step), step)
        mean1 = coef[0, at]
        mean2 = coef[1, at]
        rstd = norm[1, at]
        for r in range(image):
            gz_ref[r, at] = (rstd * (gn[r, at] - mean1 - ns[r, at] * mean2)).astype(BF16)
        return carry

    lax.fori_loop(0, half // step, rounded, 0)


def filter_kernel(own_ref, other_ref, xs, *refs, blocks, rows, groups_dp, span):
    outs = refs[:groups_dp]
    gz_out, gz, taps, flat = refs[groups_dp:]
    image, half, width = own_ref.shape
    chans = 2 * half
    home = lax.axis_index("height")
    part = lax.axis_index("dp")
    core = home & 1
    step = 16

    edge = jnp.zeros((chans, width), BF16)
    gz[0] = edge
    gz[image + 1] = edge
    for r in range(image):
        gz[r + 1, pl.ds(pl.multiple_of(core * half, step), half)] = own_ref[r]
        gz[r + 1, pl.ds(pl.multiple_of((1 - core) * half, step), half)] = other_ref[r]
    for r in range(rows + 2):
        gz_out[r] = gz[home * rows + r]

    block = 9 * chans // blocks
    tap0 = (home * block) // chans
    left = jnp.concatenate([gz[r + 1] for r in range(image)], axis=1)
    for j in range(span):
        tap = jnp.minimum(tap0 + j, 8)
        a = tap // 3
        side = pl.ds(pl.multiple_of((tap - a * 3) * chans, step), chans)
        right = jnp.concatenate([xs[r + a, side] for r in range(image)], axis=1)
        rows_of = dot(left, right, ((1,), (1,)))
        for i, (start, size) in enumerate(lane_tiles(chans)):
            taps[i, j * chans : (j + 1) * chans, :size] = rows_of[:, start : start + size]

    off = pl.multiple_of(home * block - tap0 * chans, 8)
    shared = math.gcd(chans, LANES)
    few, many = LANES // shared, chans // shared
    for i in range(taps.shape[0]):
        taps[i, :block] = taps[i, pl.ds(off, block)]
    lines = jnp.concatenate(
        [
            taps[i, pl.ds(line, block // few, stride=few)][:, :size]
            for line in range(few)
            for i, (_, size) in enumerate(lane_tiles(chans))
        ],
        axis=1,
    )
    for i in range(many):
        flat[pl.ds(i, block // few, stride=many)] = lines[:, i * LANES : (i + 1) * LANES]
    piece = flat.shape[0] // groups_dp
    for s in range(groups_dp):
        dest = part ^ s
        value = flat[pl.ds(dest * piece, piece)]
        outs[s][...] = value.astype(outs[s].dtype)


def grad_x_kernel(gz_ref, w_ref, out_ref, *, rows):
    chans, width = gz_ref.shape[1:]
    total = None
    for a in range(3):
        right = jnp.concatenate([gz_ref[2 - a + r] for r in range(rows)], axis=1)
        term = dot(w_ref[a], right, ((0,), (0,)))
        total = term if total is None else total + term
    for r in range(rows):
        part = total[:, r * width : (r + 1) * width]
        value = part[chans : 2 * chans]
        value = value + moved(part[:chans], -1) + moved(part[2 * chans :], 1)
        out_ref[r] = value.astype(BF16)


def vmem(count):
    return [pl.BlockSpec(memory_space=pltpu.VMEM)] * count


def pairs(size, offset):
    return [(i, i ^ offset) for i in range(size)]


def call(kernel, out_shape, args, scratch=(), flops=0, **static):
    single = not isinstance(out_shape, tuple)
    return pl.pallas_call(
        functools.partial(kernel, **static),
        out_shape=out_shape,
        in_specs=vmem(len(args)),
        out_specs=vmem(1)[0] if single else tuple(vmem(len(out_shape))),
        scratch_shapes=list(scratch),
        compiler_params=params(),
        cost_estimate=pl.CostEstimate(flops=flops, bytes_accessed=0, transcendentals=0),
    )(*args)


def gathered(x_next, x_cur, grad_out, kernel, gamma, beta):
    rows, chans, width = x_next.shape[1:]
    blocks = lax.axis_size("height")
    groups_dp = lax.axis_size("dp")
    image = blocks * rows
    half = chans // 2
    count = image * (chans // GROUPS) * width
    block = 9 * chans // blocks
    span = max((h * block % chans + block - 1) // chans + 1 for h in range(blocks))
    piece = block * chans // (groups_dp * LANES)
    flops = 18 * chans * chans * width
    x_next, grad_out = x_next[0], grad_out[0]
    shape = jax.ShapeDtypeStruct

    chips = sorted(range(2, blocks, 2), key=lambda k: -bin(k).count("1"))

    def far(own, offsets):
        return {k: lax.ppermute(own, "height", pairs(blocks, k)) for k in offsets}

    def near(own):
        return lax.ppermute(own, "height", pairs(blocks, 1))

    x_far = {0: x_cur[0]} | far(x_cur[0], chips)
    edge = pl.pallas_call(
        edge_kernel,
        out_shape=shape((chans, width), BF16),
        in_specs=[pl.BlockSpec(memory_space=pltpu.HBM)],
        out_specs=vmem(1)[0],
        scratch_shapes=[pltpu.SemaphoreType.DMA],
        compiler_params=params(),
        cost_estimate=pl.CostEstimate(flops=image * flops, bytes_accessed=0, transcendentals=0),
        name="edge",
    )(pltpu.with_memory_space_constraint(x_next, pltpu.HBM))
    next_near = near(x_next)
    swaps = [(i, i + 1) for i in range(1, blocks - 1, 2)]
    edge = lax.ppermute(edge, "height", swaps + [(j, i) for i, j in swaps])
    g_near = near(grad_out)
    g_pair = call(
        halves_kernel, shape((2, rows, half, width), BF16), (grad_out, g_near), flops=image * flops
    )
    g_far = {0: g_pair} | far(g_pair, chips)
    gain = jnp.broadcast_to(gamma[:, None], (chans, width))
    shift = jnp.broadcast_to(beta[:, None], (chans, width))
    w_flat = call(weights_kernel, shape((3, chans, 3 * chans), BF16), (kernel,))

    x_far, w_flat, gain, shift, _ = lax.optimization_barrier((x_far, w_flat, gain, shift, g_pair))
    x_all = []
    for k in range(0, blocks, 2):
        x_all += [x_far[k], near(x_far[k])]
    z_next, stat = call(
        next_conv_kernel,
        (shape((rows, chans, width), F32), shape((8 * -(-2 * len(lane_tiles(chans)) // 8), LANES), F32)),
        (edge, next_near, x_next, w_flat),
        flops=rows * flops,
        rows=rows,
    )
    stat_near = near(stat)
    x_all, z_next = lax.optimization_barrier((x_all, z_next))
    xs, z_cur, norm = call(
        conv_kernel,
        (
            shape((image + 2, 3 * chans, width), BF16),
            shape((image, half, width), F32),
            shape((2, half, width), F32),
        ),
        (*x_all, w_flat),
        scratch=(pltpu.VMEM((2, half, width), F32),),
        flops=image * flops // 2,
        blocks=blocks,
        rows=rows,
        count=count,
        wide=4 if image % 4 == 0 else 2,
    )
    stat_pair = jnp.stack((stat, stat_near))
    gz_own = call(
        pull_kernel,
        shape((image, half, width), BF16),
        (*[g_far[k] for k in range(0, blocks, 2)], z_cur, norm, gain, shift),
        scratch=(
            pltpu.VMEM((image, half, width), F32),
            pltpu.VMEM((image, half, width), F32),
            pltpu.VMEM((2, half, width), F32),
        ),
        flops=image * flops // 8,
        blocks=blocks,
        rows=rows,
        count=count,
    )
    gz_other = near(gz_own)
    stat_pair, gz_own = lax.optimization_barrier((stat_pair, gz_own))
    stat_far = far(stat_pair, chips)
    results = call(
        filter_kernel,
        (shape((piece, LANES), F32),)
        + (shape((piece, LANES), BF16),) * (groups_dp - 1)
        + (shape((rows + 2, chans, width), BF16),),
        (gz_own, gz_other, xs),
        scratch=(
            pltpu.VMEM((image + 2, chans, width), BF16),
            pltpu.VMEM((len(lane_tiles(chans)), span * chans, LANES), F32),
            pltpu.VMEM((groups_dp * piece, LANES), F32),
        ),
        flops=image * flops // 4,
        blocks=blocks,
        rows=rows,
        groups_dp=groups_dp,
        span=span,
    )
    total = results[0]
    for s in range(groups_dp - 1, 0, -1):
        total = total + lax.ppermute(results[s], "dp", pairs(groups_dp, s)).astype(F32)
    grad_x = call(
        grad_x_kernel,
        shape((rows, chans, width), BF16),
        (results[groups_dp], w_flat),
        flops=rows * flops,
        rows=rows,
    )
    y_next = call(
        next_out_kernel,
        shape((rows, chans, width), BF16),
        (stat_pair, *stat_far.values(), z_next, gain, shift),
        flops=rows * flops // 4,
        rows=rows,
        count=count,
    )
    return (y_next[None], grad_x[None], total.reshape(piece * LANES))


def fits(shape, blocks, groups_dp):
    batch, rows, chans, width = shape
    image = blocks * rows
    scratch = image * chans * width * 20 + 9 * chans * chans * 4
    few = LANES // math.gcd(chans, LANES)
    return (
        batch == 1
        and width == LANES
        and chans % 32 == 0
        and chans % GROUPS == 0
        and GROUPS % 2 == 0
        and blocks > 1
        and image % 2 == 0
        and blocks & (blocks - 1) == 0
        and groups_dp & (groups_dp - 1) == 0
        and (9 * chans) % (8 * blocks) == 0
        and (9 * chans // blocks) % few == 0
        and (9 * chans // blocks) * chans % (groups_dp * LANES) == 0
        and scratch < 32 * 1024 * 1024
    )


def solution(mesh):
    blocks, groups_dp = mesh.shape["height"], mesh.shape["dp"]

    def local(x_next, x_cur, grad_out, kernel, gamma, beta):
        if not fits(x_next.shape, blocks, groups_dp):
            return row_sharded(x_next, x_cur, grad_out, kernel, gamma, beta)
        return gathered(x_next, x_cur, grad_out, kernel, gamma, beta)

    placed = (
        P("dp", "height", None, None),
        P("dp", "height", None, None),
        P("dp", "height", None, None),
        P(),
        P(),
        P(),
    )
    return jax.shard_map(
        local,
        mesh=mesh,
        in_specs=placed,
        out_specs=(
            P("dp", "height", None, None),
            P("dp", "height", None, None),
            P(("height", "dp")),
        ),
        check_vma=False,
    )
```

```python
import functools
import math

import jax
import jax.numpy as jnp
from jax import lax
from jax.experimental import pallas as pl
from jax.experimental.pallas import tpu as pltpu
from jax.sharding import PartitionSpec as P

GROUPS = 32

eps = 1e-05


LANES = 128
F32 = jnp.float32
BF16 = jnp.bfloat16


def extended(cells, sides, width):
    for axis, dim in sides:
        count = lax.axis_size(axis)
        ends = count - 1
        head = lax.slice_in_dim(cells, 0, width, axis=dim)
        tail = lax.slice_in_dim(cells, cells.shape[dim] - width, cells.shape[dim], axis=dim)
        cells = jnp.concatenate(
            [
                lax.ppermute(tail, axis, [(i, (i + 1) % count) for i in range(ends)]),
                cells,
                lax.ppermute(head, axis, [((i + 1) % count, i) for i in range(ends)]),
            ],
            axis=dim,
        )
    return cells


def conv_rows(padded, kernel, count):
    width = padded.shape[-1]
    wide = jnp.pad(padded, ((0, 0), (0, 0), (0, 0), (1, 1)))
    total = None
    for tap_row in range(3):
        for tap_col in range(3):
            window = wide[:, tap_row : tap_row + count, :, tap_col : tap_col + width]
            term = jnp.einsum(
                "oc,bhcw->bhow",
                kernel[tap_row, tap_col],
                window,
                preferred_element_type=jnp.float32,
            )
            total = term if total is None else total + term
    return total


def group_sum(value):
    batch, rows, chans, width = value.shape
    return jnp.sum(value.reshape(batch, rows, GROUPS, chans // GROUPS, width), axis=(1, 3, 4))


def row_sharded(x_next, x_cur, grad_out, kernel, gamma, beta):
    _, rows, chans, width = x_next.shape
    height_count = lax.axis_size("height")
    count = height_count * rows * (chans // GROUPS) * width
    gain = gamma[None, None, :, None]
    shift_b = beta[None, None, :, None]

    def expand(stat):
        return jnp.repeat(stat, chans // GROUPS, axis=1)[:, None, :, None]

    stacked = jnp.stack((x_next, x_cur))
    padded = extended(stacked, (("height", 2),), 1)
    xp_next = padded[0]
    xp_cur = padded[1]
    z_next = conv_rows(xp_next, kernel, rows)
    z_cur = conv_rows(xp_cur, kernel, rows)
    sum_next, sum_cur, sq_next, sq_cur = lax.psum(
        (group_sum(z_next), group_sum(z_cur), group_sum(z_next * z_next), group_sum(z_cur * z_cur)),
        "height",
    )
    mean_next = sum_next / count
    mean_cur = sum_cur / count
    var_next = sq_next / count - mean_next * mean_next
    var_cur = sq_cur / count - mean_cur * mean_cur
    rstd_next = lax.rsqrt(var_next + eps)
    rstd_cur = lax.rsqrt(var_cur + eps)
    affine_next = (z_next - expand(mean_next)) * expand(rstd_next) * gain + shift_b
    y_next = (affine_next * jax.nn.sigmoid(affine_next)).astype(jnp.bfloat16)
    normed = (z_cur - expand(mean_cur)) * expand(rstd_cur)
    affine = normed * gain + shift_b
    sig = jax.nn.sigmoid(affine)
    grad_n = grad_out.astype(jnp.float32) * (sig * (1.0 + affine * (1.0 - sig))) * gain
    first_sum, second_sum = lax.psum((group_sum(grad_n), group_sum(grad_n * normed)), "height")
    grad_z = (
        expand(rstd_cur)
        * (grad_n - expand(first_sum / count) - normed * expand(second_sum / count))
    ).astype(jnp.bfloat16)
    grad_pad = extended(grad_z, (("height", 1),), 1)
    grad_own = grad_pad[:, 1:-1]
    grad_wide = jnp.pad(grad_pad, ((0, 0), (0, 0), (0, 0), (1, 1)))
    x_wide = jnp.pad(xp_cur, ((0, 0), (0, 0), (0, 0), (1, 1)))
    grad_input = None
    taps = []
    for tap_row in range(3):
        tap_list = []
        for tap_col in range(3):
            window = grad_wide[
                :, 2 - tap_row : 2 - tap_row + rows, :, 2 - tap_col : 2 - tap_col + width
            ]
            term = jnp.einsum(
                "oc,bhow->bhcw",
                kernel[tap_row, tap_col],
                window,
                preferred_element_type=jnp.float32,
            )
            grad_input = term if grad_input is None else grad_input + term
            source = x_wide[:, tap_row : tap_row + rows, :, tap_col : tap_col + width]
            tap_list.append(
                jnp.einsum("bhow,bhcw->oc", grad_own, source, preferred_element_type=jnp.float32)
            )
        taps.append(jnp.stack(tap_list))
    grad_local = jnp.stack(taps)
    grad_x = grad_input.astype(jnp.bfloat16)
    group_count = lax.axis_size("dp")
    piece = grad_local.size // (height_count * group_count)
    blocks = grad_local.reshape(height_count, group_count, piece)
    shares = lax.psum_scatter(blocks, "dp", scatter_dimension=1, tiled=True)
    grad_kernel = lax.psum_scatter(shares, "height", scatter_dimension=0, tiled=True).reshape(piece)
    return (y_next, grad_x, grad_kernel)


def params(limit=None):
    return pltpu.CompilerParams(vmem_limit_bytes=limit or 40 * 1024 * 1024)


def moved(value, by):
    width = value.shape[-1]
    lane = lax.broadcasted_iota(jnp.int32, value.shape, value.ndim - 1)
    rolled = pltpu.roll(value, by % width, value.ndim - 1)
    keep = lane >= by if by > 0 else lane < width + by
    return jnp.where(keep, rolled, jnp.zeros_like(rolled))


def moved_bf16(value, by):
    return moved(value.astype(F32), by).astype(BF16)


def same_group(rows, chans):
    size = chans // GROUPS
    row = lax.broadcasted_iota(jnp.int32, (rows, rows), 0).astype(F32)
    col = lax.broadcasted_iota(jnp.int32, (rows, rows), 1).astype(F32)
    left = jnp.floor((row + 0.5) * (1.0 / size))
    right = jnp.floor((col + 0.5) * (1.0 / size))
    return jnp.where(left == right, 1.0, 0.0).astype(BF16)


def split3(value):
    high = value.astype(BF16)
    rest = value - high.astype(F32)
    mid = rest.astype(BF16)
    low = (rest - mid.astype(F32)).astype(BF16)
    return high, mid, low


def dot(left, right, dims=((1,), (0,))):
    return lax.dot_general(left, right, (dims, ((), ())), preferred_element_type=F32)


def group_totals(same, values, scale):
    width = values[0].shape[1]
    columns = [jnp.sum(value, axis=1, keepdims=True) * scale for value in values]
    wide = jnp.concatenate([jnp.broadcast_to(c, values[0].shape) for c in columns], axis=1)
    high, mid, low = split3(wide)
    total = dot(same, high) + (dot(same, mid) + dot(same, low))
    return [total[:, i * width : (i + 1) * width] for i in range(len(values))]


def lane_tiles(size):
    return [(at, min(LANES, size - at)) for at in range(0, size, LANES)]


def sigmoid(value):
    return 1.0 / (1.0 + jnp.exp(-value))


def weights_kernel(w_ref, flat_ref):
    chans = flat_ref.shape[1]
    for a in range(3):
        for b in range(3):
            flat_ref[a, :, b * chans : (b + 1) * chans] = w_ref[a, b]


def edge_kernel(x_ref, edge_ref, sem):
    row = (lax.axis_index("height") & 1) * (x_ref.shape[0] - 1)
    copy = pltpu.make_async_copy(x_ref.at[row], edge_ref, sem)
    copy.start()
    copy.wait()


def halves_kernel(own_ref, near_ref, out_ref):
    half = out_ref.shape[2]
    core = lax.axis_index("height") & 1
    mine = pl.ds(pl.multiple_of(core * half, 16), half)
    for r in range(out_ref.shape[1]):
        out_ref[0, r] = own_ref[r, mine]
        out_ref[1, r] = near_ref[r, mine]


def next_conv_kernel(edge_ref, near_ref, x_ref, w_ref, z_ref, stat_ref, *, rows):
    even = (lax.axis_index("height") & 1) == 0
    side = edge_ref[...].astype(F32)
    top = jnp.where(even, side, near_ref[rows - 1].astype(F32)).astype(BF16)
    bottom = jnp.where(even, near_ref[0].astype(F32), side).astype(BF16)
    cells = [top] + [x_ref[r] for r in range(rows)] + [bottom]
    chans, width = cells[0].shape
    sides = [[moved_bf16(cell, 1) for cell in cells], cells, [moved_bf16(cell, -1) for cell in cells]]
    stacks = [jnp.concatenate([side[r] for side in sides], axis=0) for r in range(rows + 2)]
    total = None
    for a in range(3):
        term = dot(w_ref[a], jnp.concatenate(stacks[a : a + rows], axis=1))
        total = term if total is None else total + term
    parts = [total[:, r * width : (r + 1) * width] for r in range(rows)]
    for r in range(rows):
        z_ref[r] = parts[r]
    line = functools.reduce(jnp.add, parts)
    mean = jnp.sum(line, axis=1, keepdims=True) * (1.0 / (rows * width))
    off = functools.reduce(jnp.add, [(part - mean) * (part - mean) for part in parts])
    ones = jnp.ones((8, width), BF16)
    row = lax.broadcasted_iota(jnp.int32, stat_ref.shape, 0)
    packed = jnp.zeros(stat_ref.shape, F32)
    at = 0
    for value in (line, off):
        lane_sum = sum(dot(ones, part, ((1,), (1,))) for part in split3(value))
        for start, size in lane_tiles(chans):
            piece = lane_sum[:1, start : start + size]
            if size < LANES:
                piece = jnp.concatenate([piece, jnp.zeros((1, LANES - size), F32)], axis=1)
            packed = jnp.where(row == at, jnp.broadcast_to(piece, packed.shape), packed)
            at += 1
    stat_ref[...] = packed


def next_out_kernel(*refs, rows, count):
    stat_refs = refs[:-4]
    z_ref, gain_ref, shift_ref, y_ref = refs[-4:]
    chans, width = gain_ref.shape
    same = same_group(chans, chans)
    tiles = lane_tiles(chans)

    def line(value):
        at = value * len(tiles)
        cells = [
            jnp.concatenate([ref[j, at + i : at + i + 1, :size] for i, (_, size) in enumerate(tiles)], axis=1)
            for ref in stat_refs
            for j in range(ref.shape[0])
        ]
        return jnp.concatenate(cells, axis=0)

    sums = line(0)
    offs = line(1)
    each = rows * width
    total = jnp.broadcast_to(jnp.sum(sums, axis=0, keepdims=True), (width, chans))
    mean_line = sum(dot(part, same) for part in split3(total[:8])) * (1.0 / count)
    apart = sums * (1.0 / each) - mean_line[:1]
    spread = jnp.sum(offs + apart * apart * float(each), axis=0, keepdims=True)
    spread = jnp.broadcast_to(spread, (width, chans))
    mean = sum(dot(same, part, ((1,), (1,))) for part in split3(total)) * (1.0 / count)
    var = sum(dot(same, part, ((1,), (1,))) for part in split3(spread)) * (1.0 / count)
    rstd = lax.rsqrt(var + eps)
    for r in range(rows):
        affine = (z_ref[r] - mean) * rstd * gain_ref[...] + shift_ref[...]
        y_ref[r] = (affine * sigmoid(affine)).astype(BF16)


def conv_kernel(*refs, blocks, rows, count, wide):
    x_refs = refs[:blocks]
    w_ref, xs, z, norm, lane = refs[blocks:]
    image, half, width = z.shape
    chans = x_refs[0].shape[1]
    home = lax.axis_index("height")
    mine = pl.ds(pl.multiple_of((home & 1) * half, 16), half)

    edge = jnp.zeros((3 * chans, width), BF16)
    xs[0] = edge
    xs[image + 1] = edge
    for k in range(blocks):
        base = (home ^ k) * rows + 1
        for r in range(rows):
            cell = x_refs[k][r]
            xs[base + r, chans : 2 * chans] = cell
            xs[base + r, :chans] = moved_bf16(cell, 1)
            xs[base + r, 2 * chans :] = moved_bf16(cell, -1)

    def conv(p, start=False):
        row = p * wide
        total = None
        for a in range(3):
            right = jnp.concatenate([xs[row + a + i] for i in range(wide)], axis=1)
            term = dot(w_ref[a, mine], right)
            total = term if total is None else total + term
        parts = [total[:, i * width : (i + 1) * width] for i in range(wide)]
        for i in range(wide):
            z[row + i] = parts[i]
        sums = functools.reduce(jnp.add, parts)
        squares = functools.reduce(jnp.add, [part * part for part in parts])
        lane[0] = sums if start else lane[0] + sums
        lane[1] = squares if start else lane[1] + squares

    conv(0, True)
    lax.fori_loop(1, image // wide, lambda p, carry: conv(p) or carry, 0)
    mean, square = group_totals(same_group(half, chans), (lane[0], lane[1]), 1.0 / count)
    norm[0] = mean
    norm[1] = lax.rsqrt(square - mean * mean + eps)


def pull_kernel(*refs, blocks, rows, count):
    g_refs = refs[: blocks // 2]
    z, norm, gain_ref, shift_ref, gz_ref, gn, ns, coef = refs[blocks // 2 :]
    image, half, _ = z.shape
    chans = gain_ref.shape[0]
    home = lax.axis_index("height")
    core = home & 1
    step = 16

    def pulled(i, carry):
        start = pl.multiple_of(i * step, step)
        at = pl.ds(start, step)
        all_at = pl.ds(pl.multiple_of(core * half + start, step), step)
        mean = norm[0, at]
        rstd = norm[1, at]
        gain = gain_ref[all_at]
        shift = shift_ref[all_at]
        first = None
        second = None
        for k in range(blocks):
            base = (home ^ k) * rows
            for r in range(rows):
                n = (z[base + r, at] - mean) * rstd
                affine = n * gain + shift
                sig = sigmoid(affine)
                slope = sig * (1.0 + affine * (1.0 - sig))
                value = g_refs[k // 2][k % 2, r, at].astype(F32) * slope * gain
                gn[base + r, at] = value
                ns[base + r, at] = n
                first = value if first is None else first + value
                second = value * n if second is None else second + value * n
        coef[0, at] = first
        coef[1, at] = second
        return carry

    lax.fori_loop(0, half // step, pulled, 0)
    coef[0], coef[1] = group_totals(same_group(half, chans), (coef[0], coef[1]), 1.0 / count)

    def rounded(i, carry):
        at = pl.ds(pl.multiple_of(i * step, step), step)
        mean1 = coef[0, at]
        mean2 = coef[1, at]
        rstd = norm[1, at]
        for r in range(image):
            gz_ref[r, at] = (rstd * (gn[r, at] - mean1 - ns[r, at] * mean2)).astype(BF16)
        return carry

    lax.fori_loop(0, half // step, rounded, 0)


def filter_kernel(own_ref, other_ref, xs, *refs, blocks, rows, groups_dp, span):
    outs = refs[:groups_dp]
    gz_out, gz, taps, flat = refs[groups_dp:]
    image, half, width = own_ref.shape
    chans = 2 * half
    home = lax.axis_index("height")
    part = lax.axis_index("dp")
    core = home & 1
    step = 16

    edge = jnp.zeros((chans, width), BF16)
    gz[0] = edge
    gz[image + 1] = edge
    for r in range(image):
        gz[r + 1, pl.ds(pl.multiple_of(core * half, step), half)] = own_ref[r]
        gz[r + 1, pl.ds(pl.multiple_of((1 - core) * half, step), half)] = other_ref[r]
    for r in range(rows + 2):
        gz_out[r] = gz[home * rows + r]

    block = 9 * chans // blocks
    unit0 = (home * block) // half
    for j in range(span):
        unit = jnp.minimum(unit0 + j, 17)
        tap = unit // 2
        a = tap // 3
        these = pl.ds(pl.multiple_of((unit - tap * 2) * half, step), half)
        side = pl.ds(pl.multiple_of((tap - a * 3) * chans, step), chans)
        left = jnp.concatenate([gz[r + 1, these] for r in range(image)], axis=1)
        right = jnp.concatenate([xs[r + a, side] for r in range(image)], axis=1)
        rows_of = dot(left, right, ((1,), (1,)))
        for i, (start, size) in enumerate(lane_tiles(chans)):
            taps[i, j * half : (j + 1) * half, :size] = rows_of[:, start : start + size]

    off = pl.multiple_of(home * block - unit0 * half, 8)
    shared = math.gcd(chans, LANES)
    few, many = LANES // shared, chans // shared
    for i in range(taps.shape[0]):
        taps[i, :block] = taps[i, pl.ds(off, block)]
    lines = jnp.concatenate(
        [
            taps[i, pl.ds(line, block // few, stride=few)][:, :size]
            for line in range(few)
            for i, (_, size) in enumerate(lane_tiles(chans))
        ],
        axis=1,
    )
    for i in range(many):
        flat[pl.ds(i, block // few, stride=many)] = lines[:, i * LANES : (i + 1) * LANES]
    piece = flat.shape[0] // groups_dp
    for s in range(groups_dp):
        dest = part ^ s
        value = flat[pl.ds(dest * piece, piece)]
        outs[s][...] = value.astype(outs[s].dtype)


def grad_x_kernel(gz_ref, w_ref, out_ref, *, rows):
    chans, width = gz_ref.shape[1:]
    total = None
    for a in range(3):
        right = jnp.concatenate([gz_ref[2 - a + r] for r in range(rows)], axis=1)
        term = dot(w_ref[a], right, ((0,), (0,)))
        total = term if total is None else total + term
    for r in range(rows):
        part = total[:, r * width : (r + 1) * width]
        value = part[chans : 2 * chans]
        value = value + moved(part[:chans], -1) + moved(part[2 * chans :], 1)
        out_ref[r] = value.astype(BF16)


def vmem(count):
    return [pl.BlockSpec(memory_space=pltpu.VMEM)] * count


def pairs(size, offset):
    return [(i, i ^ offset) for i in range(size)]


def call(kernel, out_shape, args, scratch=(), flops=0, **static):
    single = not isinstance(out_shape, tuple)
    return pl.pallas_call(
        functools.partial(kernel, **static),
        out_shape=out_shape,
        in_specs=vmem(len(args)),
        out_specs=vmem(1)[0] if single else tuple(vmem(len(out_shape))),
        scratch_shapes=list(scratch),
        compiler_params=params(),
        cost_estimate=pl.CostEstimate(flops=flops, bytes_accessed=0, transcendentals=0),
    )(*args)


def gathered(x_next, x_cur, grad_out, kernel, gamma, beta):
    rows, chans, width = x_next.shape[1:]
    blocks = lax.axis_size("height")
    groups_dp = lax.axis_size("dp")
    image = blocks * rows
    half = chans // 2
    count = image * (chans // GROUPS) * width
    block = 9 * chans // blocks
    span = max((h * block % half + block - 1) // half + 1 for h in range(blocks))
    piece = block * chans // (groups_dp * LANES)
    flops = 18 * chans * chans * width
    x_next, grad_out = x_next[0], grad_out[0]
    shape = jax.ShapeDtypeStruct

    chips = sorted(range(2, blocks, 2), key=lambda k: -bin(k).count("1"))

    def far(own, offsets):
        return {k: lax.ppermute(own, "height", pairs(blocks, k)) for k in offsets}

    def near(own):
        return lax.ppermute(own, "height", pairs(blocks, 1))

    x_far = {0: x_cur[0]} | far(x_cur[0], chips)
    edge = pl.pallas_call(
        edge_kernel,
        out_shape=shape((chans, width), BF16),
        in_specs=[pl.BlockSpec(memory_space=pltpu.HBM)],
        out_specs=vmem(1)[0],
        scratch_shapes=[pltpu.SemaphoreType.DMA],
        compiler_params=params(),
        cost_estimate=pl.CostEstimate(flops=image * flops, bytes_accessed=0, transcendentals=0),
        name="edge",
    )(pltpu.with_memory_space_constraint(x_next, pltpu.HBM))
    next_near = near(x_next)
    swaps = [(i, i + 1) for i in range(1, blocks - 1, 2)]
    edge = lax.ppermute(edge, "height", swaps + [(j, i) for i, j in swaps])
    g_near = near(grad_out)
    g_pair = call(
        halves_kernel, shape((2, rows, half, width), BF16), (grad_out, g_near), flops=image * flops
    )
    g_far = {0: g_pair} | far(g_pair, chips)
    gain = jnp.broadcast_to(gamma[:, None], (chans, width))
    shift = jnp.broadcast_to(beta[:, None], (chans, width))
    w_flat = call(weights_kernel, shape((3, chans, 3 * chans), BF16), (kernel,))

    x_far, w_flat, gain, shift, _ = lax.optimization_barrier((x_far, w_flat, gain, shift, g_pair))
    x_all = []
    for k in range(0, blocks, 2):
        x_all += [x_far[k], near(x_far[k])]
    z_next, stat = call(
        next_conv_kernel,
        (shape((rows, chans, width), F32), shape((8 * -(-2 * len(lane_tiles(chans)) // 8), LANES), F32)),
        (edge, next_near, x_next, w_flat),
        flops=rows * flops,
        rows=rows,
    )
    stat_near = near(stat)
    x_all, z_next = lax.optimization_barrier((x_all, z_next))
    xs, z_cur, norm = call(
        conv_kernel,
        (
            shape((image + 2, 3 * chans, width), BF16),
            shape((image, half, width), F32),
            shape((2, half, width), F32),
        ),
        (*x_all, w_flat),
        scratch=(pltpu.VMEM((2, half, width), F32),),
        flops=image * flops // 2,
        blocks=blocks,
        rows=rows,
        count=count,
        wide=4 if image % 4 == 0 else 2,
    )
    stat_pair = jnp.stack((stat, stat_near))
    stat_pair, norm = lax.optimization_barrier((stat_pair, norm))
    stat_far = far(stat_pair, chips[:1])
    gz_own = call(
        pull_kernel,
        shape((image, half, width), BF16),
        (*[g_far[k] for k in range(0, blocks, 2)], z_cur, norm, gain, shift),
        scratch=(
            pltpu.VMEM((image, half, width), F32),
            pltpu.VMEM((image, half, width), F32),
            pltpu.VMEM((2, half, width), F32),
        ),
        flops=image * flops // 8,
        blocks=blocks,
        rows=rows,
        count=count,
    )
    gz_other = near(gz_own)
    stat_rest, gz_own = lax.optimization_barrier((stat_pair, gz_own))
    stat_far |= far(stat_rest, chips[1:])
    results = call(
        filter_kernel,
        (shape((piece, LANES), F32),)
        + (shape((piece, LANES), BF16),) * (groups_dp - 1)
        + (shape((rows + 2, chans, width), BF16),),
        (gz_own, gz_other, xs),
        scratch=(
            pltpu.VMEM((image + 2, chans, width), BF16),
            pltpu.VMEM((len(lane_tiles(chans)), span * half, LANES), F32),
            pltpu.VMEM((groups_dp * piece, LANES), F32),
        ),
        flops=image * flops // 4,
        blocks=blocks,
        rows=rows,
        groups_dp=groups_dp,
        span=span,
    )
    total = results[0]
    for s in range(groups_dp - 1, 0, -1):
        total = total + lax.ppermute(results[s], "dp", pairs(groups_dp, s)).astype(F32)
    grad_x = call(
        grad_x_kernel,
        shape((rows, chans, width), BF16),
        (results[groups_dp], w_flat),
        flops=rows * flops,
        rows=rows,
    )
    y_next = call(
        next_out_kernel,
        shape((rows, chans, width), BF16),
        (stat_pair, *stat_far.values(), z_next, gain, shift),
        flops=rows * flops // 4,
        rows=rows,
        count=count,
    )
    return (y_next[None], grad_x[None], total.reshape(piece * LANES))


def fits(shape, blocks, groups_dp):
    batch, rows, chans, width = shape
    image = blocks * rows
    scratch = image * chans * width * 20 + 9 * chans * chans * 4
    few = LANES // math.gcd(chans, LANES)
    return (
        batch == 1
        and width == LANES
        and chans % 32 == 0
        and chans % GROUPS == 0
        and GROUPS % 2 == 0
        and blocks > 1
        and image % 2 == 0
        and blocks & (blocks - 1) == 0
        and groups_dp & (groups_dp - 1) == 0
        and (9 * chans) % (8 * blocks) == 0
        and (9 * chans // blocks) % few == 0
        and (9 * chans // blocks) * chans % (groups_dp * LANES) == 0
        and scratch < 32 * 1024 * 1024
    )


def solution(mesh):
    blocks, groups_dp = mesh.shape["height"], mesh.shape["dp"]

    def local(x_next, x_cur, grad_out, kernel, gamma, beta):
        if not fits(x_next.shape, blocks, groups_dp):
            return row_sharded(x_next, x_cur, grad_out, kernel, gamma, beta)
        return gathered(x_next, x_cur, grad_out, kernel, gamma, beta)

    placed = (
        P("dp", "height", None, None),
        P("dp", "height", None, None),
        P("dp", "height", None, None),
        P(),
        P(),
        P(),
    )
    return jax.shard_map(
        local,
        mesh=mesh,
        in_specs=placed,
        out_specs=(
            P("dp", "height", None, None),
            P("dp", "height", None, None),
            P(("height", "dp")),
        ),
        check_vma=False,
    )
```

```python
import functools
import math

import jax
import jax.numpy as jnp
from jax import lax
from jax.experimental import pallas as pl
from jax.experimental.pallas import tpu as pltpu
from jax.sharding import PartitionSpec as P

GROUPS = 32

eps = 1e-05


LANES = 128
F32 = jnp.float32
BF16 = jnp.bfloat16


def extended(cells, sides, width):
    for axis, dim in sides:
        count = lax.axis_size(axis)
        ends = count - 1
        head = lax.slice_in_dim(cells, 0, width, axis=dim)
        tail = lax.slice_in_dim(cells, cells.shape[dim] - width, cells.shape[dim], axis=dim)
        cells = jnp.concatenate(
            [
                lax.ppermute(tail, axis, [(i, (i + 1) % count) for i in range(ends)]),
                cells,
                lax.ppermute(head, axis, [((i + 1) % count, i) for i in range(ends)]),
            ],
            axis=dim,
        )
    return cells


def conv_rows(padded, kernel, count):
    width = padded.shape[-1]
    wide = jnp.pad(padded, ((0, 0), (0, 0), (0, 0), (1, 1)))
    total = None
    for tap_row in range(3):
        for tap_col in range(3):
            window = wide[:, tap_row : tap_row + count, :, tap_col : tap_col + width]
            term = jnp.einsum(
                "oc,bhcw->bhow",
                kernel[tap_row, tap_col],
                window,
                preferred_element_type=jnp.float32,
            )
            total = term if total is None else total + term
    return total


def group_sum(value):
    batch, rows, chans, width = value.shape
    return jnp.sum(value.reshape(batch, rows, GROUPS, chans // GROUPS, width), axis=(1, 3, 4))


def row_sharded(x_next, x_cur, grad_out, kernel, gamma, beta):
    _, rows, chans, width = x_next.shape
    height_count = lax.axis_size("height")
    count = height_count * rows * (chans // GROUPS) * width
    gain = gamma[None, None, :, None]
    shift_b = beta[None, None, :, None]

    def expand(stat):
        return jnp.repeat(stat, chans // GROUPS, axis=1)[:, None, :, None]

    stacked = jnp.stack((x_next, x_cur))
    padded = extended(stacked, (("height", 2),), 1)
    xp_next = padded[0]
    xp_cur = padded[1]
    z_next = conv_rows(xp_next, kernel, rows)
    z_cur = conv_rows(xp_cur, kernel, rows)
    sum_next, sum_cur, sq_next, sq_cur = lax.psum(
        (group_sum(z_next), group_sum(z_cur), group_sum(z_next * z_next), group_sum(z_cur * z_cur)),
        "height",
    )
    mean_next = sum_next / count
    mean_cur = sum_cur / count
    var_next = sq_next / count - mean_next * mean_next
    var_cur = sq_cur / count - mean_cur * mean_cur
    rstd_next = lax.rsqrt(var_next + eps)
    rstd_cur = lax.rsqrt(var_cur + eps)
    affine_next = (z_next - expand(mean_next)) * expand(rstd_next) * gain + shift_b
    y_next = (affine_next * jax.nn.sigmoid(affine_next)).astype(jnp.bfloat16)
    normed = (z_cur - expand(mean_cur)) * expand(rstd_cur)
    affine = normed * gain + shift_b
    sig = jax.nn.sigmoid(affine)
    grad_n = grad_out.astype(jnp.float32) * (sig * (1.0 + affine * (1.0 - sig))) * gain
    first_sum, second_sum = lax.psum((group_sum(grad_n), group_sum(grad_n * normed)), "height")
    grad_z = (
        expand(rstd_cur)
        * (grad_n - expand(first_sum / count) - normed * expand(second_sum / count))
    ).astype(jnp.bfloat16)
    grad_pad = extended(grad_z, (("height", 1),), 1)
    grad_own = grad_pad[:, 1:-1]
    grad_wide = jnp.pad(grad_pad, ((0, 0), (0, 0), (0, 0), (1, 1)))
    x_wide = jnp.pad(xp_cur, ((0, 0), (0, 0), (0, 0), (1, 1)))
    grad_input = None
    taps = []
    for tap_row in range(3):
        tap_list = []
        for tap_col in range(3):
            window = grad_wide[
                :, 2 - tap_row : 2 - tap_row + rows, :, 2 - tap_col : 2 - tap_col + width
            ]
            term = jnp.einsum(
                "oc,bhow->bhcw",
                kernel[tap_row, tap_col],
                window,
                preferred_element_type=jnp.float32,
            )
            grad_input = term if grad_input is None else grad_input + term
            source = x_wide[:, tap_row : tap_row + rows, :, tap_col : tap_col + width]
            tap_list.append(
                jnp.einsum("bhow,bhcw->oc", grad_own, source, preferred_element_type=jnp.float32)
            )
        taps.append(jnp.stack(tap_list))
    grad_local = jnp.stack(taps)
    grad_x = grad_input.astype(jnp.bfloat16)
    group_count = lax.axis_size("dp")
    piece = grad_local.size // (height_count * group_count)
    blocks = grad_local.reshape(height_count, group_count, piece)
    shares = lax.psum_scatter(blocks, "dp", scatter_dimension=1, tiled=True)
    grad_kernel = lax.psum_scatter(shares, "height", scatter_dimension=0, tiled=True).reshape(piece)
    return (y_next, grad_x, grad_kernel)


def params(limit=None):
    return pltpu.CompilerParams(vmem_limit_bytes=limit or 40 * 1024 * 1024)


def moved(value, by):
    width = value.shape[-1]
    lane = lax.broadcasted_iota(jnp.int32, value.shape, value.ndim - 1)
    rolled = pltpu.roll(value, by % width, value.ndim - 1)
    keep = lane >= by if by > 0 else lane < width + by
    return jnp.where(keep, rolled, jnp.zeros_like(rolled))


def moved_bf16(value, by):
    return moved(value.astype(F32), by).astype(BF16)


def same_group(rows, chans):
    size = chans // GROUPS
    row = lax.broadcasted_iota(jnp.int32, (rows, rows), 0).astype(F32)
    col = lax.broadcasted_iota(jnp.int32, (rows, rows), 1).astype(F32)
    left = jnp.floor((row + 0.5) * (1.0 / size))
    right = jnp.floor((col + 0.5) * (1.0 / size))
    return jnp.where(left == right, 1.0, 0.0).astype(BF16)


def split3(value):
    high = value.astype(BF16)
    rest = value - high.astype(F32)
    mid = rest.astype(BF16)
    low = (rest - mid.astype(F32)).astype(BF16)
    return high, mid, low


def dot(left, right, dims=((1,), (0,))):
    return lax.dot_general(left, right, (dims, ((), ())), preferred_element_type=F32)


def group_totals(same, values, scale):
    width = values[0].shape[1]
    columns = [jnp.sum(value, axis=1, keepdims=True) * scale for value in values]
    wide = jnp.concatenate([jnp.broadcast_to(c, values[0].shape) for c in columns], axis=1)
    high, mid, low = split3(wide)
    total = dot(same, high) + (dot(same, mid) + dot(same, low))
    return [total[:, i * width : (i + 1) * width] for i in range(len(values))]


def lane_tiles(size):
    return [(at, min(LANES, size - at)) for at in range(0, size, LANES)]


def weights_kernel(w_ref, flat_ref):
    chans = flat_ref.shape[1]
    for a in range(3):
        for b in range(3):
            flat_ref[a, :, b * chans : (b + 1) * chans] = w_ref[a, b]


def edge_kernel(x_ref, edge_ref, sem):
    row = (lax.axis_index("height") & 1) * (x_ref.shape[0] - 1)
    copy = pltpu.make_async_copy(x_ref.at[row], edge_ref, sem)
    copy.start()
    copy.wait()


def halves_kernel(own_ref, near_ref, out_ref):
    half = out_ref.shape[2]
    core = lax.axis_index("height") & 1
    mine = pl.ds(pl.multiple_of(core * half, 16), half)
    for r in range(out_ref.shape[1]):
        out_ref[0, r] = own_ref[r, mine]
        out_ref[1, r] = near_ref[r, mine]


def next_conv_kernel(edge_ref, near_ref, x_ref, w_ref, z_ref, stat_ref, *, rows):
    even = (lax.axis_index("height") & 1) == 0
    side = edge_ref[...].astype(F32)
    top = jnp.where(even, side, near_ref[rows - 1].astype(F32)).astype(BF16)
    bottom = jnp.where(even, near_ref[0].astype(F32), side).astype(BF16)
    cells = [top] + [x_ref[r] for r in range(rows)] + [bottom]
    chans, width = cells[0].shape
    sides = [[moved_bf16(cell, 1) for cell in cells], cells, [moved_bf16(cell, -1) for cell in cells]]
    stacks = [jnp.concatenate([side[r] for side in sides], axis=0) for r in range(rows + 2)]
    total = None
    for a in range(3):
        term = dot(w_ref[a], jnp.concatenate(stacks[a : a + rows], axis=1))
        total = term if total is None else total + term
    parts = [total[:, r * width : (r + 1) * width] for r in range(rows)]
    for r in range(rows):
        z_ref[r] = parts[r]
    line = functools.reduce(jnp.add, parts)
    mean = jnp.sum(line, axis=1, keepdims=True) * (1.0 / (rows * width))
    off = functools.reduce(jnp.add, [(part - mean) * (part - mean) for part in parts])
    ones = jnp.ones((8, width), BF16)
    row = lax.broadcasted_iota(jnp.int32, stat_ref.shape, 0)
    packed = jnp.zeros(stat_ref.shape, F32)
    at = 0
    for value in (line, off):
        lane_sum = sum(dot(ones, part, ((1,), (1,))) for part in split3(value))
        for start, size in lane_tiles(chans):
            piece = lane_sum[:1, start : start + size]
            if size < LANES:
                piece = jnp.concatenate([piece, jnp.zeros((1, LANES - size), F32)], axis=1)
            packed = jnp.where(row == at, jnp.broadcast_to(piece, packed.shape), packed)
            at += 1
    stat_ref[...] = packed


def next_out_kernel(*refs, rows, count):
    stat_refs = refs[:-4]
    z_ref, gain_ref, shift_ref, y_ref = refs[-4:]
    chans, width = gain_ref.shape
    same = same_group(chans, chans)
    tiles = lane_tiles(chans)

    def line(value):
        at = value * len(tiles)
        cells = [
            jnp.concatenate([ref[j, at + i : at + i + 1, :size] for i, (_, size) in enumerate(tiles)], axis=1)
            for ref in stat_refs
            for j in range(ref.shape[0])
        ]
        return jnp.concatenate(cells, axis=0)

    sums = line(0)
    offs = line(1)
    each = rows * width
    total = jnp.broadcast_to(jnp.sum(sums, axis=0, keepdims=True), (width, chans))
    mean_line = sum(dot(part, same) for part in split3(total[:8])) * (1.0 / count)
    apart = sums * (1.0 / each) - mean_line[:1]
    spread = jnp.sum(offs + apart * apart * float(each), axis=0, keepdims=True)
    spread = jnp.broadcast_to(spread, (width, chans))
    mean = sum(dot(same, part, ((1,), (1,))) for part in split3(total)) * (1.0 / count)
    var = sum(dot(same, part, ((1,), (1,))) for part in split3(spread)) * (1.0 / count)
    rstd = lax.rsqrt(var + eps)
    for r in range(rows):
        middle = ((z_ref[r] - mean) * rstd * gain_ref[...] + shift_ref[...]) * 0.5
        y_ref[r] = (middle + middle * jnp.tanh(middle)).astype(BF16)


def conv_kernel(*refs, blocks, rows, count, wide):
    x_refs = refs[:blocks]
    w_ref, xs, z, norm, lane = refs[blocks:]
    image, half, width = z.shape
    chans = x_refs[0].shape[1]
    home = lax.axis_index("height")
    mine = pl.ds(pl.multiple_of((home & 1) * half, 16), half)

    edge = jnp.zeros((3 * chans, width), BF16)
    xs[0] = edge
    xs[image + 1] = edge
    for k in range(blocks):
        base = (home ^ k) * rows + 1
        for r in range(rows):
            cell = x_refs[k][r]
            xs[base + r, chans : 2 * chans] = cell
            xs[base + r, :chans] = moved_bf16(cell, 1)
            xs[base + r, 2 * chans :] = moved_bf16(cell, -1)

    def conv(p, start=False):
        row = p * wide
        total = None
        for a in range(3):
            right = jnp.concatenate([xs[row + a + i] for i in range(wide)], axis=1)
            term = dot(w_ref[a, mine], right)
            total = term if total is None else total + term
        parts = [total[:, i * width : (i + 1) * width] for i in range(wide)]
        for i in range(wide):
            z[row + i] = parts[i]
        sums = functools.reduce(jnp.add, parts)
        squares = functools.reduce(jnp.add, [part * part for part in parts])
        lane[0] = sums if start else lane[0] + sums
        lane[1] = squares if start else lane[1] + squares

    conv(0, True)
    lax.fori_loop(1, image // wide, lambda p, carry: conv(p) or carry, 0)
    mean, square = group_totals(same_group(half, chans), (lane[0], lane[1]), 1.0 / count)
    norm[0] = mean
    norm[1] = lax.rsqrt(square - mean * mean + eps)


def pull_kernel(*refs, blocks, rows, count):
    g_refs = refs[: blocks // 2]
    z, norm, gain_ref, shift_ref, gz_ref, gn, ns, coef = refs[blocks // 2 :]
    image, half, _ = z.shape
    chans = gain_ref.shape[0]
    home = lax.axis_index("height")
    core = home & 1
    step = 16

    def pulled(i, carry):
        start = pl.multiple_of(i * step, step)
        at = pl.ds(start, step)
        all_at = pl.ds(pl.multiple_of(core * half + start, step), step)
        mean = norm[0, at]
        rstd = norm[1, at]
        gain = gain_ref[all_at] * 0.5
        shift = shift_ref[all_at] * 0.5
        first = None
        second = None
        for k in range(blocks):
            base = (home ^ k) * rows
            for r in range(rows):
                n = (z[base + r, at] - mean) * rstd
                middle = n * gain + shift
                bent = jnp.tanh(middle)
                slope = (1.0 + bent) * (1.0 + middle * (1.0 - bent))
                value = (g_refs[k // 2][k % 2, r, at].astype(F32) * gain) * slope
                gn[base + r, at] = value
                ns[base + r, at] = n
                first = value if first is None else first + value
                second = value * n if second is None else second + value * n
        coef[0, at] = first
        coef[1, at] = second
        return carry

    lax.fori_loop(0, half // step, pulled, 0)
    coef[0], coef[1] = group_totals(same_group(half, chans), (coef[0], coef[1]), 1.0 / count)

    def rounded(i, carry):
        at = pl.ds(pl.multiple_of(i * step, step), step)
        mean1 = coef[0, at]
        mean2 = coef[1, at]
        rstd = norm[1, at]
        for r in range(image):
            gz_ref[r, at] = (rstd * (gn[r, at] - mean1 - ns[r, at] * mean2)).astype(BF16)
        return carry

    lax.fori_loop(0, half // step, rounded, 0)


def filter_kernel(own_ref, other_ref, xs, *refs, blocks, rows, groups_dp, span):
    outs = refs[:groups_dp]
    gz_out, gz, taps, flat = refs[groups_dp:]
    image, half, width = own_ref.shape
    chans = 2 * half
    home = lax.axis_index("height")
    part = lax.axis_index("dp")
    core = home & 1
    step = 16

    edge = jnp.zeros((chans, width), BF16)
    gz[0] = edge
    gz[image + 1] = edge
    for r in range(image):
        gz[r + 1, pl.ds(pl.multiple_of(core * half, step), half)] = own_ref[r]
        gz[r + 1, pl.ds(pl.multiple_of((1 - core) * half, step), half)] = other_ref[r]
    for r in range(rows + 2):
        gz_out[r] = gz[home * rows + r]

    block = 9 * chans // blocks
    tap0 = (home * block) // chans
    left = jnp.concatenate([gz[r + 1] for r in range(image)], axis=1)
    for j in range(span):
        tap = jnp.minimum(tap0 + j, 8)
        a = tap // 3
        side = pl.ds(pl.multiple_of((tap - a * 3) * chans, step), chans)
        right = jnp.concatenate([xs[r + a, side] for r in range(image)], axis=1)
        rows_of = dot(left, right, ((1,), (1,)))
        for i, (start, size) in enumerate(lane_tiles(chans)):
            taps[i, j * chans : (j + 1) * chans, :size] = rows_of[:, start : start + size]

    off = pl.multiple_of(home * block - tap0 * chans, 8)
    shared = math.gcd(chans, LANES)
    few, many = LANES // shared, chans // shared
    for i in range(taps.shape[0]):
        taps[i, :block] = taps[i, pl.ds(off, block)]
    lines = jnp.concatenate(
        [
            taps[i, pl.ds(line, block // few, stride=few)][:, :size]
            for line in range(few)
            for i, (_, size) in enumerate(lane_tiles(chans))
        ],
        axis=1,
    )
    for i in range(many):
        flat[pl.ds(i, block // few, stride=many)] = lines[:, i * LANES : (i + 1) * LANES]
    piece = flat.shape[0] // groups_dp
    for s in range(groups_dp):
        dest = part ^ s
        value = flat[pl.ds(dest * piece, piece)]
        outs[s][...] = value.astype(outs[s].dtype)


def grad_x_kernel(gz_ref, w_ref, out_ref, *, rows):
    chans, width = gz_ref.shape[1:]
    total = None
    for a in range(3):
        right = jnp.concatenate([gz_ref[2 - a + r] for r in range(rows)], axis=1)
        term = dot(w_ref[a], right, ((0,), (0,)))
        total = term if total is None else total + term
    for r in range(rows):
        part = total[:, r * width : (r + 1) * width]
        value = part[chans : 2 * chans]
        value = value + moved(part[:chans], -1) + moved(part[2 * chans :], 1)
        out_ref[r] = value.astype(BF16)


def vmem(count):
    return [pl.BlockSpec(memory_space=pltpu.VMEM)] * count


def pairs(size, offset):
    return [(i, i ^ offset) for i in range(size)]


def call(kernel, out_shape, args, scratch=(), flops=0, **static):
    single = not isinstance(out_shape, tuple)
    return pl.pallas_call(
        functools.partial(kernel, **static),
        out_shape=out_shape,
        in_specs=vmem(len(args)),
        out_specs=vmem(1)[0] if single else tuple(vmem(len(out_shape))),
        scratch_shapes=list(scratch),
        compiler_params=params(),
        cost_estimate=pl.CostEstimate(flops=flops, bytes_accessed=0, transcendentals=0),
    )(*args)


def gathered(x_next, x_cur, grad_out, kernel, gamma, beta):
    rows, chans, width = x_next.shape[1:]
    blocks = lax.axis_size("height")
    groups_dp = lax.axis_size("dp")
    image = blocks * rows
    half = chans // 2
    count = image * (chans // GROUPS) * width
    block = 9 * chans // blocks
    span = max((h * block % chans + block - 1) // chans + 1 for h in range(blocks))
    piece = block * chans // (groups_dp * LANES)
    flops = 18 * chans * chans * width
    x_next, grad_out = x_next[0], grad_out[0]
    shape = jax.ShapeDtypeStruct

    chips = sorted(range(2, blocks, 2), key=lambda k: bin(k).count("1"))

    def far(own, offsets):
        return {k: lax.ppermute(own, "height", pairs(blocks, k)) for k in offsets}

    def near(own):
        return lax.ppermute(own, "height", pairs(blocks, 1))

    x_far = {0: x_cur[0]} | far(x_cur[0], chips)
    edge = pl.pallas_call(
        edge_kernel,
        out_shape=shape((chans, width), BF16),
        in_specs=[pl.BlockSpec(memory_space=pltpu.HBM)],
        out_specs=vmem(1)[0],
        scratch_shapes=[pltpu.SemaphoreType.DMA],
        compiler_params=params(),
        cost_estimate=pl.CostEstimate(flops=image * flops, bytes_accessed=0, transcendentals=0),
        name="edge",
    )(pltpu.with_memory_space_constraint(x_next, pltpu.HBM))
    next_near = near(x_next)
    swaps = [(i, i + 1) for i in range(1, blocks - 1, 2)]
    edge = lax.ppermute(edge, "height", swaps + [(j, i) for i, j in swaps])
    g_near = near(grad_out)
    g_pair = call(
        halves_kernel, shape((2, rows, half, width), BF16), (grad_out, g_near), flops=image * flops
    )
    g_far = {0: g_pair} | far(g_pair, chips)
    gain = jnp.broadcast_to(gamma[:, None], (chans, width))
    shift = jnp.broadcast_to(beta[:, None], (chans, width))
    w_flat = call(weights_kernel, shape((3, chans, 3 * chans), BF16), (kernel,))

    x_far, w_flat, gain, shift, _ = lax.optimization_barrier((x_far, w_flat, gain, shift, g_pair))
    x_all = []
    for k in range(0, blocks, 2):
        x_all += [x_far[k], near(x_far[k])]
    z_next, stat = call(
        next_conv_kernel,
        (shape((rows, chans, width), F32), shape((8 * -(-2 * len(lane_tiles(chans)) // 8), LANES), F32)),
        (edge, next_near, x_next, w_flat),
        flops=rows * flops,
        rows=rows,
    )
    stat_near = near(stat)
    x_all, z_next = lax.optimization_barrier((x_all, z_next))
    xs, z_cur, norm = call(
        conv_kernel,
        (
            shape((image + 2, 3 * chans, width), BF16),
            shape((image, half, width), F32),
            shape((2, half, width), F32),
        ),
        (*x_all, w_flat),
        scratch=(pltpu.VMEM((2, half, width), F32),),
        flops=image * flops // 2,
        blocks=blocks,
        rows=rows,
        count=count,
        wide=4 if image % 4 == 0 else 2,
    )
    stat_pair = jnp.stack((stat, stat_near))
    gz_own = call(
        pull_kernel,
        shape((image, half, width), BF16),
        (*[g_far[k] for k in range(0, blocks, 2)], z_cur, norm, gain, shift),
        scratch=(
            pltpu.VMEM((image, half, width), F32),
            pltpu.VMEM((image, half, width), F32),
            pltpu.VMEM((2, half, width), F32),
        ),
        flops=image * flops // 8,
        blocks=blocks,
        rows=rows,
        count=count,
    )
    gz_other = near(gz_own)
    stat_pair, gz_own = lax.optimization_barrier((stat_pair, gz_own))
    stat_far = far(stat_pair, chips)
    results = call(
        filter_kernel,
        (shape((piece, LANES), F32),)
        + (shape((piece, LANES), BF16),) * (groups_dp - 1)
        + (shape((rows + 2, chans, width), BF16),),
        (gz_own, gz_other, xs),
        scratch=(
            pltpu.VMEM((image + 2, chans, width), BF16),
            pltpu.VMEM((len(lane_tiles(chans)), span * chans, LANES), F32),
            pltpu.VMEM((groups_dp * piece, LANES), F32),
        ),
        flops=image * flops // 4,
        blocks=blocks,
        rows=rows,
        groups_dp=groups_dp,
        span=span,
    )
    total = results[0]
    for s in range(groups_dp - 1, 0, -1):
        total = total + lax.ppermute(results[s], "dp", pairs(groups_dp, s)).astype(F32)
    grad_x = call(
        grad_x_kernel,
        shape((rows, chans, width), BF16),
        (results[groups_dp], w_flat),
        flops=rows * flops,
        rows=rows,
    )
    y_next = call(
        next_out_kernel,
        shape((rows, chans, width), BF16),
        (stat_pair, *stat_far.values(), z_next, gain, shift),
        flops=rows * flops // 4,
        rows=rows,
        count=count,
    )
    return (y_next[None], grad_x[None], total.reshape(piece * LANES))


def fits(shape, blocks, groups_dp):
    batch, rows, chans, width = shape
    image = blocks * rows
    scratch = image * chans * width * 20 + 9 * chans * chans * 4
    few = LANES // math.gcd(chans, LANES)
    return (
        batch == 1
        and width == LANES
        and chans % 32 == 0
        and chans % GROUPS == 0
        and GROUPS % 2 == 0
        and blocks > 1
        and image % 2 == 0
        and blocks & (blocks - 1) == 0
        and groups_dp & (groups_dp - 1) == 0
        and (9 * chans) % (8 * blocks) == 0
        and (9 * chans // blocks) % few == 0
        and (9 * chans // blocks) * chans % (groups_dp * LANES) == 0
        and scratch < 32 * 1024 * 1024
    )


def solution(mesh):
    blocks, groups_dp = mesh.shape["height"], mesh.shape["dp"]

    def local(x_next, x_cur, grad_out, kernel, gamma, beta):
        if not fits(x_next.shape, blocks, groups_dp):
            return row_sharded(x_next, x_cur, grad_out, kernel, gamma, beta)
        return gathered(x_next, x_cur, grad_out, kernel, gamma, beta)

    placed = (
        P("dp", "height", None, None),
        P("dp", "height", None, None),
        P("dp", "height", None, None),
        P(),
        P(),
        P(),
    )
    return jax.shard_map(
        local,
        mesh=mesh,
        in_specs=placed,
        out_specs=(
            P("dp", "height", None, None),
            P("dp", "height", None, None),
            P(("height", "dp")),
        ),
        check_vma=False,
    )
```
